8 devices in a mesh: dp: 1 (over z), tp: 2 (over y), cp: 4 (over x, core).
Axes of the slice: x: 2, y: 2, z: 1, core: 2. Of those that a mesh axis runs over, the one named last changes fastest.
Arguments:
- x_in: bfloat16 [4096, 896], P(('dp', 'cp', 'tp'))
- w_query: bfloat16 [896, 14, 64], P(None, 'tp')
- w_key: bfloat16 [896, 2, 64], P(None, 'tp')
- w_value: bfloat16 [896, 2, 64], P(None, 'tp')
- w_out: bfloat16 [14, 64, 896], P('tp')
- d_out: bfloat16 [4096, 896], P(('dp', 'cp', 'tp'))
Outputs:
- output 1: bfloat16 [4096, 896], P(('dp', 'cp', 'tp'))
- output 2: bfloat16 [4096, 896], P(('dp', 'cp', 'tp'))
- output 3: bfloat16 [4, 896, 14, 64], P(('dp', 'cp'), None, 'tp')
- output 4: bfloat16 [4, 896, 2, 64], P(('dp', 'cp'), None, 'tp')
- output 5: bfloat16 [4, 896, 2, 64], P(('dp', 'cp'), None, 'tp')
- output 6: bfloat16 [4, 14, 64, 896], P(('dp', 'cp'), 'tp')
All inputs are finite; a program needn't handle non-finite values.
Results may differ from the reference program's by a relative error of at most 0.0103152.
Values are sent between devices in bfloat16 or wider.
A program may use at most 1 GiB of HBM per device.

```python
import math
import jax
import jax.numpy as jnp
from jax import lax

MODEL_DIM = 896
NUM_HEADS = 14
NUM_KV_HEADS = 2
HEAD_DIM = 64
SEQ_LEN = 4096
SEQ_SHARDS = 4
QUERY_BLOCK = 32


def setup_inputs(seed: int = 0, part: int = 0) -> dict:
    shared_keys = jax.random.split(jax.random.key(seed), 4)
    part_keys = jax.random.split(jax.random.fold_in(jax.random.key(seed), part), 2)
    logit_gain = 1.6
    in_scale = 1.0 / math.sqrt(MODEL_DIM)
    x_in = jax.random.normal(part_keys[0], (SEQ_LEN, MODEL_DIM), jnp.float32)
    w_query = jax.random.normal(shared_keys[0], (MODEL_DIM, NUM_HEADS, HEAD_DIM), jnp.float32) * (logit_gain * in_scale)
    w_key = jax.random.normal(shared_keys[1], (MODEL_DIM, NUM_KV_HEADS, HEAD_DIM), jnp.float32) * (logit_gain * in_scale)
    w_value = jax.random.normal(shared_keys[2], (MODEL_DIM, NUM_KV_HEADS, HEAD_DIM), jnp.float32) * in_scale
    w_out = jax.random.normal(shared_keys[3], (NUM_HEADS, HEAD_DIM, MODEL_DIM), jnp.float32) / math.sqrt(NUM_HEADS * HEAD_DIM)
    d_out = jax.random.normal(part_keys[1], (SEQ_LEN, MODEL_DIM), jnp.float32)
    return {"x_in": x_in.astype(jnp.bfloat16), "w_query": w_query.astype(jnp.bfloat16), "w_key": w_key.astype(jnp.bfloat16), "w_value": w_value.astype(jnp.bfloat16), "w_out": w_out.astype(jnp.bfloat16), "d_out": d_out.astype(jnp.bfloat16)}


def stored_positions():
    half_rows = SEQ_LEN // (2 * SEQ_SHARDS)
    row_ids = jnp.arange(SEQ_LEN, dtype=jnp.int32)
    shard_id = row_ids // (2 * half_rows)
    within = row_ids % (2 * half_rows)
    return jnp.where(within < half_rows, shard_id * half_rows + within, (2 * SEQ_SHARDS - 1 - shard_id) * half_rows + within - half_rows)


def reference(x_in, w_query, w_key, w_value, w_out, d_out):
    groups = NUM_HEADS // NUM_KV_HEADS
    attn_scale = 1.0 / math.sqrt(HEAD_DIM)
    n_blocks = SEQ_LEN // QUERY_BLOCK
    shard_rows = SEQ_LEN // SEQ_SHARDS
    q_cols = NUM_HEADS * HEAD_DIM
    kv_cols = NUM_KV_HEADS * HEAD_DIM
    wq_flat = w_query.reshape(MODEL_DIM, q_cols)
    wk_flat = w_key.reshape(MODEL_DIM, kv_cols)
    wv_flat = w_value.reshape(MODEL_DIM, kv_cols)
    wo_flat = w_out.reshape(q_cols, MODEL_DIM)
    q_flat = jnp.dot(x_in, wq_flat, preferred_element_type=jnp.float32).astype(jnp.bfloat16)
    k_flat = jnp.dot(x_in, wk_flat, preferred_element_type=jnp.float32).astype(jnp.bfloat16)
    v_flat = jnp.dot(x_in, wv_flat, preferred_element_type=jnp.float32).astype(jnp.bfloat16)
    positions = stored_positions()
    k_heads = k_flat.reshape(SEQ_LEN, NUM_KV_HEADS, HEAD_DIM).astype(jnp.float32)
    v_heads = v_flat.reshape(SEQ_LEN, NUM_KV_HEADS, HEAD_DIM).astype(jnp.float32)
    q_blocks = q_flat.reshape(n_blocks, QUERY_BLOCK, NUM_KV_HEADS, groups, HEAD_DIM)
    pos_blocks = positions.reshape(n_blocks, QUERY_BLOCK)

    def block_scores(q_blk, pos_blk):
        scores = jnp.einsum("qhgd,khd->qhgk", q_blk.astype(jnp.float32), k_heads) * attn_scale
        visible = pos_blk[:, None, None, None] >= positions[None, None, None, :]
        return jnp.where(visible, scores, -jnp.inf)

    def forward_block(block_in):
        q_blk, pos_blk = block_in
        scores = block_scores(q_blk, pos_blk)
        row_max = jnp.max(scores, axis=-1)
        prob_mat = jnp.exp(scores - row_max[..., None])
        row_sum = jnp.sum(prob_mat, axis=-1)
        pv_sum = jnp.einsum("qhgk,khd->qhgd", prob_mat.astype(jnp.bfloat16).astype(jnp.float32), v_heads)
        out_blk = (pv_sum / row_sum[..., None]).astype(jnp.bfloat16)
        return out_blk, row_max + jnp.log(row_sum)

    o_blocks, lse_blocks = lax.map(forward_block, (q_blocks, pos_blocks))
    o_flat = o_blocks.reshape(SEQ_LEN, q_cols)
    y_out = jnp.dot(o_flat, wo_flat, preferred_element_type=jnp.float32).astype(jnp.bfloat16)

    do_flat = jnp.dot(d_out, wo_flat.T, preferred_element_type=jnp.float32).astype(jnp.bfloat16)
    do_blocks = do_flat.reshape(n_blocks, QUERY_BLOCK, NUM_KV_HEADS, groups, HEAD_DIM)
    dot_blocks = jnp.sum(do_blocks.astype(jnp.float32) * o_blocks.astype(jnp.float32), axis=-1)

    def backward_block(grad_carry, block_in):
        dk_acc, dv_acc = grad_carry
        q_blk, pos_blk, lse_blk, do_blk, dot_blk = block_in
        scores = block_scores(q_blk, pos_blk)
        prob_mat = jnp.exp(scores - lse_blk[..., None])
        do_wide = do_blk.astype(jnp.float32)
        d_probs = jnp.einsum("qhgd,khd->qhgk", do_wide, v_heads)
        d_scores = (prob_mat * (d_probs - dot_blk[..., None])).astype(jnp.bfloat16).astype(jnp.float32)
        dv_acc = dv_acc + jnp.einsum("qhgk,qhgd->khd", prob_mat.astype(jnp.bfloat16).astype(jnp.float32), do_wide)
        dk_acc = dk_acc + jnp.einsum("qhgk,qhgd->khd", d_scores, q_blk.astype(jnp.float32)) * attn_scale
        dq_blk = jnp.einsum("qhgk,khd->qhgd", d_scores, k_heads) * attn_scale
        return (dk_acc, dv_acc), dq_blk.astype(jnp.bfloat16)

    zero_kv = jnp.zeros((SEQ_LEN, NUM_KV_HEADS, HEAD_DIM), jnp.float32)
    grad_kv, dq_blocks = lax.scan(backward_block, (zero_kv, zero_kv), (q_blocks, pos_blocks, lse_blocks, do_blocks, dot_blocks))
    dq_flat = dq_blocks.reshape(SEQ_LEN, q_cols)
    dk_flat = grad_kv[0].astype(jnp.bfloat16).reshape(SEQ_LEN, kv_cols)
    dv_flat = grad_kv[1].astype(jnp.bfloat16).reshape(SEQ_LEN, kv_cols)
    dx_sum = (jnp.dot(dq_flat, wq_flat.T, preferred_element_type=jnp.float32)
              + jnp.dot(dk_flat, wk_flat.T, preferred_element_type=jnp.float32)
              + jnp.dot(dv_flat, wv_flat.T, preferred_element_type=jnp.float32))
    grad_x = dx_sum.astype(jnp.bfloat16)
    x_shards = x_in.reshape(SEQ_SHARDS, shard_rows, MODEL_DIM).astype(jnp.float32)
    grad_wq = jnp.einsum("rsm,rsc->rmc", x_shards, dq_flat.reshape(SEQ_SHARDS, shard_rows, q_cols).astype(jnp.float32)).astype(jnp.bfloat16).reshape(SEQ_SHARDS, MODEL_DIM, NUM_HEADS, HEAD_DIM)
    grad_wk = jnp.einsum("rsm,rsc->rmc", x_shards, dk_flat.reshape(SEQ_SHARDS, shard_rows, kv_cols).astype(jnp.float32)).astype(jnp.bfloat16).reshape(SEQ_SHARDS, MODEL_DIM, NUM_KV_HEADS, HEAD_DIM)
    grad_wv = jnp.einsum("rsm,rsc->rmc", x_shards, dv_flat.reshape(SEQ_SHARDS, shard_rows, kv_cols).astype(jnp.float32)).astype(jnp.bfloat16).reshape(SEQ_SHARDS, MODEL_DIM, NUM_KV_HEADS, HEAD_DIM)
    grad_wo = jnp.einsum("rsc,rsm->rcm", o_flat.reshape(SEQ_SHARDS, shard_rows, q_cols).astype(jnp.float32), d_out.reshape(SEQ_SHARDS, shard_rows, MODEL_DIM).astype(jnp.float32)).astype(jnp.bfloat16).reshape(SEQ_SHARDS, NUM_HEADS, HEAD_DIM, MODEL_DIM)
    return y_out, grad_x, grad_wq, grad_wk, grad_wv, grad_wo
```

```python
import functools
import math

import jax
import jax.numpy as jnp
from jax import lax
from jax.experimental import pallas as pl
from jax.experimental.pallas import tpu as pltpu
from jax.sharding import PartitionSpec as P

ROW_SPEC = P(("dp", "cp", "tp"), None)
HEAD_SPEC = P(None, "tp", None)
OUT_W_SPEC = P("tp", None, None)
GRAD_SPEC = P(("dp", "cp"), None, "tp", None)
GRAD_OUT_SPEC = P(("dp", "cp"), "tp", None, None)
F32 = jnp.float32
BF16 = jnp.bfloat16
NT = (((1,), (1,)), ((), ()))
VMEM = pl.BlockSpec(memory_space=pltpu.VMEM)
SMEM = pl.BlockSpec(memory_space=pltpu.SMEM)
VMEM_LIMIT = 60 * 1024 * 1024


def dot(a, b):
    return jnp.dot(a, b, preferred_element_type=F32)


def dot_nt(a, b):
    return lax.dot_general(a, b, NT, preferred_element_type=F32)


def unit_list(rank, half, dists):
    units = []
    for d in dists:
        if d == 0:
            units += [(half, half, True, True), (1 - half, half, False, False), (1 - half, 1 - half, True, False)]
        else:
            early = rank >= d
            units += [(jnp.where(early, half, 1 - half), 2 * d + half, False, early),
                      (1 - half, 2 * d + jnp.where(early, half, 1 - half), False, False)]
    return units


def diag_mask(rows, cols):
    key = lax.broadcasted_iota(jnp.int32, (rows, cols), 0)
    query = lax.broadcasted_iota(jnp.int32, (rows, cols), 1)
    return query >= key


def pick(flag, a, b):
    if flag is True:
        return a
    if flag is False:
        return b
    return jnp.where(flag, a, b)


def transpose_bf16(x):
    return x.astype(F32).T.astype(BF16)


def fwd_kernel(c_scale, n_heads, hd, idx_ref, q0_ref, q1_ref, *refs):
    kv_refs = refs[:8]
    o_ref, lse_ref = refs[8:10]
    q_s, k_s, vt_s, s_s = refs[10:]
    rank, half = idx_ref[0], idx_ref[1]
    n_cols = q_s.shape[-1]
    q_s[0] = q0_ref[...]
    q_s[1] = q1_ref[...]
    for tile in range(8):
        k_s[tile] = transpose_bf16(kv_refs[tile][:hd, :])
        vt_s[tile] = kv_refs[tile][hd:, :]
    units = unit_list(rank, half, (0, 1, 2, 3))
    groups = n_cols // 8

    def head(h, _):
        maxes = []
        for u, (qi, kt, diag, _) in enumerate(units):
            s = dot(k_s[kt], q_s[qi, h])
            if diag:
                s = jnp.where(diag_mask(n_cols, n_cols), s, -jnp.inf)
            s_s[u] = s
            maxes.append(jnp.max(s.reshape(groups, 8, n_cols), axis=0))
        m_half = [None, None]
        for (_, _, _, first), mx in zip(units, maxes):
            for g in (0, 1):
                if first is (g == 1):
                    continue
                val = mx if isinstance(first, bool) else jnp.where(first if g == 0 else jnp.logical_not(first), mx, -jnp.inf)
                m_half[g] = val if m_half[g] is None else jnp.maximum(m_half[g], val)
        m_half = [jnp.max(m, axis=0, keepdims=True) * c_scale for m in m_half]
        l_half = [jnp.zeros((8, n_cols), F32), jnp.zeros((8, n_cols), F32)]
        o_half = [jnp.zeros((hd, n_cols), F32), jnp.zeros((hd, n_cols), F32)]
        for u, (qi, kt, diag, first) in enumerate(units):
            m = pick(first, m_half[0], m_half[1])
            p = jnp.exp2(s_s[u] * c_scale - m)
            l_u = jnp.sum(p.reshape(groups, 8, n_cols), axis=0)
            o_u = dot(vt_s[kt], p.astype(BF16))
            if isinstance(first, bool):
                g = 0 if first else 1
                l_half[g] += l_u
                o_half[g] += o_u
            else:
                l_half = [l_half[0] + jnp.where(first, l_u, 0.0), l_half[1] + jnp.where(first, 0.0, l_u)]
                o_half = [o_half[0] + jnp.where(first, o_u, 0.0), o_half[1] + jnp.where(first, 0.0, o_u)]
        for g in (0, 1):
            slot = half if g == 0 else 1 - half
            l_row = jnp.sum(l_half[g], axis=0, keepdims=True)
            o_ref[slot, h] = (o_half[g] / l_row).astype(BF16)
            lse_ref[slot, h] = m_half[g] + jnp.log2(l_row)
        return 0

    lax.fori_loop(0, n_heads, head, 0)


def bwd_kernel(c_scale, scale, n_heads, hd, dists, first_call, idx_ref, q0_ref, q1_ref, d0_ref, d1_ref, o_ref, lse_ref, *refs):
    n_kv = 2 * len(dists)
    kv_refs = refs[:n_kv]
    refs = refs[n_kv:]
    if not first_call:
        dq_in, refs = refs[0], refs[1:]
    dq_ref, dkv_ref = refs[:2]
    q_s, do_s, k_s, v_s, kt_s = refs[2:]
    rank, half = idx_ref[0], idx_ref[1]
    n_cols = q_s.shape[-1]
    q_s[0] = q0_ref[...]
    q_s[1] = q1_ref[...]
    do_s[0] = d0_ref[...]
    do_s[1] = d1_ref[...]
    base = 2 * dists[0]
    for tile in range(n_kv):
        k_s[tile] = transpose_bf16(kv_refs[tile][:hd, :])
        v_s[tile] = transpose_bf16(kv_refs[tile][hd:, :])
        kt_s[tile] = kv_refs[tile][:hd, :]
    dkv_ref[...] = jnp.zeros_like(dkv_ref)
    units = unit_list(rank, half, dists)

    def head(h, _):
        delta, lse = [], []
        for g in (0, 1):
            slot = half if g == 0 else 1 - half
            delta.append(jnp.sum(do_s[slot, h].astype(F32) * o_ref[slot, h].astype(F32), axis=0, keepdims=True))
            lse.append(lse_ref[slot, h])
        dq_half = [jnp.zeros((hd, n_cols), F32), jnp.zeros((hd, n_cols), F32)]
        for qi, kt, diag, first in units:
            kt = kt - base
            q, do = q_s[qi, h], do_s[qi, h]
            p = jnp.exp2(dot(k_s[kt], q) * c_scale - pick(first, lse[0], lse[1]))
            if diag:
                p = jnp.where(diag_mask(n_cols, n_cols), p, 0.0)
            ds = (p * (dot(v_s[kt], do) - pick(first, delta[0], delta[1]))).astype(BF16)
            dkv_ref[kt, hd:, :] += dot_nt(do, p.astype(BF16))
            dkv_ref[kt, :hd, :] += dot_nt(q, ds)
            dq_u = dot(kt_s[kt], ds)
            if isinstance(first, bool):
                dq_half[0 if first else 1] += dq_u
            else:
                dq_half = [dq_half[0] + jnp.where(first, dq_u, 0.0), dq_half[1] + jnp.where(first, 0.0, dq_u)]
        for g in (0, 1):
            slot = half if g == 0 else 1 - half
            if first_call:
                dq_ref[slot, h] = dq_half[g]
            else:
                dq_ref[slot, h] = ((dq_half[g] + dq_in[slot, h]) * scale).astype(BF16)
        return 0

    lax.fori_loop(0, n_heads, head, 0)
    dkv_ref[:, :hd, :] = dkv_ref[:, :hd, :] * scale


def solution(mesh):
    seq_shards = mesh.shape["cp"]

    def device_fn(x_own, w_query, w_key, w_value, w_out, dy_own):
        rank = lax.axis_index("cp")
        half = lax.axis_index("tp")
        model_dim, n_heads, hd = w_query.shape
        n_cols = x_own.shape[0]
        hw = n_heads * hd
        scale = hd ** -0.5
        c_scale = scale * math.log2(math.e)
        idx = jnp.stack([rank, half]).astype(jnp.int32)
        swap = [(0, 1), (1, 0)]
        wq = w_query.reshape(model_dim, hw)
        wkv = jnp.concatenate([w_key.reshape(model_dim, hd), w_value.reshape(model_dim, hd)], axis=1)
        wo = w_out.reshape(hw, model_dim)

        def peer(a):
            return lax.ppermute(a, "tp", swap)

        def ring(a, d):
            return lax.ppermute(a, "cp", [(i, (i + d) % seq_shards) for i in range(seq_shards)])

        def proj_t(w, rows):
            return lax.dot_general(w, rows, (((0,), (1,)), ((), ())), preferred_element_type=F32).astype(BF16)

        x_peer = peer(x_own)
        dy_peer = peer(dy_own)
        kv_own = proj_t(wkv, x_own)
        q_own = proj_t(wq, x_own).reshape(n_heads, hd, n_cols)
        do_own = lax.dot_general(wo, dy_own, NT, preferred_element_type=F32).astype(BF16).reshape(n_heads, hd, n_cols)
        kv_peer = proj_t(wkv, x_peer)
        q_peer = proj_t(wq, x_peer).reshape(n_heads, hd, n_cols)
        do_peer = lax.dot_general(wo, dy_peer, NT, preferred_element_type=F32).astype(BF16).reshape(n_heads, hd, n_cols)
        kvs = [kv_own, kv_peer]
        for d in range(1, seq_shards):
            kvs += [ring(kv_own, d), ring(kv_peer, d)]

        core = rank % 2
        pair = [(0, 1), (1, 0), (2, 3), (3, 2)]

        def fetch(w):
            rows = w.shape[0] // 2
            got = peer(lax.dynamic_slice_in_dim(w, core * rows, rows, 0))
            other = lax.ppermute(got, "cp", pair)
            return jnp.where(core == 0, jnp.concatenate([got, other]), jnp.concatenate([other, got]))

        wq_p, wkv_p, wo_p = fetch(wq), fetch(wkv), fetch(wo)

        units_all = n_heads * 9
        tile_fl = 2 * n_cols * n_cols * hd
        o_t, lse = pl.pallas_call(
            functools.partial(fwd_kernel, c_scale, n_heads, hd),
            out_shape=(jax.ShapeDtypeStruct((2, n_heads, hd, n_cols), BF16), jax.ShapeDtypeStruct((2, n_heads, 1, n_cols), F32)),
            in_specs=[SMEM] + [VMEM] * 10,
            out_specs=(VMEM, VMEM),
            scratch_shapes=[pltpu.VMEM((2, n_heads, hd, n_cols), BF16), pltpu.VMEM((8, n_cols, hd), BF16),
                            pltpu.VMEM((8, hd, n_cols), BF16), pltpu.VMEM((9, n_cols, n_cols), F32)],
            compiler_params=pltpu.CompilerParams(vmem_limit_bytes=VMEM_LIMIT),
            cost_estimate=pl.CostEstimate(flops=units_all * 2 * tile_fl * 4, bytes_accessed=4 << 20, transcendentals=units_all * n_cols * n_cols),
            name="attend",
        )(idx, q_own, q_peer, *kvs)

        def bwd(dists, first_call, extra):
            tiles = 2 * len(dists)
            n_units = 3 if dists == (0,) else 2 * len(dists)
            return pl.pallas_call(
                functools.partial(bwd_kernel, c_scale, scale, n_heads, hd, dists, first_call),
                out_shape=(jax.ShapeDtypeStruct((2, n_heads, hd, n_cols), F32 if first_call else BF16),
                           jax.ShapeDtypeStruct((tiles, 2 * hd, n_cols), F32)),
                in_specs=[SMEM] + [VMEM] * (6 + tiles + len(extra)),
                out_specs=(VMEM, VMEM),
                scratch_shapes=[pltpu.VMEM((2, n_heads, hd, n_cols), BF16), pltpu.VMEM((2, n_heads, hd, n_cols), BF16),
                                pltpu.VMEM((tiles, n_cols, hd), BF16), pltpu.VMEM((tiles, n_cols, hd), BF16),
                                pltpu.VMEM((tiles, hd, n_cols), BF16)],
                compiler_params=pltpu.CompilerParams(vmem_limit_bytes=VMEM_LIMIT),
                cost_estimate=pl.CostEstimate(flops=n_heads * n_units * 5 * tile_fl * 4, bytes_accessed=4 << 20,
                                              transcendentals=n_heads * n_units * n_cols * n_cols),
                name="attend_grad",
            )(idx, q_own, q_peer, do_own, do_peer, o_t, lse, *kvs[2 * dists[0]:2 * dists[-1] + 2], *extra)

        o_got = peer(o_t[1]).reshape(hw, n_cols)
        dq_part, dkv_far = bwd((1, 2, 3), True, ())
        dq_t, dkv_near = bwd((0,), False, (dq_part,))
        for d in range(1, seq_shards):
            dkv_near = dkv_near + ring(dkv_far[2 * d - 2:2 * d], -d)
        dkv = dkv_near.astype(BF16)
        dq_got = peer(dq_t[1]).reshape(hw, n_cols)
        dkv_got = peer(dkv[1])

        def tn(a, b):
            return lax.dot_general(a, b, (((0,), (0,)), ((), ())), preferred_element_type=F32)

        o_t = o_t.reshape(2, hw, n_cols)
        dq_t = dq_t.reshape(2, hw, n_cols)
        y_blk = (tn(o_t[0], wo) + tn(o_got, wo_p)).astype(BF16)
        grad_wo = (dot(o_t[0], dy_own) + dot(o_t[1], dy_peer)).astype(BF16).reshape(n_heads, hd, model_dim)

        def back(g, w):
            return lax.dot_general(g, w, (((0,), (1,)), ((), ())), preferred_element_type=F32)

        dx_blk = (back(dq_t[0], wq) + back(dq_got, wq_p) + back(dkv[0], wkv) + back(dkv_got, wkv_p)).astype(BF16)

        def wgrad(g):
            own = lax.dot_general(x_own, g[0], (((0,), (1,)), ((), ())), preferred_element_type=F32)
            return (own + lax.dot_general(x_peer, g[1], (((0,), (1,)), ((), ())), preferred_element_type=F32)).astype(BF16)

        grad_wq = wgrad(dq_t).reshape(model_dim, n_heads, hd)
        grad_wkv = wgrad(dkv)
        grad_wk = grad_wkv[:, :hd].reshape(model_dim, 1, hd)
        grad_wv = grad_wkv[:, hd:].reshape(model_dim, 1, hd)
        return y_blk, dx_blk, grad_wq[None], grad_wk[None], grad_wv[None], grad_wo[None]

    return jax.shard_map(device_fn, mesh=mesh,
                         in_specs=(ROW_SPEC, HEAD_SPEC, HEAD_SPEC, HEAD_SPEC, OUT_W_SPEC, ROW_SPEC),
                         out_specs=(ROW_SPEC, ROW_SPEC, GRAD_SPEC, GRAD_SPEC, GRAD_SPEC, GRAD_OUT_SPEC),
                         check_vma=False)
```

```python
import functools
import math

import jax
import jax.numpy as jnp
from jax import lax
from jax.experimental import pallas as pl
from jax.experimental.pallas import tpu as pltpu
from jax.sharding import PartitionSpec as P

ROW_SPEC = P(("dp", "cp", "tp"), None)
HEAD_SPEC = P(None, "tp", None)
OUT_W_SPEC = P("tp", None, None)
GRAD_SPEC = P(("dp", "cp"), None, "tp", None)
GRAD_OUT_SPEC = P(("dp", "cp"), "tp", None, None)
F32 = jnp.float32
BF16 = jnp.bfloat16
NT = (((1,), (1,)), ((), ()))
TN = (((0,), (0,)), ((), ()))
VMEM = pl.BlockSpec(memory_space=pltpu.VMEM)
ANY = pl.BlockSpec(memory_space=pl.ANY)
VMEM_LIMIT = 64 * 1024 * 1024
N_COPIES = 22


def dot(a, b):
    return jnp.dot(a, b, preferred_element_type=F32)


def dot_nt(a, b):
    return lax.dot_general(a, b, NT, preferred_element_type=F32)


def dot_tn(a, b):
    return lax.dot_general(a, b, TN, preferred_element_type=F32)


def far_units(rank, half, shards):
    units = []
    for d in range(1, shards):
        early = (rank + shards - d) // shards
        slot = early * half + (1 - early) * (1 - half)
        units += [(slot, 2 * d + half, early), (1 - half, 2 * d + slot, 0)]
    return units


def diag_mask(size):
    return lax.broadcasted_iota(jnp.int32, (size, size), 1) >= lax.broadcasted_iota(jnp.int32, (size, size), 0)


def pick(first, pair):
    if isinstance(first, int):
        return pair[1 - first]
    return jnp.where(first == 1, pair[0], pair[1])


def add_to(pair, first, value):
    if isinstance(first, int):
        pair[1 - first] = pair[1 - first] + value
    else:
        pair[0] = pair[0] + jnp.where(first == 1, value, 0.0)
        pair[1] = pair[1] + jnp.where(first == 1, 0.0, value)


def transpose_bf16(x):
    return x.astype(F32).T.astype(BF16)


def kernel(shards, n_heads, hd, c_scale, scale,
           x_hbm, dy_hbm, wq_hbm, wk_hbm, wv_hbm, wo_hbm,
           y_ref, dx_ref, gq_ref, gk_ref, gv_ref, go_ref,
           x_s, xp, dy_s, dyp, wq, wk, wv, wo, wqp, wkp, wvp, wop,
           q_s, do_s, o_s, og, dq_s, dqg, kvt, k_s, v_s, acc, m_s, l_s, s_s, dkv, rcv, dkvb, dkvg,
           send, recv, local):
    rank = lax.axis_index("cp")
    half = lax.axis_index("tp")
    core = rank % 2
    cols = q_s.shape[-1]
    hw = n_heads * hd
    groups = cols // 8
    peer = {"tp": 1 - half}
    partner = {"cp": rank + 1 - 2 * core}

    def at_cp(i):
        return {"cp": i % shards}

    def copy(i, src, dst, device):
        return pltpu.make_async_remote_copy(src_ref=src, dst_ref=dst, send_sem=send.at[i], recv_sem=recv.at[i],
                                            device_id=device, device_id_type=pl.DeviceIdType.MESH)

    loads = [pltpu.make_async_copy(src, dst, local.at[i]) for i, (src, dst) in enumerate(
        [(x_hbm, x_s), (wk_hbm, wk), (wv_hbm, wv), (wq_hbm, wq), (wo_hbm, wo), (dy_hbm, dy_s)])]
    for c in loads:
        c.start()
    barrier = pltpu.get_barrier_semaphore()
    pl.semaphore_signal(barrier, inc=1, device_id=peer, device_id_type=pl.DeviceIdType.MESH)
    for d in range(1, shards):
        pl.semaphore_signal(barrier, inc=1, device_id=at_cp(rank + d), device_id_type=pl.DeviceIdType.MESH)
    pl.semaphore_wait(barrier, shards)

    c_x = copy(0, x_hbm, xp, peer)
    c_dy = copy(1, dy_hbm, dyp, peer)
    c_w = [copy(2 + i, src.at[core], dst.at[core], peer)
           for i, (src, dst) in enumerate([(wo_hbm, wop), (wq_hbm, wqp), (wk_hbm, wkp), (wv_hbm, wvp)])]
    c_relay = [copy(6 + i, dst.at[core], dst.at[core], partner) for i, dst in enumerate([wop, wqp, wkp, wvp])]
    c_x.start()
    c_dy.start()
    for c in c_w:
        c.start()

    def flat(ref):
        return ref[...].reshape(ref.shape[0] * ref.shape[1], ref.shape[2])

    def send_kv(slot):
        cs = [copy(10 + 3 * slot + d - 1, kvt.at[slot], kvt.at[2 * d + slot], at_cp(rank + d)) for d in range(1, shards)]
        for c in cs:
            c.start()
        return cs

    def keys_ready(tile):
        k_s[tile] = transpose_bf16(kvt[tile, :hd, :])
        v_s[tile] = transpose_bf16(kvt[tile, hd:, :])

    for c in loads[:3]:
        c.wait()
    kvt[0, :hd, :] = dot_nt(flat(wk), x_s[...]).astype(BF16)
    kvt[0, hd:, :] = dot_nt(flat(wv), x_s[...]).astype(BF16)
    c_kv = send_kv(0)
    loads[3].wait()
    q_s[0] = dot_nt(flat(wq), x_s[...]).astype(BF16).reshape(n_heads, hd, cols)
    loads[4].wait()
    loads[5].wait()
    do_s[0] = dot_nt(flat(wo), dy_s[...]).astype(BF16).reshape(n_heads, hd, cols)
    keys_ready(0)
    c_x.wait_recv()
    kvt[1, :hd, :] = dot_nt(flat(wk), xp[...]).astype(BF16)
    kvt[1, hd:, :] = dot_nt(flat(wv), xp[...]).astype(BF16)
    c_kv += send_kv(1)
    q_s[1] = dot_nt(flat(wq), xp[...]).astype(BF16).reshape(n_heads, hd, cols)
    keys_ready(1)

    near = [(half, half, 1, True), (1 - half, half, 0, False), (1 - half, 1 - half, 0, True)]
    far = [u + (False,) for u in far_units(rank, half, shards)]
    slots = (half, 1 - half)

    def forward(units, h, is_near):
        maxes = [None, None]
        for u, (qi, kt, first, diag) in enumerate(units):
            s = dot(k_s[kt], q_s[qi, h])
            if diag:
                s = jnp.where(diag_mask(cols), s, -jnp.inf)
            s_s[u] = s
            mx = jnp.max(s.reshape(groups, 8, cols), axis=0)
            for g in (0, 1):
                if isinstance(first, int):
                    if first == g:
                        continue
                    val = mx
                else:
                    val = jnp.where(first == 1 - g, mx, -jnp.inf)
                maxes[g] = val if maxes[g] is None else jnp.maximum(maxes[g], val)
        m = [jnp.max(v, axis=0, keepdims=True) * c_scale for v in maxes]
        if is_near:
            l = [jnp.zeros((8, cols), F32), jnp.zeros((8, cols), F32)]
            o = [jnp.zeros((hd, cols), F32), jnp.zeros((hd, cols), F32)]
        else:
            old = [m_s[slots[g], h] for g in (0, 1)]
            m = [jnp.maximum(a, b) for a, b in zip(m, old)]
            fix = [jnp.exp2(a - b) for a, b in zip(old, m)]
            l = [l_s[slots[g], h] * fix[g] for g in (0, 1)]
            o = [acc[slots[g], h] * fix[g] for g in (0, 1)]
        for u, (qi, kt, first, diag) in enumerate(units):
            p = jnp.exp2(s_s[u] * c_scale - pick(first, m))
            add_to(l, first, jnp.sum(p.reshape(groups, 8, cols), axis=0))
            add_to(o, first, dot(kvt[kt, hd:, :], p.astype(BF16)))
        for g in (0, 1):
            if is_near:
                m_s[slots[g], h] = m[g]
                l_s[slots[g], h] = l[g]
                acc[slots[g], h] = o[g]
            else:
                l_row = jnp.sum(l[g], axis=0, keepdims=True)
                o_s[slots[g], h] = (o[g] / l_row).astype(BF16)
                m_s[slots[g], h] = m[g] + jnp.log2(l_row)

    def near_fwd(h, _):
        forward(near, h, True)
        return 0

    def far_fwd(h, _):
        forward(far, h, False)
        copy(20, o_s.at[1, h], og.at[h], peer).start()
        return 0

    lax.fori_loop(0, n_heads, near_fwd, 0)
    for i, c in enumerate(c_kv):
        c.wait_recv()
    for tile in range(2, 2 * shards):
        keys_ready(tile)
    lax.fori_loop(0, n_heads, far_fwd, 0)
    for c in c_w:
        c.wait_recv()
    for c in c_relay:
        c.start()
    c_dy.wait_recv()
    do_s[1] = dot_nt(flat(wo), dyp[...]).astype(BF16).reshape(n_heads, hd, cols)
    dkv[...] = jnp.zeros_like(dkv)

    def backward(units, h):
        delta = [jnp.sum(do_s[s, h].astype(F32) * o_s[s, h].astype(F32), axis=0, keepdims=True) for s in slots]
        lse = [m_s[s, h] for s in slots]
        dq = [jnp.zeros((hd, cols), F32), jnp.zeros((hd, cols), F32)]
        for qi, kt, first, diag in units:
            q, do = q_s[qi, h], do_s[qi, h]
            p = jnp.exp2(dot(k_s[kt], q) * c_scale - pick(first, lse))
            if diag:
                p = jnp.where(diag_mask(cols), p, 0.0)
            ds = (p * (dot(v_s[kt], do) - pick(first, delta))).astype(BF16)
            dkv[kt, hd:, :] += dot_nt(do, p.astype(BF16))
            dkv[kt, :hd, :] += dot_nt(q, ds)
            add_to(dq, first, dot(kvt[kt, :hd, :], ds))
        return dq

    def far_bwd(h, _):
        dq = backward(far, h)
        for g in (0, 1):
            acc[slots[g], h] = dq[g]
        return 0

    def near_bwd(h, _):
        dq = backward(near, h)
        for g in (0, 1):
            dq_s[slots[g], h] = ((dq[g] + acc[slots[g], h]) * scale).astype(BF16)
        copy(21, dq_s.at[1, h], dqg.at[h], peer).start()
        return 0

    lax.fori_loop(0, n_heads, far_bwd, 0)
    c_dkv = [copy(16 + d - 1, dkv.at[pl.ds(2 * d, 2)], rcv.at[d - 1], at_cp(rank + shards - d)) for d in range(1, shards)]
    for c in c_dkv:
        c.start()
    lax.fori_loop(0, n_heads, near_bwd, 0)

    for c in c_relay:
        c.wait_recv()
    c_o = copy(20, o_s.at[1], og, peer)
    c_o.wait_recv()
    rows = 128
    for i in range(cols // rows):
        part = slice(i * rows, (i + 1) * rows)
        y = dot_tn(o_s[0, :, :, part].reshape(hw, rows), flat(wo)) + dot_tn(og[:, :, part].reshape(hw, rows), flat(wop))
        y_ref[part, :] = y.astype(BF16)
    for h in range(n_heads):
        go_ref[h] = (dot(o_s[0, h], dy_s[...]) + dot(o_s[1, h], dyp[...])).astype(BF16)
        gq_ref[h] = (dot(dq_s[0, h], x_s[...]) + dot(dq_s[1, h], xp[...])).astype(BF16)

    for c in c_dkv:
        c.wait_recv()
    for slot in (1, 0):
        total = dkv[slot] + rcv[0, slot] + rcv[1, slot] + rcv[2, slot]
        dkvb[slot, :hd, :] = (total[:hd, :] * scale).astype(BF16)
        dkvb[slot, hd:, :] = total[hd:, :].astype(BF16)
    c_last = copy(19, dkvb.at[1], dkvg, peer)
    c_last.start()
    gkv = dot(dkvb[0], x_s[...]) + dot(dkvb[1], xp[...])
    gk_ref[...] = gkv[:hd, :].astype(BF16)
    gv_ref[...] = gkv[hd:, :].astype(BF16)
    c_dq = copy(21, dq_s.at[1], dqg, peer)
    c_dq.wait_recv()
    c_last.wait_recv()
    for i in range(cols // rows):
        part = slice(i * rows, (i + 1) * rows)
        dx = dot_tn(dq_s[0, :, :, part].reshape(hw, rows), flat(wq)) + dot_tn(dqg[:, :, part].reshape(hw, rows), flat(wqp))
        dx += dot_tn(dkvb[0, :hd, part], flat(wk)) + dot_tn(dkvb[0, hd:, part], flat(wv))
        dx += dot_tn(dkvg[:hd, part], flat(wkp)) + dot_tn(dkvg[hd:, part], flat(wvp))
        dx_ref[part, :] = dx.astype(BF16)
    for c in [c_x, c_dy, c_o, c_dq, c_last] + c_w + c_relay + c_kv + c_dkv:
        c.wait_send()


def solution(mesh):
    shards = mesh.shape["cp"]

    def device_fn(x_own, w_query, w_key, w_value, w_out, dy_own):
        model, n_heads, hd = w_query.shape
        cols = x_own.shape[0]
        hw = n_heads * hd
        scale = hd ** -0.5
        wq = w_query.transpose(1, 2, 0).reshape(2, hw // 2, model)
        wk = w_key.transpose(1, 2, 0).reshape(2, hd // 2, model)
        wv = w_value.transpose(1, 2, 0).reshape(2, hd // 2, model)
        wo = w_out.reshape(2, hw // 2, model)
        per_head = (2, n_heads, hd, cols)
        b = lambda *s: pltpu.VMEM(s, BF16)
        f = lambda *s: pltpu.VMEM(s, F32)
        area = n_heads * 9 * cols * cols
        y, dx, gq, gk, gv, go = pl.pallas_call(
            functools.partial(kernel, shards, n_heads, hd, scale * math.log2(math.e), scale),
            out_shape=(jax.ShapeDtypeStruct((cols, model), BF16), jax.ShapeDtypeStruct((cols, model), BF16),
                       jax.ShapeDtypeStruct((n_heads, hd, model), BF16), jax.ShapeDtypeStruct((hd, model), BF16),
                       jax.ShapeDtypeStruct((hd, model), BF16), jax.ShapeDtypeStruct((n_heads, hd, model), BF16)),
            in_specs=[ANY] * 6,
            out_specs=(VMEM,) * 6,
            scratch_shapes=[b(cols, model)] * 4 + [b(2, hw // 2, model), b(2, hd // 2, model), b(2, hd // 2, model), b(2, hw // 2, model)] * 2
            + [b(*per_head), b(*per_head), b(*per_head), b(*per_head[1:]), b(*per_head), b(*per_head[1:]),
               b(2 * shards, 2 * hd, cols), b(2 * shards, cols, hd), b(2 * shards, cols, hd), f(*per_head),
               f(2, n_heads, 1, cols), f(2, n_heads, 8, cols), f(6, cols, cols), f(2 * shards, 2 * hd, cols),
               f(shards - 1, 2, 2 * hd, cols), b(2, 2 * hd, cols), b(2 * hd, cols),
               pltpu.SemaphoreType.DMA((N_COPIES,)), pltpu.SemaphoreType.DMA((N_COPIES,)), pltpu.SemaphoreType.DMA((6,))],
            compiler_params=pltpu.CompilerParams(vmem_limit_bytes=VMEM_LIMIT, collective_id=0, has_side_effects=True),
            cost_estimate=pl.CostEstimate(flops=area * 7 * 2 * hd, bytes_accessed=16 << 20, transcendentals=2 * area),
            name="attention",
        )(x_own, dy_own, wq, wk, wv, wo)
        back = lambda g, n: g.reshape(n, hd, model).transpose(2, 0, 1)[None]
        return y, dx, back(gq, n_heads), back(gk, 1), back(gv, 1), go[None]

    return jax.shard_map(device_fn, mesh=mesh,
                         in_specs=(ROW_SPEC, HEAD_SPEC, HEAD_SPEC, HEAD_SPEC, OUT_W_SPEC, ROW_SPEC),
                         out_specs=(ROW_SPEC, ROW_SPEC, GRAD_SPEC, GRAD_SPEC, GRAD_SPEC, GRAD_OUT_SPEC),
                         check_vma=False)
```

```python
import functools
import math

import jax
import jax.numpy as jnp
from jax import lax
from jax.experimental import pallas as pl
from jax.experimental.pallas import tpu as pltpu
from jax.sharding import PartitionSpec as P

ROW_SPEC = P(("dp", "cp", "tp"), None)
HEAD_SPEC = P(None, "tp", None)
OUT_W_SPEC = P("tp", None, None)
GRAD_SPEC = P(("dp", "cp"), None, "tp", None)
GRAD_OUT_SPEC = P(("dp", "cp"), "tp", None, None)
F32 = jnp.float32
BF16 = jnp.bfloat16
NT = (((1,), (1,)), ((), ()))
TN = (((0,), (0,)), ((), ()))
VMEM = pl.BlockSpec(memory_space=pltpu.VMEM)
ANY = pl.BlockSpec(memory_space=pl.ANY)
VMEM_LIMIT = 64 * 1024 * 1024
N_COPIES = 22


def dot(a, b):
    return jnp.dot(a, b, preferred_element_type=F32)


def dot_nt(a, b):
    return lax.dot_general(a, b, NT, preferred_element_type=F32)


def dot_tn(a, b):
    return lax.dot_general(a, b, TN, preferred_element_type=F32)


def far_units(rank, half, shards):
    units = []
    for d in range(1, shards):
        early = (rank + shards - d) // shards
        slot = early * half + (1 - early) * (1 - half)
        units += [(slot, 2 * d + half, early), (1 - half, 2 * d + slot, 0)]
    return units


def diag_mask(size):
    return lax.broadcasted_iota(jnp.int32, (size, size), 1) >= lax.broadcasted_iota(jnp.int32, (size, size), 0)


def pick(first, pair):
    if isinstance(first, int):
        return pair[1 - first]
    return jnp.where(first == 1, pair[0], pair[1])


def add_to(pair, first, value):
    if isinstance(first, int):
        pair[1 - first] = pair[1 - first] + value
    else:
        pair[0] = pair[0] + jnp.where(first == 1, value, 0.0)
        pair[1] = pair[1] + jnp.where(first == 1, 0.0, value)


def transpose_bf16(x):
    return x.astype(F32).T.astype(BF16)


def kernel(shards, n_heads, hd, c_scale, scale,
           x_hbm, dy_hbm, wq_hbm, wk_hbm, wv_hbm, wo_hbm,
           y_ref, dx_ref, gq_ref, gk_ref, gv_ref, go_ref,
           x_s, xp, dy_s, dyp, wq, wk, wv, wo, wqp, wkp, wvp, wop,
           q_s, do_s, o_s, og, dq_s, dqg, kvt, k_s, v_s, acc, m_s, l_s, d_s, max_s, s_s, pb, db, dkv, rcv, dkvb, dkvg,
           send, recv, local):
    rank = lax.axis_index("cp")
    half = lax.axis_index("tp")
    core = rank % 2
    cols = q_s.shape[-1]
    hw = n_heads * hd
    peer = {"tp": 1 - half}
    partner = {"cp": rank + 1 - 2 * core}

    def at_cp(i):
        return {"cp": i % shards}

    def copy(i, src, dst, device):
        return pltpu.make_async_remote_copy(src_ref=src, dst_ref=dst, send_sem=send.at[i], recv_sem=recv.at[i],
                                            device_id=device, device_id_type=pl.DeviceIdType.MESH)

    loads = [pltpu.make_async_copy(src, dst, local.at[i]) for i, (src, dst) in enumerate(
        [(x_hbm, x_s), (wk_hbm, wk), (wv_hbm, wv), (wq_hbm, wq), (wo_hbm, wo), (dy_hbm, dy_s)])]
    for c in loads:
        c.start()
    barrier = pltpu.get_barrier_semaphore()
    pl.semaphore_signal(barrier, inc=1, device_id=peer, device_id_type=pl.DeviceIdType.MESH)
    for d in range(1, shards):
        pl.semaphore_signal(barrier, inc=1, device_id=at_cp(rank + d), device_id_type=pl.DeviceIdType.MESH)
    pl.semaphore_wait(barrier, shards)

    c_x = copy(0, x_hbm, xp, peer)
    c_dy = copy(1, dy_hbm, dyp, peer)
    c_w = [copy(2 + i, src.at[core], dst.at[core], peer)
           for i, (src, dst) in enumerate([(wo_hbm, wop), (wq_hbm, wqp), (wk_hbm, wkp), (wv_hbm, wvp)])]
    c_relay = [copy(6 + i, dst.at[core], dst.at[core], partner) for i, dst in enumerate([wop, wqp, wkp, wvp])]
    c_x.start()
    c_dy.start()
    for c in c_w:
        c.start()

    def flat(ref):
        return ref[...].reshape(ref.shape[0] * ref.shape[1], ref.shape[2])

    def send_kv(slot):
        cs = [copy(10 + 3 * slot + d - 1, kvt.at[slot], kvt.at[2 * d + slot], at_cp(rank + d)) for d in range(1, shards)]
        for c in cs:
            c.start()
        return cs

    def keys_ready(tile):
        k_s[tile] = transpose_bf16(kvt[tile, :hd, :])
        v_s[tile] = transpose_bf16(kvt[tile, hd:, :])

    for c in loads[:3]:
        c.wait()
    kvt[0, :hd, :] = dot_nt(flat(wk), x_s[...]).astype(BF16)
    kvt[0, hd:, :] = dot_nt(flat(wv), x_s[...]).astype(BF16)
    c_kv = send_kv(0)
    loads[3].wait()
    q_s[0] = dot_nt(flat(wq), x_s[...]).astype(BF16).reshape(n_heads, hd, cols)
    loads[4].wait()
    loads[5].wait()
    do_s[0] = dot_nt(flat(wo), dy_s[...]).astype(BF16).reshape(n_heads, hd, cols)
    keys_ready(0)
    c_x.wait_recv()
    kvt[1, :hd, :] = dot_nt(flat(wk), xp[...]).astype(BF16)
    kvt[1, hd:, :] = dot_nt(flat(wv), xp[...]).astype(BF16)
    c_kv += send_kv(1)
    q_s[1] = dot_nt(flat(wq), xp[...]).astype(BF16).reshape(n_heads, hd, cols)
    keys_ready(1)

    near = [(half, half, 1, True), (1 - half, half, 0, False), (1 - half, 1 - half, 0, True)]
    far = [u + (False,) for u in far_units(rank, half, shards)]
    slots = (half, 1 - half)
    part = cols // 2
    triangle = diag_mask(part)

    def spans(diag, c):
        return slice(c * part, (c + 1) * part), slice(c * part, cols) if diag else slice(0, cols)

    def masked(x, diag, fill):
        if not diag:
            return x
        left = jnp.where(triangle, x[:, :part], fill)
        return left if x.shape[1] == part else jnp.concatenate([left, x[:, part:]], axis=1)

    def widen(x, fill):
        if x.shape[1] == cols:
            return x
        return jnp.concatenate([jnp.full((x.shape[0], cols - x.shape[1]), fill, x.dtype), x], axis=1)

    def interleave(first_list, second_list):
        i = j = 0
        while i < len(first_list) or j < len(second_list):
            if j >= len(second_list) or (i < len(first_list) and i * len(second_list) <= j * len(first_list)):
                first_list[i]()
                i += 1
            else:
                second_list[j]()
                j += 1

    def score_steps(units, base, h, maxes):
        def step(u, c):
            qi, kt, first, diag = units[u]
            r, q = spans(diag, c)
            s = masked(dot(k_s[kt, r], q_s[qi, h, :, q]), diag, -jnp.inf)
            s_s[base + u, r, q] = s
            mx = widen(jnp.max(s.reshape(part // 8, 8, s.shape[1]), axis=0), -jnp.inf)
            maxes[u] = mx if c == 0 else jnp.maximum(maxes[u], mx)
        return [functools.partial(step, u, c) for u in range(len(units)) for c in (0, 1)]

    def score_max(units, maxes):
        for g in (0, 1):
            best = None
            for u, (_, _, first, _) in enumerate(units):
                if isinstance(first, int):
                    if first == g:
                        continue
                    val = maxes[u]
                else:
                    val = jnp.where(first == 1 - g, maxes[u], -jnp.inf)
                best = val if best is None else jnp.maximum(best, val)
            max_s[g] = jnp.max(best, axis=0, keepdims=True) * c_scale

    def attend_steps(units, base, h, is_near):
        m = [max_s[0], max_s[1]]
        if is_near:
            l = [jnp.zeros((8, cols), F32), jnp.zeros((8, cols), F32)]
            o = [jnp.zeros((hd, cols), F32), jnp.zeros((hd, cols), F32)]
        else:
            old = [m_s[slots[g], h] for g in (0, 1)]
            m = [jnp.maximum(x, y) for x, y in zip(m, old)]
            fix = [jnp.exp2(x - y) for x, y in zip(old, m)]
            l = [l_s[slots[g], h] * fix[g] for g in (0, 1)]
            o = [acc[slots[g], h] * fix[g] for g in (0, 1)]
        sums = {}

        def step(u, c):
            qi, kt, first, diag = units[u]
            r, q = spans(diag, c)
            p = jnp.exp2(s_s[base + u, r, q] * c_scale - pick(first, m)[:, q])
            l_u = widen(jnp.sum(p.reshape(part // 8, 8, p.shape[1]), axis=0), 0.0)
            o_u = widen(dot(kvt[kt, hd:, r], p.astype(BF16)), 0.0)
            if c == 0:
                sums[u] = (l_u, o_u)
            else:
                add_to(l, first, sums[u][0] + l_u)
                add_to(o, first, sums[u][1] + o_u)

        def finish():
            for g in (0, 1):
                if is_near:
                    m_s[slots[g], h] = m[g]
                    l_s[slots[g], h] = l[g]
                    acc[slots[g], h] = o[g]
                else:
                    l_row = jnp.sum(l[g], axis=0, keepdims=True)
                    o_s[slots[g], h] = (o[g] / l_row).astype(BF16)
                    m_s[slots[g], h] = m[g] + jnp.log2(l_row)

        return [functools.partial(step, u, c) for u in range(len(units)) for c in (0, 1)], finish

    def forward(units, base, h, is_near, nxt):
        steps, finish = attend_steps(units, base, h, is_near)
        maxes = {}
        following = score_steps(*nxt, maxes) if nxt else []
        interleave(steps, following)
        finish()
        if nxt:
            score_max(nxt[0], maxes)

    def send_o(h):
        copy(20, o_s.at[1, h], og.at[h], peer).start()

    def near_fwd(h, _):
        forward(near, 6, h, True, (near, 6, h + 1))
        return 0

    def far_fwd(h, _):
        forward(far, 0, h, False, (far, 0, h + 1))
        send_o(h)
        return 0

    last = n_heads - 1
    maxes = {}
    for step in score_steps(near, 6, 0, maxes):
        step()
    score_max(near, maxes)
    lax.fori_loop(0, last, near_fwd, 0)
    for i, c in enumerate(c_kv):
        c.wait_recv()
    for tile in range(2, 2 * shards):
        keys_ready(tile)
    forward(near, 6, last, True, (far, 0, 0))
    lax.fori_loop(0, last, far_fwd, 0)
    for c in c_w:
        c.wait_recv()
    for c in c_relay:
        c.start()
    c_dy.wait_recv()
    do_s[1] = dot_nt(flat(wo), dyp[...]).astype(BF16).reshape(n_heads, hd, cols)
    forward(far, 0, last, False, None)
    send_o(last)
    dkv[...] = jnp.zeros_like(dkv)

    def row_dots(h, _):
        for s in (0, 1):
            d_s[s, h] = jnp.sum(do_s[s, h].astype(F32) * o_s[s, h].astype(F32), axis=0, keepdims=True)
        return 0

    lax.fori_loop(0, n_heads, row_dots, 0)

    def prob_steps(units, bufs, h, which):
        def step(u, c):
            qi, kt, first, diag = units[u]
            r, q = spans(diag, c)
            buf = bufs[u % len(bufs)]
            p = jnp.exp2(dot(k_s[kt, r], q_s[qi, h, :, q]) * c_scale - m_s[qi, h, :, q])
            p = masked(p, diag, 0.0)
            pb[buf, r, q] = p.astype(BF16)
            db[buf, r, q] = (p * (dot(v_s[kt, r], do_s[qi, h, :, q]) - d_s[qi, h, :, q])).astype(BF16)
        return [functools.partial(step, u, c) for u in which for c in (0, 1)]

    def grad_steps(units, bufs, h, u, dq):
        qi, kt, first, diag = units[u]
        buf = bufs[u % len(bufs)]
        kept = {}

        def over_queries(name, src, lhs, rows, c):
            q = slice(c * part, (c + 1) * part)
            keys = slice(0, part) if diag and c == 0 else slice(0, cols)
            val = dot_nt(lhs[qi, h, :, q], src[buf, keys, q])
            if c == 0 and not diag:
                kept[name] = val
            elif diag:
                dkv[kt, rows, keys] += val
            else:
                dkv[kt, rows, :] += kept[name] + val

        def over_keys(c):
            r, q = spans(diag, c)
            val = widen(dot(kvt[kt, :hd, r], db[buf, r, q]), 0.0)
            if c == 0:
                kept["q"] = val
            else:
                add_to(dq, first, kept["q"] + val)

        return ([functools.partial(over_queries, "v", pb, do_s, slice(hd, 2 * hd), c) for c in (0, 1)]
                + [functools.partial(over_queries, "k", db, q_s, slice(0, hd), c) for c in (0, 1)]
                + [functools.partial(over_keys, c) for c in (0, 1)])

    def backward(units, bufs, h, nxt):
        dq = [jnp.zeros((hd, cols), F32), jnp.zeros((hd, cols), F32)]
        for u in range(len(units)):
            if u + 1 < len(units):
                ahead = prob_steps(units, bufs, h, [u + 1])
            else:
                ahead = prob_steps(*nxt, [0]) if nxt else []
            interleave(ahead, grad_steps(units, bufs, h, u, dq))
        return dq

    near_bufs, far_bufs = (0, 1, 2), (3, 4)

    def far_bwd(h, nxt):
        dq = backward(far, far_bufs, h, nxt)
        for g in (0, 1):
            acc[slots[g], h] = dq[g]

    def near_bwd(h, nxt):
        dq = backward(near, near_bufs, h, nxt)
        for g in (0, 1):
            dq_s[slots[g], h] = ((dq[g] + acc[slots[g], h]) * scale).astype(BF16)
        copy(21, dq_s.at[1, h], dqg.at[h], peer).start()

    def far_loop(h, _):
        far_bwd(h, (far, far_bufs, h + 1))
        return 0

    def near_loop(h, _):
        near_bwd(h, (near, near_bufs, h + 1))
        return 0

    for step in prob_steps(far, far_bufs, 0, [0]):
        step()
    lax.fori_loop(0, last, far_loop, 0)
    far_bwd(last, (near, near_bufs, 0))
    c_dkv = [copy(16 + d - 1, dkv.at[pl.ds(2 * d, 2)], rcv.at[d - 1], at_cp(rank + shards - d)) for d in range(1, shards)]
    for c in c_dkv:
        c.start()
    lax.fori_loop(0, last, near_loop, 0)
    near_bwd(last, None)

    for c in c_relay:
        c.wait_recv()
    c_o = copy(20, o_s.at[1], og, peer)
    c_o.wait_recv()
    rows = 128
    for i in range(cols // rows):
        blk = slice(i * rows, (i + 1) * rows)
        y = dot_tn(o_s[0, :, :, blk].reshape(hw, rows), flat(wo)) + dot_tn(og[:, :, blk].reshape(hw, rows), flat(wop))
        y_ref[blk, :] = y.astype(BF16)
    for h in range(n_heads):
        go_ref[h] = (dot(o_s[0, h], dy_s[...]) + dot(o_s[1, h], dyp[...])).astype(BF16)
        gq_ref[h] = (dot(dq_s[0, h], x_s[...]) + dot(dq_s[1, h], xp[...])).astype(BF16)

    for c in c_dkv:
        c.wait_recv()
    for slot in (1, 0):
        total = dkv[slot] + rcv[0, slot] + rcv[1, slot] + rcv[2, slot]
        dkvb[slot, :hd, :] = (total[:hd, :] * scale).astype(BF16)
        dkvb[slot, hd:, :] = total[hd:, :].astype(BF16)
    c_last = copy(19, dkvb.at[1], dkvg, peer)
    c_last.start()
    gkv = dot(dkvb[0], x_s[...]) + dot(dkvb[1], xp[...])
    gk_ref[...] = gkv[:hd, :].astype(BF16)
    gv_ref[...] = gkv[hd:, :].astype(BF16)
    c_dq = copy(21, dq_s.at[1], dqg, peer)
    c_dq.wait_recv()
    c_last.wait_recv()
    for i in range(cols // rows):
        blk = slice(i * rows, (i + 1) * rows)
        dx = dot_tn(dq_s[0, :, :, blk].reshape(hw, rows), flat(wq)) + dot_tn(dqg[:, :, blk].reshape(hw, rows), flat(wqp))
        dx += dot_tn(dkvb[0, :hd, blk], flat(wk)) + dot_tn(dkvb[0, hd:, blk], flat(wv))
        dx += dot_tn(dkvg[:hd, blk], flat(wkp)) + dot_tn(dkvg[hd:, blk], flat(wvp))
        dx_ref[blk, :] = dx.astype(BF16)
    for c in [c_x, c_dy, c_o, c_dq, c_last] + c_w + c_relay + c_kv + c_dkv:
        c.wait_send()


def solution(mesh):
    shards = mesh.shape["cp"]

    def device_fn(x_own, w_query, w_key, w_value, w_out, dy_own):
        model, n_heads, hd = w_query.shape
        cols = x_own.shape[0]
        hw = n_heads * hd
        scale = hd ** -0.5
        wq = w_query.transpose(1, 2, 0).reshape(2, hw // 2, model)
        wk = w_key.transpose(1, 2, 0).reshape(2, hd // 2, model)
        wv = w_value.transpose(1, 2, 0).reshape(2, hd // 2, model)
        wo = w_out.reshape(2, hw // 2, model)
        per_head = (2, n_heads, hd, cols)
        b = lambda *s: pltpu.VMEM(s, BF16)
        f = lambda *s: pltpu.VMEM(s, F32)
        area = n_heads * 9 * cols * cols
        y, dx, gq, gk, gv, go = pl.pallas_call(
            functools.partial(kernel, shards, n_heads, hd, scale * math.log2(math.e), scale),
            out_shape=(jax.ShapeDtypeStruct((cols, model), BF16), jax.ShapeDtypeStruct((cols, model), BF16),
                       jax.ShapeDtypeStruct((n_heads, hd, model), BF16), jax.ShapeDtypeStruct((hd, model), BF16),
                       jax.ShapeDtypeStruct((hd, model), BF16), jax.ShapeDtypeStruct((n_heads, hd, model), BF16)),
            in_specs=[ANY] * 6,
            out_specs=(VMEM,) * 6,
            scratch_shapes=[b(cols, model)] * 4 + [b(2, hw // 2, model), b(2, hd // 2, model), b(2, hd // 2, model), b(2, hw // 2, model)] * 2
            + [b(*per_head), b(*per_head), b(*per_head), b(*per_head[1:]), b(*per_head), b(*per_head[1:]),
               b(2 * shards, 2 * hd, cols), b(2 * shards, cols, hd), b(2 * shards, cols, hd), f(*per_head),
               f(2, n_heads, 1, cols), f(2, n_heads, 8, cols), f(2, n_heads, 1, cols), f(2, 1, cols),
               f(9, cols, cols), b(5, cols, cols), b(5, cols, cols), f(2 * shards, 2 * hd, cols),
               f(shards - 1, 2, 2 * hd, cols), b(2, 2 * hd, cols), b(2 * hd, cols),
               pltpu.SemaphoreType.DMA((N_COPIES,)), pltpu.SemaphoreType.DMA((N_COPIES,)), pltpu.SemaphoreType.DMA((6,))],
            compiler_params=pltpu.CompilerParams(vmem_limit_bytes=VMEM_LIMIT, collective_id=0, has_side_effects=True),
            cost_estimate=pl.CostEstimate(flops=area * 7 * 2 * hd, bytes_accessed=16 << 20, transcendentals=2 * area),
            name="attention",
        )(x_own, dy_own, wq, wk, wv, wo)
        back = lambda g, n: g.reshape(n, hd, model).transpose(2, 0, 1)[None]
        return y, dx, back(gq, n_heads), back(gk, 1), back(gv, 1), go[None]

    return jax.shard_map(device_fn, mesh=mesh,
                         in_specs=(ROW_SPEC, HEAD_SPEC, HEAD_SPEC, HEAD_SPEC, OUT_W_SPEC, ROW_SPEC),
                         out_specs=(ROW_SPEC, ROW_SPEC, GRAD_SPEC, GRAD_SPEC, GRAD_SPEC, GRAD_OUT_SPEC),
                         check_vma=False)
```

```python
import functools
import math

import jax
import jax.numpy as jnp
from jax import lax
from jax.experimental import pallas as pl
from jax.experimental.pallas import tpu as pltpu
from jax.sharding import PartitionSpec as P

ROW_SPEC = P(("dp", "cp", "tp"), None)
HEAD_SPEC = P(None, "tp", None)
OUT_W_SPEC = P("tp", None, None)
GRAD_SPEC = P(("dp", "cp"), None, "tp", None)
GRAD_OUT_SPEC = P(("dp", "cp"), "tp", None, None)
F32 = jnp.float32
BF16 = jnp.bfloat16
NT = (((1,), (1,)), ((), ()))
TN = (((0,), (0,)), ((), ()))
VMEM = pl.BlockSpec(memory_space=pltpu.VMEM)
ANY = pl.BlockSpec(memory_space=pl.ANY)
VMEM_LIMIT = 64 * 1024 * 1024
N_COPIES = 22


def dot(a, b):
    return jnp.dot(a, b, preferred_element_type=F32)


def dot_nt(a, b):
    return lax.dot_general(a, b, NT, preferred_element_type=F32)


def dot_tn(a, b):
    return lax.dot_general(a, b, TN, preferred_element_type=F32)


def shard_units(rank, half, d, shards):
    early = (rank + shards - d) // shards
    slot = early * half + (1 - early) * (1 - half)
    return [(slot, 2 * d + half, early, False), (1 - half, 2 * d + slot, 0, False)]


def diag_mask(size):
    return lax.broadcasted_iota(jnp.int32, (size, size), 1) >= lax.broadcasted_iota(jnp.int32, (size, size), 0)


def pick(first, pair):
    if isinstance(first, int):
        return pair[1 - first]
    return jnp.where(first == 1, pair[0], pair[1])


def add_to(pair, first, value):
    if isinstance(first, int):
        pair[1 - first] = pair[1 - first] + value
    else:
        pair[0] = pair[0] + jnp.where(first == 1, value, 0.0)
        pair[1] = pair[1] + jnp.where(first == 1, 0.0, value)


def transpose_bf16(x):
    return x.astype(F32).T.astype(BF16)


def kernel(shards, n_heads, hd, c_scale, scale,
           x_hbm, dy_hbm, wq_hbm, wk_hbm, wv_hbm, wo_hbm,
           y_ref, dx_ref, gq_ref, gk_ref, gv_ref, go_ref,
           x_s, xp, dy_s, dyp, w_own, w_peer,
           q_s, do_s, o_s, og, dq_s, dqg, kvt, k_s, v_s, acc, m_s, l_s, d_s, max_s, s_s, pb, db, dkv, rcv, dkvb, dkvg,
           y_s, dx_s, dx_f, gq_s, gkv_s, go_s, send, recv, local):
    rank = lax.axis_index("cp")
    half = lax.axis_index("tp")
    core = rank % 2
    cols = q_s.shape[-1]
    hw = n_heads * hd
    peer = {"tp": 1 - half}
    partner = {"cp": rank + 1 - 2 * core}

    d_near = shards - 1 - 2 * core
    d_far = (2, 1 + 2 * core)

    def at_cp(i):
        return {"cp": i % shards}

    def copy(i, src, dst, device):
        return pltpu.make_async_remote_copy(src_ref=src, dst_ref=dst, send_sem=send.at[i], recv_sem=recv.at[i],
                                            device_id=device, device_id_type=pl.DeviceIdType.MESH)

    n_o, n_k = hw // shards, hd // shards
    w_rows = {"o": (0, n_o), "q": (n_o, n_o), "k": (2 * n_o, n_k), "v": (2 * n_o + n_k, n_k)}

    def load(i, src, name):
        start, size = w_rows[name]
        return pltpu.make_async_copy(src, w_own.at[:, pl.ds(start, size), :], local.at[i])

    def weight(ref, name):
        start, size = w_rows[name]
        return ref[:, start:start + size, :].reshape(shards * size, ref.shape[2])

    loads = [pltpu.make_async_copy(x_hbm, x_s, local.at[0]), load(1, wk_hbm, "k"), load(2, wv_hbm, "v"), load(3, wq_hbm, "q"),
             load(4, wo_hbm, "o"), pltpu.make_async_copy(dy_hbm, dy_s, local.at[5])]
    for c in loads:
        c.start()
    barrier = pltpu.get_barrier_semaphore()
    pl.semaphore_signal(barrier, inc=1, device_id=peer, device_id_type=pl.DeviceIdType.MESH)
    for d in range(1, shards):
        pl.semaphore_signal(barrier, inc=1, device_id=at_cp(rank + d), device_id_type=pl.DeviceIdType.MESH)
    pl.semaphore_wait(barrier, shards)

    across = (rank + 2) % shards
    c_x = copy(0, x_hbm, xp, peer)
    c_dy = copy(1, dy_hbm, dyp, peer)
    c_w = copy(2, w_own.at[rank], w_peer.at[rank], peer)
    c_relay = [copy(3, w_peer.at[rank], w_peer.at[rank], partner), copy(4, w_peer.at[rank], w_peer.at[rank], at_cp(across)),
               copy(5, w_peer.at[across], w_peer.at[across], partner)]
    c_x.start()
    c_dy.start()

    def send_kv(slot):
        ahead = (2, shards - 1 - 2 * core, 1 + 2 * core)
        cs = [copy(10 + 3 * slot + i, kvt.at[slot], kvt.at[2 * d + slot], at_cp(rank + d)) for i, d in enumerate(ahead)]
        for c in cs:
            c.start()
        return cs

    def keys_ready(tile):
        k_s[tile] = transpose_bf16(kvt[tile, :hd, :])
        v_s[tile] = transpose_bf16(kvt[tile, hd:, :])

    for c in loads[:3]:
        c.wait()
    kvt[0, :hd, :] = dot_nt(weight(w_own, "k"), x_s[...]).astype(BF16)
    kvt[0, hd:, :] = dot_nt(weight(w_own, "v"), x_s[...]).astype(BF16)
    c_kv = send_kv(0)
    loads[3].wait()
    q_s[0] = dot_nt(weight(w_own, "q"), x_s[...]).astype(BF16).reshape(n_heads, hd, cols)
    loads[4].wait()
    c_w.start()
    loads[5].wait()
    do_s[0] = dot_nt(weight(w_own, "o"), dy_s[...]).astype(BF16).reshape(n_heads, hd, cols)
    keys_ready(0)
    c_x.wait_recv()
    kvt[1, :hd, :] = dot_nt(weight(w_own, "k"), xp[...]).astype(BF16)
    kvt[1, hd:, :] = dot_nt(weight(w_own, "v"), xp[...]).astype(BF16)
    c_kv += send_kv(1)
    q_s[1] = dot_nt(weight(w_own, "q"), xp[...]).astype(BF16).reshape(n_heads, hd, cols)
    keys_ready(1)

    near = ([(half, half, 1, True), (1 - half, half, 0, False), (1 - half, 1 - half, 0, True)]
            + shard_units(rank, half, d_near, shards))
    far = shard_units(rank, half, d_far[0], shards) + shard_units(rank, half, d_far[1], shards)
    slots = (half, 1 - half)
    part = cols // 2
    triangle = diag_mask(part)

    def spans(diag, c):
        return slice(c * part, (c + 1) * part), slice(c * part, cols) if diag else slice(0, cols)

    def masked(x, diag, fill):
        if not diag:
            return x
        left = jnp.where(triangle, x[:, :part], fill)
        return left if x.shape[1] == part else jnp.concatenate([left, x[:, part:]], axis=1)

    def widen(x, fill):
        if x.shape[1] == cols:
            return x
        return jnp.concatenate([jnp.full((x.shape[0], cols - x.shape[1]), fill, x.dtype), x], axis=1)

    def interleave(first_list, second_list):
        i = j = 0
        while i < len(first_list) or j < len(second_list):
            if j >= len(second_list) or (i < len(first_list) and i * len(second_list) <= j * len(first_list)):
                first_list[i]()
                i += 1
            else:
                second_list[j]()
                j += 1

    def score_steps(units, base, h, maxes):
        def step(u, c):
            qi, kt, first, diag = units[u]
            r, q = spans(diag, c)
            s = masked(dot(k_s[kt, r], q_s[qi, h, :, q]), diag, -jnp.inf)
            s_s[base + u, r, q] = s
            mx = widen(jnp.max(s.reshape(part // 8, 8, s.shape[1]), axis=0), -jnp.inf)
            maxes[u] = mx if c == 0 else jnp.maximum(maxes[u], mx)
        return [functools.partial(step, u, c) for u in range(len(units)) for c in (0, 1)]

    def score_max(units, maxes):
        for g in (0, 1):
            best = None
            for u, (_, _, first, _) in enumerate(units):
                if isinstance(first, int):
                    if first == g:
                        continue
                    val = maxes[u]
                else:
                    val = jnp.where(first == 1 - g, maxes[u], -jnp.inf)
                best = val if best is None else jnp.maximum(best, val)
            max_s[g] = jnp.max(best, axis=0, keepdims=True) * c_scale

    def attend_steps(units, base, h, is_near):
        m = [max_s[0], max_s[1]]
        if is_near:
            l = [jnp.zeros((8, cols), F32), jnp.zeros((8, cols), F32)]
            o = [jnp.zeros((hd, cols), F32), jnp.zeros((hd, cols), F32)]
        else:
            old = [m_s[slots[g], h] for g in (0, 1)]
            m = [jnp.maximum(x, y) for x, y in zip(m, old)]
            fix = [jnp.exp2(x - y) for x, y in zip(old, m)]
            l = [l_s[slots[g], h] * fix[g] for g in (0, 1)]
            o = [acc[slots[g], h] * fix[g] for g in (0, 1)]
        sums = {}

        def step(u, c):
            qi, kt, first, diag = units[u]
            r, q = spans(diag, c)
            p = jnp.exp2(s_s[base + u, r, q] * c_scale - pick(first, m)[:, q])
            l_u = widen(jnp.sum(p.reshape(part // 8, 8, p.shape[1]), axis=0), 0.0)
            o_u = widen(dot(kvt[kt, hd:, r], p.astype(BF16)), 0.0)
            if c == 0:
                sums[u] = (l_u, o_u)
            else:
                add_to(l, first, sums[u][0] + l_u)
                add_to(o, first, sums[u][1] + o_u)

        def finish():
            for g in (0, 1):
                if is_near:
                    m_s[slots[g], h] = m[g]
                    l_s[slots[g], h] = l[g]
                    acc[slots[g], h] = o[g]
                else:
                    l_row = jnp.sum(l[g], axis=0, keepdims=True)
                    o_s[slots[g], h] = (o[g] / l_row).astype(BF16)
                    m_s[slots[g], h] = m[g] + jnp.log2(l_row)

        return [functools.partial(step, u, c) for u in range(len(units)) for c in (0, 1)], finish

    def forward(units, base, h, is_near, nxt):
        steps, finish = attend_steps(units, base, h, is_near)
        maxes = {}
        following = score_steps(*nxt, maxes) if nxt else []
        interleave(steps, following)
        finish()
        if nxt:
            score_max(nxt[0], maxes)

    def send_o(h):
        copy(20, o_s.at[1, h], og.at[h], peer).start()

    def near_fwd(h, _):
        forward(near, 4, h, True, (near, 4, h + 1))
        return 0

    def far_fwd(h, _):
        forward(far, 0, h, False, (far, 0, h + 1))
        send_o(h)
        return 0

    last = n_heads - 1
    maxes = {}
    for c in (c_kv[2], c_kv[5]):
        c.wait_recv()
    keys_ready(2 * d_near)
    keys_ready(2 * d_near + 1)
    for step in score_steps(near, 4, 0, maxes):
        step()
    score_max(near, maxes)
    lax.fori_loop(0, last, near_fwd, 0)
    for c in (c_kv[0], c_kv[1], c_kv[3], c_kv[4]):
        c.wait_recv()
    for d in d_far:
        keys_ready(2 * d)
        keys_ready(2 * d + 1)
    forward(near, 4, last, True, (far, 0, 0))
    lax.fori_loop(0, last, far_fwd, 0)
    c_dy.wait_recv()
    do_s[1] = dot_nt(weight(w_own, "o"), dyp[...]).astype(BF16).reshape(n_heads, hd, cols)
    forward(far, 0, last, False, None)
    send_o(last)
    dkv[...] = jnp.zeros_like(dkv)

    def row_dots(h, _):
        for s in (0, 1):
            d_s[s, h] = jnp.sum(do_s[s, h].astype(F32) * o_s[s, h].astype(F32), axis=0, keepdims=True)
        return 0

    lax.fori_loop(0, n_heads, row_dots, 0)

    def prob_steps(units, bufs, h, which):
        def step(u, c):
            qi, kt, first, diag = units[u]
            r, q = spans(diag, c)
            buf = bufs[u % len(bufs)]
            p = jnp.exp2(dot(k_s[kt, r], q_s[qi, h, :, q]) * c_scale - m_s[qi, h, :, q])
            p = masked(p, diag, 0.0)
            pb[buf, r, q] = p.astype(BF16)
            db[buf, r, q] = (p * (dot(v_s[kt, r], do_s[qi, h, :, q]) - d_s[qi, h, :, q])).astype(BF16)
        return [functools.partial(step, u, c) for u in which for c in (0, 1)]

    def grad_steps(units, bufs, h, u, dq):
        qi, kt, first, diag = units[u]
        buf = bufs[u % len(bufs)]
        kept = {}

        def over_queries(name, src, lhs, rows, c):
            q = slice(c * part, (c + 1) * part)
            keys = slice(0, part) if diag and c == 0 else slice(0, cols)
            val = dot_nt(lhs[qi, h, :, q], src[buf, keys, q])
            if c == 0 and not diag:
                kept[name] = val
            elif diag:
                dkv[kt, rows, keys] += val
            else:
                dkv[kt, rows, :] += kept[name] + val

        def over_keys(c):
            r, q = spans(diag, c)
            val = widen(dot(kvt[kt, :hd, r], db[buf, r, q]), 0.0)
            if c == 0:
                kept["q"] = val
            else:
                add_to(dq, first, kept["q"] + val)

        return ([functools.partial(over_queries, "v", pb, do_s, slice(hd, 2 * hd), c) for c in (0, 1)]
                + [functools.partial(over_queries, "k", db, q_s, slice(0, hd), c) for c in (0, 1)]
                + [functools.partial(over_keys, c) for c in (0, 1)])

    def backward(units, bufs, h, nxt):
        dq = [jnp.zeros((hd, cols), F32), jnp.zeros((hd, cols), F32)]
        for u in range(len(units)):
            if u + 1 < len(units):
                ahead = prob_steps(units, bufs, h, [u + 1])
            else:
                ahead = prob_steps(*nxt, [0]) if nxt else []
            interleave(ahead, grad_steps(units, bufs, h, u, dq))
        return dq

    near_bufs, far_bufs = (0, 1, 2), (3, 4)

    def far_bwd(h, nxt):
        dq = backward(far, far_bufs, h, nxt)
        for g in (0, 1):
            acc[slots[g], h] = dq[g]

    def near_bwd(h, nxt):
        dq = backward(near, near_bufs, h, nxt)
        for g in (0, 1):
            dq_s[slots[g], h] = ((dq[g] + acc[slots[g], h]) * scale).astype(BF16)
        copy(21, dq_s.at[1, h], dqg.at[h], peer).start()

    def far_loop(h, _):
        far_bwd(h, (far, far_bufs, h + 1))
        return 0

    def near_loop(h, _):
        near_bwd(h, (near, near_bufs, h + 1))
        return 0

    for step in prob_steps(far, far_bufs, 0, [0]):
        step()
    lax.fori_loop(0, last, far_loop, 0)
    far_bwd(last, (near, near_bufs, 0))
    c_dkv = [copy(16 + i, dkv.at[pl.ds(2 * d, 2)], rcv.at[i], at_cp(rank + shards - d)) for i, d in enumerate(d_far + (d_near,))]
    for c in c_dkv[:2]:
        c.start()
    c_w.wait_recv()
    for c in c_relay[:2]:
        c.start()
    lax.fori_loop(0, last, near_loop, 0)
    near_bwd(last, None)
    c_dkv[2].start()
    c_relay[1].wait_recv()
    c_relay[2].start()

    stores = []

    def leave(src, dst):
        c = pltpu.make_async_copy(src, dst, local.at[6 + len(stores)])
        c.start()
        stores.append(c)

    for h in range(n_heads):
        go_s[h] = (dot(o_s[0, h], dy_s[...]) + dot(o_s[1, h], dyp[...])).astype(BF16)
    leave(go_s, go_ref)
    for c in c_dkv:
        c.wait_recv()
    for slot in (1, 0):
        total = dkv[slot] + rcv[0, slot] + rcv[1, slot] + rcv[2, slot]
        dkvb[slot, :hd, :] = (total[:hd, :] * scale).astype(BF16)
        dkvb[slot, hd:, :] = total[hd:, :].astype(BF16)
        if slot == 1:
            c_last = copy(19, dkvb.at[1], dkvg, peer)
            c_last.start()
    for h in range(n_heads):
        gq_s[h] = (dot(dq_s[0, h], x_s[...]) + dot(dq_s[1, h], xp[...])).astype(BF16)
    leave(gq_s, gq_ref)
    gkv_s[...] = (dot(dkvb[0], x_s[...]) + dot(dkvb[1], xp[...])).astype(BF16)
    leave(gkv_s.at[:hd], gk_ref)
    leave(gkv_s.at[hd:], gv_ref)
    c_o = copy(20, o_s.at[1], og, peer)
    c_o.wait_recv()
    c_relay[0].wait_recv()
    c_relay[2].wait_recv()
    rows = 128
    for i in range(cols // rows):
        blk = slice(i * rows, (i + 1) * rows)
        y = (dot_tn(o_s[0, :, :, blk].reshape(hw, rows), weight(w_own, "o"))
             + dot_tn(og[:, :, blk].reshape(hw, rows), weight(w_peer, "o")))
        y_s[blk, :] = y.astype(BF16)
    leave(y_s, y_ref)
    c_dq = copy(21, dq_s.at[1], dqg, peer)
    c_dq.wait_recv()
    for i in range(cols // rows):
        blk = slice(i * rows, (i + 1) * rows)
        dx = (dot_tn(dq_s[0, :, :, blk].reshape(hw, rows), weight(w_own, "q"))
              + dot_tn(dqg[:, :, blk].reshape(hw, rows), weight(w_peer, "q")))
        dx += dot_tn(dkvb[0, :hd, blk], weight(w_own, "k")) + dot_tn(dkvb[0, hd:, blk], weight(w_own, "v"))
        dx_f[blk, :] = dx
    c_last.wait_recv()
    for i in range(cols // rows):
        blk = slice(i * rows, (i + 1) * rows)
        dx = dx_f[blk, :] + dot_tn(dkvg[:hd, blk], weight(w_peer, "k")) + dot_tn(dkvg[hd:, blk], weight(w_peer, "v"))
        dx_s[blk, :] = dx.astype(BF16)
    leave(dx_s, dx_ref)
    for c in [c_x, c_dy, c_o, c_dq, c_last, c_w] + c_relay + c_kv + c_dkv:
        c.wait_send()
    for c in stores:
        c.wait()


def solution(mesh):
    shards = mesh.shape["cp"]

    def device_fn(x_own, w_query, w_key, w_value, w_out, dy_own):
        model, n_heads, hd = w_query.shape
        cols = x_own.shape[0]
        hw = n_heads * hd
        scale = hd ** -0.5
        wq = w_query.transpose(1, 2, 0).reshape(shards, hw // shards, model)
        wk = w_key.transpose(1, 2, 0).reshape(shards, hd // shards, model)
        wv = w_value.transpose(1, 2, 0).reshape(shards, hd // shards, model)
        wo = w_out.reshape(shards, hw // shards, model)
        per_head = (2, n_heads, hd, cols)
        b = lambda *s: pltpu.VMEM(s, BF16)
        f = lambda *s: pltpu.VMEM(s, F32)
        area = n_heads * 9 * cols * cols
        y, dx, gq, gk, gv, go = pl.pallas_call(
            functools.partial(kernel, shards, n_heads, hd, scale * math.log2(math.e), scale),
            out_shape=(jax.ShapeDtypeStruct((cols, model), BF16), jax.ShapeDtypeStruct((cols, model), BF16),
                       jax.ShapeDtypeStruct((n_heads, hd, model), BF16), jax.ShapeDtypeStruct((hd, model), BF16),
                       jax.ShapeDtypeStruct((hd, model), BF16), jax.ShapeDtypeStruct((n_heads, hd, model), BF16)),
            in_specs=[ANY] * 6,
            out_specs=(ANY,) * 6,
            scratch_shapes=[b(cols, model)] * 4 + [b(shards, 2 * (hw + hd) // shards, model)] * 2
            + [b(*per_head), b(*per_head), b(*per_head), b(*per_head[1:]), b(*per_head), b(*per_head[1:]),
               b(2 * shards, 2 * hd, cols), b(2 * shards, cols, hd), b(2 * shards, cols, hd), f(*per_head),
               f(2, n_heads, 1, cols), f(2, n_heads, 8, cols), f(2, n_heads, 1, cols), f(2, 1, cols),
               f(9, cols, cols), b(5, cols, cols), b(5, cols, cols), f(2 * shards, 2 * hd, cols),
               f(shards - 1, 2, 2 * hd, cols), b(2, 2 * hd, cols), b(2 * hd, cols),
               b(cols, model), b(cols, model), f(cols, model), b(n_heads, hd, model), b(2 * hd, model), b(n_heads, hd, model),
               pltpu.SemaphoreType.DMA((N_COPIES,)), pltpu.SemaphoreType.DMA((N_COPIES,)), pltpu.SemaphoreType.DMA((12,))],
            compiler_params=pltpu.CompilerParams(vmem_limit_bytes=VMEM_LIMIT, collective_id=0, has_side_effects=True),
            cost_estimate=pl.CostEstimate(flops=area * 7 * 2 * hd, bytes_accessed=16 << 20, transcendentals=2 * area),
            name="attention",
        )(x_own, dy_own, wq, wk, wv, wo)
        back = lambda g, n: g.reshape(n, hd, model).transpose(2, 0, 1)[None]
        return y, dx, back(gq, n_heads), back(gk, 1), back(gv, 1), go[None]

    return jax.shard_map(device_fn, mesh=mesh,
                         in_specs=(ROW_SPEC, HEAD_SPEC, HEAD_SPEC, HEAD_SPEC, OUT_W_SPEC, ROW_SPEC),
                         out_specs=(ROW_SPEC, ROW_SPEC, GRAD_SPEC, GRAD_SPEC, GRAD_SPEC, GRAD_OUT_SPEC),
                         check_vma=False)
```

```python
import functools
import math

import jax
import jax.numpy as jnp
from jax import lax
from jax.experimental import pallas as pl
from jax.experimental.pallas import tpu as pltpu
from jax.sharding import PartitionSpec as P

ROW_SPEC = P(("dp", "cp", "tp"), None)
HEAD_SPEC = P(None, "tp", None)
OUT_W_SPEC = P("tp", None, None)
GRAD_SPEC = P(("dp", "cp"), None, "tp", None)
GRAD_OUT_SPEC = P(("dp", "cp"), "tp", None, None)
F32 = jnp.float32
BF16 = jnp.bfloat16
NT = (((1,), (1,)), ((), ()))
TN = (((0,), (0,)), ((), ()))
VMEM = pl.BlockSpec(memory_space=pltpu.VMEM)
ANY = pl.BlockSpec(memory_space=pl.ANY)
VMEM_LIMIT = 52 * 1024 * 1024
N_COPIES = 23


def dot(a, b):
    return jnp.dot(a, b, preferred_element_type=F32)


def dot_nt(a, b):
    return lax.dot_general(a, b, NT, preferred_element_type=F32)


def dot_tn(a, b):
    return lax.dot_general(a, b, TN, preferred_element_type=F32)


def shard_units(rank, half, d, shards):
    early = (rank + shards - d) // shards
    slot = early * half + (1 - early) * (1 - half)
    return [(slot, 2 * d + half, early, False), (1 - half, 2 * d + slot, 0, False)]


def diag_mask(size):
    return lax.broadcasted_iota(jnp.int32, (size, size), 1) >= lax.broadcasted_iota(jnp.int32, (size, size), 0)


def pick(first, pair):
    if isinstance(first, int):
        return pair[1 - first]
    return jnp.where(first == 1, pair[0], pair[1])


def add_to(pair, first, value):
    if isinstance(first, int):
        pair[1 - first] = pair[1 - first] + value
    else:
        pair[0] = pair[0] + jnp.where(first == 1, value, 0.0)
        pair[1] = pair[1] + jnp.where(first == 1, 0.0, value)


def transpose_bf16(x):
    return x.astype(F32).T.astype(BF16)


def kernel(shards, n_heads, hd, c_scale, scale,
           x_hbm, dy_hbm, wq_hbm, wk_hbm, wv_hbm, wo_hbm,
           y_ref, dx_ref, gq_ref, gk_ref, gv_ref, go_ref,
           x_s, xp, dy_s, dyp, w_own, w_peer,
           q_s, do_s, o_s, og, dq_s, dqg, kvt, k_s, v_s, acc, m_s, l_s, d_s, max_s, s_s, pb, db, dkv, rcv, dkvb, dkvg,
           y_s, dx_s, dx_f, gq_s, gkv_s, go_s, send, recv, local):
    rank = lax.axis_index("cp")
    half = lax.axis_index("tp")
    core = rank % 2
    cols = q_s.shape[-1]
    hw = n_heads * hd
    peer = {"tp": 1 - half}
    partner = {"cp": rank + 1 - 2 * core}

    d_near = shards - 1 - 2 * core
    d_far = (2, 1 + 2 * core)

    def at_cp(i):
        return {"cp": i % shards}

    def copy(i, src, dst, device):
        return pltpu.make_async_remote_copy(src_ref=src, dst_ref=dst, send_sem=send.at[i], recv_sem=recv.at[i],
                                            device_id=device, device_id_type=pl.DeviceIdType.MESH)

    n_o, n_k = hw // shards, hd // shards
    w_rows = {"o": (0, n_o), "q": (n_o, n_o), "k": (2 * n_o, n_k), "v": (2 * n_o + n_k, n_k)}

    def load(i, src, name):
        start, size = w_rows[name]
        return pltpu.make_async_copy(src, w_own.at[:, pl.ds(start, size), :], local.at[i])

    def weight(ref, name):
        start, size = w_rows[name]
        return ref[:, start:start + size, :].reshape(shards * size, ref.shape[2])

    loads = [pltpu.make_async_copy(x_hbm, x_s, local.at[0]), load(1, wk_hbm, "k"), load(2, wv_hbm, "v"), load(3, wq_hbm, "q"),
             load(4, wo_hbm, "o"), pltpu.make_async_copy(dy_hbm, dy_s, local.at[5])]
    for c in loads:
        c.start()
    barrier = pltpu.get_barrier_semaphore()
    pl.semaphore_signal(barrier, inc=1, device_id=peer, device_id_type=pl.DeviceIdType.MESH)
    for d in range(1, shards):
        pl.semaphore_signal(barrier, inc=1, device_id=at_cp(rank + d), device_id_type=pl.DeviceIdType.MESH)
    pl.semaphore_wait(barrier, shards)

    across = (rank + 2) % shards
    mid = cols // 2
    c_x = [copy(i, x_hbm.at[pl.ds(j * mid, mid)], xp.at[pl.ds(j * mid, mid)], peer) for i, j in ((0, 0), (22, 1))]
    c_dy = copy(1, dy_hbm, dyp, peer)
    c_w = copy(2, w_own.at[rank], w_peer.at[rank], peer)
    c_relay = [copy(3, w_peer.at[rank], w_peer.at[rank], partner), copy(4, w_peer.at[rank], w_peer.at[rank], at_cp(across)),
               copy(5, w_peer.at[across], w_peer.at[across], partner)]
    for c in c_x + [c_dy]:
        c.start()

    def send_kv(slot):
        ahead = (2, shards - 1 - 2 * core, 1 + 2 * core)
        cs = [copy(10 + 3 * slot + i, kvt.at[slot], kvt.at[2 * d + slot], at_cp(rank + d)) for i, d in enumerate(ahead)]
        for c in cs:
            c.start()
        return cs

    def keys_ready(tile):
        k_s[tile] = transpose_bf16(kvt[tile, :hd, :])
        v_s[tile] = transpose_bf16(kvt[tile, hd:, :])

    for c in loads[:3]:
        c.wait()
    kvt[0, :hd, :] = dot_nt(weight(w_own, "k"), x_s[...]).astype(BF16)
    kvt[0, hd:, :] = dot_nt(weight(w_own, "v"), x_s[...]).astype(BF16)
    c_kv = send_kv(0)
    loads[3].wait()
    q_s[0] = dot_nt(weight(w_own, "q"), x_s[...]).astype(BF16).reshape(n_heads, hd, cols)
    loads[4].wait()
    c_w.start()
    loads[5].wait()
    do_s[0] = dot_nt(weight(w_own, "o"), dy_s[...]).astype(BF16).reshape(n_heads, hd, cols)
    keys_ready(0)
    for j, c in enumerate(c_x):
        q = slice(j * mid, (j + 1) * mid)
        c.wait_recv()
        kvt[1, :hd, q] = dot_nt(weight(w_own, "k"), xp[q, :]).astype(BF16)
        kvt[1, hd:, q] = dot_nt(weight(w_own, "v"), xp[q, :]).astype(BF16)
        if j == 1:
            c_kv += send_kv(1)
        q_s[1, :, :, q] = dot_nt(weight(w_own, "q"), xp[q, :]).astype(BF16).reshape(n_heads, hd, mid)
    keys_ready(1)

    near = ([(half, half, 1, True), (1 - half, half, 0, False), (1 - half, 1 - half, 0, True)]
            + shard_units(rank, half, d_near, shards))
    far = shard_units(rank, half, d_far[0], shards) + shard_units(rank, half, d_far[1], shards)
    slots = (half, 1 - half)
    part = cols // 2
    triangle = diag_mask(part)

    def spans(diag, c):
        return slice(c * part, (c + 1) * part), slice(c * part, cols) if diag else slice(0, cols)

    def masked(x, diag, fill):
        if not diag:
            return x
        left = jnp.where(triangle, x[:, :part], fill)
        return left if x.shape[1] == part else jnp.concatenate([left, x[:, part:]], axis=1)

    def widen(x, fill):
        if x.shape[1] == cols:
            return x
        return jnp.concatenate([jnp.full((x.shape[0], cols - x.shape[1]), fill, x.dtype), x], axis=1)

    def interleave(first_list, second_list):
        i = j = 0
        while i < len(first_list) or j < len(second_list):
            if j >= len(second_list) or (i < len(first_list) and i * len(second_list) <= j * len(first_list)):
                first_list[i]()
                i += 1
            else:
                second_list[j]()
                j += 1

    def score_steps(units, base, h, maxes):
        def step(u, c):
            qi, kt, first, diag = units[u]
            r, q = spans(diag, c)
            s = masked(dot(k_s[kt, r], q_s[qi, h, :, q]), diag, -jnp.inf)
            s_s[base + u, r, q] = s
            mx = widen(jnp.max(s.reshape(part // 8, 8, s.shape[1]), axis=0), -jnp.inf)
            maxes[u] = mx if c == 0 else jnp.maximum(maxes[u], mx)
        return [functools.partial(step, u, c) for u in range(len(units)) for c in (0, 1)]

    def score_max(units, maxes):
        for g in (0, 1):
            best = None
            for u, (_, _, first, _) in enumerate(units):
                if isinstance(first, int):
                    if first == g:
                        continue
                    val = maxes[u]
                else:
                    val = jnp.where(first == 1 - g, maxes[u], -jnp.inf)
                best = val if best is None else jnp.maximum(best, val)
            max_s[g] = jnp.max(best, axis=0, keepdims=True) * c_scale

    def attend_steps(units, base, h, is_near):
        m = [max_s[0], max_s[1]]
        if is_near:
            l = [jnp.zeros((8, cols), F32), jnp.zeros((8, cols), F32)]
            o = [jnp.zeros((hd, cols), F32), jnp.zeros((hd, cols), F32)]
        else:
            old = [m_s[slots[g], h] for g in (0, 1)]
            m = [jnp.maximum(x, y) for x, y in zip(m, old)]
            fix = [jnp.exp2(x - y) for x, y in zip(old, m)]
            l = [l_s[slots[g], h] * fix[g] for g in (0, 1)]
            o = [acc[slots[g], h] * fix[g] for g in (0, 1)]
        sums = {}

        def step(u, c):
            qi, kt, first, diag = units[u]
            r, q = spans(diag, c)
            p = jnp.exp2(s_s[base + u, r, q] * c_scale - pick(first, m)[:, q])
            l_u = widen(jnp.sum(p.reshape(part // 8, 8, p.shape[1]), axis=0), 0.0)
            o_u = widen(dot(kvt[kt, hd:, r], p.astype(BF16)), 0.0)
            if c == 0:
                sums[u] = (l_u, o_u)
            else:
                add_to(l, first, sums[u][0] + l_u)
                add_to(o, first, sums[u][1] + o_u)

        def finish():
            for g in (0, 1):
                if is_near:
                    m_s[slots[g], h] = m[g]
                    l_s[slots[g], h] = l[g]
                    acc[slots[g], h] = o[g]
                else:
                    l_row = jnp.sum(l[g], axis=0, keepdims=True)
                    o_s[slots[g], h] = (o[g] / l_row).astype(BF16)
                    m_s[slots[g], h] = m[g] + jnp.log2(l_row)

        return [functools.partial(step, u, c) for u in range(len(units)) for c in (0, 1)], finish

    def forward(units, base, h, is_near, nxt):
        steps, finish = attend_steps(units, base, h, is_near)
        maxes = {}
        following = score_steps(*nxt, maxes) if nxt else []
        interleave(steps, following)
        finish()
        if nxt:
            score_max(nxt[0], maxes)

    def send_o(h):
        copy(20, o_s.at[1, h], og.at[h], peer).start()

    def near_fwd(h, _):
        forward(near, 4, h, True, (near, 4, h + 1))
        return 0

    def far_fwd(h, _):
        forward(far, 0, h, False, (far, 0, h + 1))
        send_o(h)
        return 0

    last = n_heads - 1
    maxes = {}
    for c in (c_kv[2], c_kv[5]):
        c.wait_recv()
    keys_ready(2 * d_near)
    keys_ready(2 * d_near + 1)
    for step in score_steps(near, 4, 0, maxes):
        step()
    score_max(near, maxes)
    lax.fori_loop(0, last, near_fwd, 0)
    for c in (c_kv[0], c_kv[1], c_kv[3], c_kv[4]):
        c.wait_recv()
    for d in d_far:
        keys_ready(2 * d)
        keys_ready(2 * d + 1)
    forward(near, 4, last, True, (far, 0, 0))
    lax.fori_loop(0, last, far_fwd, 0)
    c_dy.wait_recv()
    do_s[1] = dot_nt(weight(w_own, "o"), dyp[...]).astype(BF16).reshape(n_heads, hd, cols)
    forward(far, 0, last, False, None)
    send_o(last)
    dkv[...] = jnp.zeros_like(dkv)

    def row_dots(h, _):
        for s in (0, 1):
            d_s[s, h] = jnp.sum(do_s[s, h].astype(F32) * o_s[s, h].astype(F32), axis=0, keepdims=True)
        return 0

    lax.fori_loop(0, n_heads, row_dots, 0)

    def prob_steps(units, bufs, h, which):
        def step(u, c):
            qi, kt, first, diag = units[u]
            r, q = spans(diag, c)
            buf = bufs[u % len(bufs)]
            p = jnp.exp2(dot(k_s[kt, r], q_s[qi, h, :, q]) * c_scale - m_s[qi, h, :, q])
            p = masked(p, diag, 0.0)
            pb[buf, r, q] = p.astype(BF16)
            db[buf, r, q] = (p * (dot(v_s[kt, r], do_s[qi, h, :, q]) - d_s[qi, h, :, q])).astype(BF16)
        return [functools.partial(step, u, c) for u in which for c in (0, 1)]

    def grad_steps(units, bufs, h, u, dq):
        qi, kt, first, diag = units[u]
        buf = bufs[u % len(bufs)]
        kept = {}

        def over_queries(name, src, lhs, rows, c):
            q = slice(c * part, (c + 1) * part)
            keys = slice(0, part) if diag and c == 0 else slice(0, cols)
            val = dot_nt(lhs[qi, h, :, q], src[buf, keys, q])
            if c == 0 and not diag:
                kept[name] = val
            elif diag:
                dkv[kt, rows, keys] += val
            else:
                dkv[kt, rows, :] += kept[name] + val

        def over_keys(c):
            r, q = spans(diag, c)
            val = widen(dot(kvt[kt, :hd, r], db[buf, r, q]), 0.0)
            if c == 0:
                kept["q"] = val
            else:
                add_to(dq, first, kept["q"] + val)

        return ([functools.partial(over_queries, "v", pb, do_s, slice(hd, 2 * hd), c) for c in (0, 1)]
                + [functools.partial(over_queries, "k", db, q_s, slice(0, hd), c) for c in (0, 1)]
                + [functools.partial(over_keys, c) for c in (0, 1)])

    def backward(units, bufs, h, nxt):
        dq = [jnp.zeros((hd, cols), F32), jnp.zeros((hd, cols), F32)]
        for u in range(len(units)):
            if u + 1 < len(units):
                ahead = prob_steps(units, bufs, h, [u + 1])
            else:
                ahead = prob_steps(*nxt, [0]) if nxt else []
            interleave(ahead, grad_steps(units, bufs, h, u, dq))
        return dq

    near_bufs, far_bufs = (0, 1, 2), (3, 4)

    def far_bwd(h, nxt):
        dq = backward(far, far_bufs, h, nxt)
        for g in (0, 1):
            acc[slots[g], h] = dq[g]

    def near_bwd(h, nxt):
        dq = backward(near, near_bufs, h, nxt)
        for g in (0, 1):
            dq_s[slots[g], h] = ((dq[g] + acc[slots[g], h]) * scale).astype(BF16)
        copy(21, dq_s.at[1, h], dqg.at[h], peer).start()

    c_pair = copy(16, dkv.at[pl.ds(2 * d_far[1], 2)], rcv.at[0], partner)
    c_cross = copy(17, dkv.at[pl.ds(2 * d_far[0], 2)], rcv.at[1], at_cp(across))
    c_near = copy(18, dkv.at[pl.ds(2 * d_near, 2)], rcv.at[2], partner)

    def far_loop(h, _):
        far_bwd(h, (far, far_bufs, h + 1))

        @pl.when(h == 3)
        def _():
            c_w.wait_recv()
            c_relay[0].start()
            c_relay[1].start()

        return 0

    def near_loop(h, _):
        near_bwd(h, (near, near_bufs, h + 1))

        @pl.when(h == 0)
        def _():
            c_pair.wait_recv()
            for slot in (0, 1):
                dkv[2 * d_far[0] + slot] += rcv[0, slot]

        @pl.when(h == 1)
        def _():
            c_cross.start()

        @pl.when(h == 3)
        def _():
            c_relay[1].wait_recv()
            c_relay[2].start()

        return 0

    for step in prob_steps(far, far_bufs, 0, [0]):
        step()
    lax.fori_loop(0, last, far_loop, 0)
    far_bwd(last, (near, near_bufs, 0))
    c_pair.start()
    lax.fori_loop(0, last, near_loop, 0)
    near_bwd(last, None)
    c_near.start()

    stores = []

    def leave(src, dst):
        c = pltpu.make_async_copy(src, dst, local.at[6 + len(stores)])
        c.start()
        stores.append(c)

    def weight_grad(out, grads, own, other):
        for start in range(0, own.shape[1], 256):
            c = slice(start, min(start + 256, own.shape[1]))
            g = dot(grads[0].reshape(hw, cols), own[:, c]) + dot(grads[1].reshape(hw, cols), other[:, c])
            out[:, :, c] = g.astype(BF16).reshape(n_heads, hd, g.shape[1])

    weight_grad(go_s, o_s, dy_s, dyp)
    leave(go_s, go_ref)
    c_cross.wait_recv()
    c_near.wait_recv()
    for slot in (1, 0):
        total = dkv[slot] + rcv[1, slot] + rcv[2, slot]
        dkvb[slot, :hd, :] = (total[:hd, :] * scale).astype(BF16)
        dkvb[slot, hd:, :] = total[hd:, :].astype(BF16)
        if slot == 1:
            c_last = copy(19, dkvb.at[1], dkvg, peer)
            c_last.start()
    weight_grad(gq_s, dq_s, x_s, xp)
    leave(gq_s, gq_ref)
    gkv_s[...] = (dot(dkvb[0], x_s[...]) + dot(dkvb[1], xp[...])).astype(BF16)
    leave(gkv_s.at[:hd], gk_ref)
    leave(gkv_s.at[hd:], gv_ref)
    c_o = copy(20, o_s.at[1], og, peer)
    c_o.wait_recv()
    c_relay[0].wait_recv()
    c_relay[2].wait_recv()
    rows = 128
    for i in range(cols // rows):
        blk = slice(i * rows, (i + 1) * rows)
        y = (dot_tn(o_s[0, :, :, blk].reshape(hw, rows), weight(w_own, "o"))
             + dot_tn(og[:, :, blk].reshape(hw, rows), weight(w_peer, "o")))
        y_s[blk, :] = y.astype(BF16)
    leave(y_s, y_ref)
    c_dq = copy(21, dq_s.at[1], dqg, peer)
    c_dq.wait_recv()
    for i in range(cols // rows):
        blk = slice(i * rows, (i + 1) * rows)
        dx = (dot_tn(dq_s[0, :, :, blk].reshape(hw, rows), weight(w_own, "q"))
              + dot_tn(dqg[:, :, blk].reshape(hw, rows), weight(w_peer, "q")))
        dx += dot_tn(dkvb[0, :hd, blk], weight(w_own, "k")) + dot_tn(dkvb[0, hd:, blk], weight(w_own, "v"))
        dx_f[blk, :] = dx
    c_last.wait_recv()
    for i in range(cols // rows):
        blk = slice(i * rows, (i + 1) * rows)
        dx = dx_f[blk, :] + dot_tn(dkvg[:hd, blk], weight(w_peer, "k")) + dot_tn(dkvg[hd:, blk], weight(w_peer, "v"))
        dx_s[blk, :] = dx.astype(BF16)
    leave(dx_s, dx_ref)
    for c in c_x + [c_dy, c_o, c_dq, c_last, c_w, c_pair, c_cross, c_near] + c_relay + c_kv:
        c.wait_send()
    for c in stores:
        c.wait()


def solution(mesh):
    shards = mesh.shape["cp"]

    def device_fn(x_own, w_query, w_key, w_value, w_out, dy_own):
        model, n_heads, hd = w_query.shape
        cols = x_own.shape[0]
        hw = n_heads * hd
        scale = hd ** -0.5
        wq = w_query.transpose(1, 2, 0).reshape(shards, hw // shards, model)
        wk = w_key.transpose(1, 2, 0).reshape(shards, hd // shards, model)
        wv = w_value.transpose(1, 2, 0).reshape(shards, hd // shards, model)
        wo = w_out.reshape(shards, hw // shards, model)
        per_head = (2, n_heads, hd, cols)
        b = lambda *s: pltpu.VMEM(s, BF16)
        f = lambda *s: pltpu.VMEM(s, F32)
        area = n_heads * 9 * cols * cols
        y, dx, gq, gk, gv, go = pl.pallas_call(
            functools.partial(kernel, shards, n_heads, hd, scale * math.log2(math.e), scale),
            out_shape=(jax.ShapeDtypeStruct((cols, model), BF16), jax.ShapeDtypeStruct((cols, model), BF16),
                       jax.ShapeDtypeStruct((n_heads, hd, model), BF16), jax.ShapeDtypeStruct((hd, model), BF16),
                       jax.ShapeDtypeStruct((hd, model), BF16), jax.ShapeDtypeStruct((n_heads, hd, model), BF16)),
            in_specs=[ANY] * 6,
            out_specs=(ANY,) * 6,
            scratch_shapes=[b(cols, model)] * 4 + [b(shards, 2 * (hw + hd) // shards, model)] * 2
            + [b(*per_head), b(*per_head), b(*per_head), b(*per_head[1:]), b(*per_head), b(*per_head[1:]),
               b(2 * shards, 2 * hd, cols), b(2 * shards, cols, hd), b(2 * shards, cols, hd), f(*per_head),
               f(2, n_heads, 1, cols), f(2, n_heads, 8, cols), f(2, n_heads, 1, cols), f(2, 1, cols),
               f(9, cols, cols), b(5, cols, cols), b(5, cols, cols), f(2 * shards, 2 * hd, cols),
               f(shards - 1, 2, 2 * hd, cols), b(2, 2 * hd, cols), b(2 * hd, cols),
               b(cols, model), b(cols, model), f(cols, model), b(n_heads, hd, model), b(2 * hd, model), b(n_heads, hd, model),
               pltpu.SemaphoreType.DMA((N_COPIES,)), pltpu.SemaphoreType.DMA((N_COPIES,)), pltpu.SemaphoreType.DMA((12,))],
            compiler_params=pltpu.CompilerParams(vmem_limit_bytes=VMEM_LIMIT, collective_id=0, has_side_effects=True),
            cost_estimate=pl.CostEstimate(flops=area * 7 * 2 * hd, bytes_accessed=16 << 20, transcendentals=2 * area),
            name="attention",
        )(x_own, dy_own, wq, wk, wv, wo)
        back = lambda g, n: g.reshape(n, hd, model).transpose(2, 0, 1)[None]
        return y, dx, back(gq, n_heads), back(gk, 1), back(gv, 1), go[None]

    return jax.shard_map(device_fn, mesh=mesh,
                         in_specs=(ROW_SPEC, HEAD_SPEC, HEAD_SPEC, HEAD_SPEC, OUT_W_SPEC, ROW_SPEC),
                         out_specs=(ROW_SPEC, ROW_SPEC, GRAD_SPEC, GRAD_SPEC, GRAD_SPEC, GRAD_OUT_SPEC),
                         check_vma=False)
```

```python
import functools
import math

import jax
import jax.numpy as jnp
from jax import lax
from jax.experimental import pallas as pl
from jax.experimental.pallas import tpu as pltpu
from jax.sharding import PartitionSpec as P

ROW_SPEC = P(("dp", "cp", "tp"), None)
HEAD_SPEC = P(None, "tp", None)
OUT_W_SPEC = P("tp", None, None)
GRAD_SPEC = P(("dp", "cp"), None, "tp", None)
GRAD_OUT_SPEC = P(("dp", "cp"), "tp", None, None)
F32 = jnp.float32
BF16 = jnp.bfloat16
NT = (((1,), (1,)), ((), ()))
TN = (((0,), (0,)), ((), ()))
VMEM = pl.BlockSpec(memory_space=pltpu.VMEM)
ANY = pl.BlockSpec(memory_space=pl.ANY)
HBM = pl.BlockSpec(memory_space=pltpu.HBM)
VMEM_LIMIT = 64 * 1024 * 1024 - 64 * 1024
N_COPIES = 23
PAD = 16
BIG = 3.0e38


def dot(a, b):
    return jnp.dot(a, b, preferred_element_type=F32)


def dot_nt(a, b):
    return lax.dot_general(a, b, NT, preferred_element_type=F32)


def dot_tn(a, b):
    return lax.dot_general(a, b, TN, preferred_element_type=F32)


def shard_units(rank, half, d, shards):
    early = (rank + shards - d) // shards
    slot = early * half + (1 - early) * (1 - half)
    return [(slot, 2 * d + half, early, False), (1 - half, 2 * d + slot, 0, False)]


def diag_mask(size):
    return lax.broadcasted_iota(jnp.int32, (size, size), 1) >= lax.broadcasted_iota(jnp.int32, (size, size), 0)


def pick(first, pair):
    if isinstance(first, int):
        return pair[1 - first]
    return jnp.where(first == 1, pair[0], pair[1])


def add_to(pair, first, value):
    if isinstance(first, int):
        pair[1 - first] = pair[1 - first] + value
    else:
        pair[0] = pair[0] + jnp.where(first == 1, value, 0.0)
        pair[1] = pair[1] + jnp.where(first == 1, 0.0, value)


def transpose_bf16(x):
    return x.astype(F32).T.astype(BF16)


def with_columns(x_t, row):
    hi = jnp.clip(row, -BIG, BIG).astype(BF16).astype(F32)
    mid = (row - hi).astype(BF16).astype(F32)
    low = row - hi - mid
    line = lax.broadcasted_iota(jnp.int32, (PAD, row.shape[1]), 0)
    extra = jnp.where(line == 0, hi, jnp.where(line == 1, mid, jnp.where(line == 2, low, 0.0)))
    return jnp.concatenate([x_t.astype(F32), extra], axis=0).T.astype(BF16)


def kernel(shards, n_heads, hd, c_scale, scale,
           x_hbm, dy_hbm, wq_hbm, wk_hbm, wv_hbm, wo_hbm,
           y_ref, dx_ref, gq_ref, gk_ref, gv_ref, go_ref,
           x_s, xp, dy_s, dyp, w_own, w_peer,
           q_s, do_s, o_s, og, dq_s, dqg, kvt, k_s, ka, q_n, do_n, acc, m_s, l_s, max_s, s_s, pb, db, dkv, rcv, dkvb, dkvg,
           y_s, dx_s, dx_f, gq_s, gkv_s, go_s, send, recv, local):
    rank = lax.axis_index("cp")
    half = lax.axis_index("tp")
    core = rank % 2
    cols = q_s.shape[-1]
    hw = n_heads * hd
    peer = {"tp": 1 - half}
    partner = {"cp": rank + 1 - 2 * core}

    d_near = shards - 1 - 2 * core
    d_far = (2, 1 + 2 * core)

    def at_cp(i):
        return {"cp": i % shards}

    def copy(i, src, dst, device):
        return pltpu.make_async_remote_copy(src_ref=src, dst_ref=dst, send_sem=send.at[i], recv_sem=recv.at[i],
                                            device_id=device, device_id_type=pl.DeviceIdType.MESH)

    n_o, n_k = hw // shards, hd // shards
    w_rows = {"o": (0, n_o), "q": (n_o, n_o), "k": (2 * n_o, n_k), "v": (2 * n_o + n_k, n_k)}

    def load(i, src, name):
        start, size = w_rows[name]
        return pltpu.make_async_copy(src, w_own.at[:, pl.ds(start, size), :], local.at[i])

    def weight(ref, name):
        start, size = w_rows[name]
        return ref[:, start:start + size, :].reshape(shards * size, ref.shape[2])

    loads = [pltpu.make_async_copy(x_hbm, x_s, local.at[0]), load(1, wk_hbm, "k"), load(2, wv_hbm, "v"), load(3, wq_hbm, "q"),
             load(4, wo_hbm, "o"), pltpu.make_async_copy(dy_hbm, dy_s, local.at[5])]
    for c in loads:
        c.start()
    barrier = pltpu.get_barrier_semaphore()
    pl.semaphore_signal(barrier, inc=1, device_id=peer, device_id_type=pl.DeviceIdType.MESH)
    for d in range(1, shards):
        pl.semaphore_signal(barrier, inc=1, device_id=at_cp(rank + d), device_id_type=pl.DeviceIdType.MESH)
    pl.semaphore_wait(barrier, shards)

    across = (rank + 2) % shards
    mid = cols // 2
    c_x = [copy(i, x_hbm.at[pl.ds(j * mid, mid)], xp.at[pl.ds(j * mid, mid)], peer) for i, j in ((0, 0), (22, 1))]
    c_dy = copy(1, dy_hbm, dyp, peer)
    c_w = copy(2, w_own.at[rank], w_peer.at[rank], peer)
    c_relay = [copy(3, w_peer.at[rank], w_peer.at[rank], partner), copy(4, w_peer.at[rank], w_peer.at[rank], at_cp(across)),
               copy(5, w_peer.at[across], w_peer.at[across], partner)]
    for c in c_x + [c_dy]:
        c.start()

    def send_kv(slot):
        ahead = (2, shards - 1 - 2 * core, 1 + 2 * core)
        cs = [copy(10 + 3 * slot + i, kvt.at[slot], kvt.at[2 * d + slot], at_cp(rank + d)) for i, d in enumerate(ahead)]
        for c in cs:
            c.start()
        return cs

    def keys_ready(tile):
        k_s[tile] = transpose_bf16(kvt[tile, :hd, :])
        minus = jnp.where(lax.broadcasted_iota(jnp.int32, (PAD, cols), 0) < 3, -1.0, 0.0).astype(BF16)
        for i in (0, 1):
            ka[tile, i, :hd, :] = kvt[tile, i * hd:(i + 1) * hd, :]
            ka[tile, i, hd:, :] = minus

    for c in loads[:3]:
        c.wait()
    kvt[0, :hd, :] = dot_nt(weight(w_own, "k"), x_s[...]).astype(BF16)
    kvt[0, hd:, :] = dot_nt(weight(w_own, "v"), x_s[...]).astype(BF16)
    c_kv = send_kv(0)
    loads[3].wait()
    q_s[0] = dot_nt(weight(w_own, "q"), x_s[...]).astype(BF16).reshape(n_heads, hd, cols)
    loads[4].wait()
    c_w.start()
    loads[5].wait()
    do_s[0] = dot_nt(weight(w_own, "o"), dy_s[...]).astype(BF16).reshape(n_heads, hd, cols)
    keys_ready(0)
    for j, c in enumerate(c_x):
        q = slice(j * mid, (j + 1) * mid)
        c.wait_recv()
        kvt[1, :hd, q] = dot_nt(weight(w_own, "k"), xp[q, :]).astype(BF16)
        kvt[1, hd:, q] = dot_nt(weight(w_own, "v"), xp[q, :]).astype(BF16)
        if j == 1:
            c_kv += send_kv(1)
        q_s[1, :, :, q] = dot_nt(weight(w_own, "q"), xp[q, :]).astype(BF16).reshape(n_heads, hd, mid)
    keys_ready(1)

    near = ([(half, half, 1, True), (1 - half, half, 0, False), (1 - half, 1 - half, 0, True)]
            + shard_units(rank, half, d_near, shards))
    far = shard_units(rank, half, d_far[0], shards) + shard_units(rank, half, d_far[1], shards)
    slots = (half, 1 - half)
    part = cols // 2
    triangle = diag_mask(part)

    def spans(diag, c):
        return slice(c * part, (c + 1) * part), slice(c * part, cols) if diag else slice(0, cols)

    def masked(x, diag, fill):
        if not diag:
            return x
        left = jnp.where(triangle, x[:, :part], fill)
        return left if x.shape[1] == part else jnp.concatenate([left, x[:, part:]], axis=1)

    def widen(x, fill):
        if x.shape[1] == cols:
            return x
        return jnp.concatenate([jnp.full((x.shape[0], cols - x.shape[1]), fill, x.dtype), x], axis=1)

    def interleave(first_list, second_list):
        i = j = 0
        while i < len(first_list) or j < len(second_list):
            if j >= len(second_list) or (i < len(first_list) and i * len(second_list) <= j * len(first_list)):
                first_list[i]()
                i += 1
            else:
                second_list[j]()
                j += 1

    def score_steps(units, base, h, maxes):
        def step(u, c):
            qi, kt, first, diag = units[u]
            r, q = spans(diag, c)
            s = masked(dot(k_s[kt, r], q_s[qi, h, :, q]), diag, -jnp.inf)
            s_s[base + u, r, q] = s
            mx = widen(jnp.max(s.reshape(part // 8, 8, s.shape[1]), axis=0), -jnp.inf)
            maxes[u] = mx if c == 0 else jnp.maximum(maxes[u], mx)
        return [functools.partial(step, u, c) for u in range(len(units)) for c in (0, 1)]

    def score_max(units, maxes):
        for g in (0, 1):
            best = None
            for u, (_, _, first, _) in enumerate(units):
                if isinstance(first, int):
                    if first == g:
                        continue
                    val = maxes[u]
                else:
                    val = jnp.where(first == 1 - g, maxes[u], -jnp.inf)
                best = val if best is None else jnp.maximum(best, val)
            max_s[g] = jnp.max(best, axis=0, keepdims=True) * c_scale

    def attend_steps(units, base, h, is_near):
        m = [max_s[0], max_s[1]]
        if is_near:
            l = [jnp.zeros((8, cols), F32), jnp.zeros((8, cols), F32)]
            o = [jnp.zeros((hd, cols), F32), jnp.zeros((hd, cols), F32)]
        else:
            old = [m_s[slots[g], h] for g in (0, 1)]
            m = [jnp.maximum(x, y) for x, y in zip(m, old)]
            fix = [jnp.exp2(x - y) for x, y in zip(old, m)]
            l = [l_s[slots[g], h] * fix[g] for g in (0, 1)]
            o = [acc[slots[g], h] * fix[g] for g in (0, 1)]
        sums = {}

        def step(u, c):
            qi, kt, first, diag = units[u]
            r, q = spans(diag, c)
            p = jnp.exp2(s_s[base + u, r, q] * c_scale - pick(first, m)[:, q])
            l_u = widen(jnp.sum(p.reshape(part // 8, 8, p.shape[1]), axis=0), 0.0)
            o_u = widen(dot(kvt[kt, hd:, r], p.astype(BF16)), 0.0)
            if c == 0:
                sums[u] = (l_u, o_u)
            else:
                add_to(l, first, sums[u][0] + l_u)
                add_to(o, first, sums[u][1] + o_u)

        def finish():
            for g in (0, 1):
                if is_near:
                    m_s[slots[g], h] = m[g]
                    l_s[slots[g], h] = l[g]
                    acc[slots[g], h] = o[g]
                else:
                    l_row = jnp.sum(l[g], axis=0, keepdims=True)
                    o_s[slots[g], h] = (o[g] / l_row).astype(BF16)
                    q_n[slots[g], h] = with_columns(q_s[slots[g], h], (m[g] + jnp.log2(l_row)) * (1.0 / c_scale))

        return [functools.partial(step, u, c) for u in range(len(units)) for c in (0, 1)], finish

    def forward(units, base, h, is_near, nxt):
        steps, finish = attend_steps(units, base, h, is_near)
        maxes = {}
        following = score_steps(*nxt, maxes) if nxt else []
        interleave(steps, following)
        finish()
        if nxt:
            score_max(nxt[0], maxes)

    def send_o(h):
        copy(20, o_s.at[1, h], og.at[h], peer).start()

    def near_fwd(h, _):
        forward(near, 4, h, True, (near, 4, h + 1))
        return 0

    def far_fwd(h, _):
        forward(far, 0, h, False, (far, 0, h + 1))
        send_o(h)
        return 0

    last = n_heads - 1
    maxes = {}
    for c in (c_kv[2], c_kv[5]):
        c.wait_recv()
    keys_ready(2 * d_near)
    keys_ready(2 * d_near + 1)
    for step in score_steps(near, 4, 0, maxes):
        step()
    score_max(near, maxes)
    lax.fori_loop(0, last, near_fwd, 0)
    for c in (c_kv[0], c_kv[1], c_kv[3], c_kv[4]):
        c.wait_recv()
    for d in d_far:
        keys_ready(2 * d)
        keys_ready(2 * d + 1)
    forward(near, 4, last, True, (far, 0, 0))
    lax.fori_loop(0, last, far_fwd, 0)
    c_dy.wait_recv()
    do_s[1] = dot_nt(weight(w_own, "o"), dyp[...]).astype(BF16).reshape(n_heads, hd, cols)
    forward(far, 0, last, False, None)
    send_o(last)
    dkv[...] = jnp.zeros_like(dkv)

    for h in range(n_heads):
        for i in (0, 1):
            delta = jnp.sum(do_s[i, h].astype(F32) * o_s[i, h].astype(F32), axis=0, keepdims=True)
            do_n[i, h] = with_columns(do_s[i, h], delta)
    lower = lax.broadcasted_iota(jnp.int32, (part, part), 0) >= lax.broadcasted_iota(jnp.int32, (part, part), 1)

    def prob_steps(units, bufs, h, u):
        qi, kt, first, diag = units[u]
        buf = bufs[u % len(bufs)]
        kept = {}

        def probs(c):
            r, k = slice(c * part, (c + 1) * part), slice(0, part if diag and c == 0 else cols)
            p = jnp.exp2(dot(q_n[qi, h, r], ka[kt, 0, :, k]) * c_scale)
            if diag:
                p = jnp.concatenate([p[:, :c * part], jnp.where(lower, p[:, c * part:], 0.0)], axis=1) if c else jnp.where(lower, p, 0.0)
            pb[buf, r, k] = p.astype(BF16)
            kept[c] = p

        def grads(c):
            r, k = slice(c * part, (c + 1) * part), slice(0, part if diag and c == 0 else cols)
            db[buf, r, k] = (kept[c] * dot(do_n[qi, h, r], ka[kt, 1, :, k])).astype(BF16)

        return [functools.partial(f, c) for c in (0, 1) for f in (probs, grads)]

    def grad_steps(units, bufs, h, u, dq):
        qi, kt, first, diag = units[u]
        buf = bufs[u % len(bufs)]
        kept = {}

        def over_queries(name, src, lhs, rows, c):
            q, k = slice(c * part, (c + 1) * part), slice(0, part if diag and c == 0 else cols)
            val = dot(lhs[qi, h, :, q], src[buf, q, k])
            if diag:
                dkv[kt, rows, k] += val
            elif c == 0:
                kept[name] = val
            else:
                dkv[kt, rows, :] += kept[name] + val

        def over_keys(c):
            k, q = spans(diag, c)
            val = widen(dot_nt(kvt[kt, :hd, k], db[buf, q, k]), 0.0)
            if c == 0:
                kept["q"] = val
            else:
                add_to(dq, first, kept["q"] + val)

        return ([functools.partial(over_queries, "v", pb, do_s, slice(hd, 2 * hd), c) for c in (0, 1)]
                + [functools.partial(over_queries, "k", db, q_s, slice(0, hd), c) for c in (0, 1)]
                + [functools.partial(over_keys, c) for c in (0, 1)])

    def backward(units, bufs, h, nxt):
        dq = [jnp.zeros((hd, cols), F32), jnp.zeros((hd, cols), F32)]
        for u in range(len(units)):
            if u + 1 < len(units):
                ahead = prob_steps(units, bufs, h, u + 1)
            else:
                ahead = prob_steps(*nxt, 0) if nxt else []
            products = grad_steps(units, bufs, h, u, dq)
            for i, step in enumerate(products):
                step()
                if i < len(ahead):
                    ahead[i]()
        return dq

    near_bufs, far_bufs = (0, 1, 2), (3, 4)

    def far_bwd(h, nxt):
        dq = backward(far, far_bufs, h, nxt)
        for g in (0, 1):
            acc[slots[g], h] = dq[g]

    def near_bwd(h, nxt):
        dq = backward(near, near_bufs, h, nxt)
        for g in (0, 1):
            dq_s[slots[g], h] = ((dq[g] + acc[slots[g], h]) * scale).astype(BF16)
        copy(21, dq_s.at[1, h], dqg.at[h], peer).start()

    c_pair = copy(16, dkv.at[pl.ds(2 * d_far[1], 2)], rcv.at[0], partner)
    c_cross = copy(17, dkv.at[pl.ds(2 * d_far[0], 2)], rcv.at[1], at_cp(across))
    c_near = copy(18, dkv.at[pl.ds(2 * d_near, 2)], rcv.at[2], partner)

    def far_loop(h, _):
        far_bwd(h, (far, far_bufs, h + 1))

        @pl.when(h == 3)
        def _():
            c_w.wait_recv()
            c_relay[0].start()
            c_relay[1].start()

        return 0

    def near_loop(h, _):
        near_bwd(h, (near, near_bufs, h + 1))

        @pl.when(h == 0)
        def _():
            c_pair.wait_recv()
            for slot in (0, 1):
                dkv[2 * d_far[0] + slot] += rcv[0, slot]

        @pl.when(h == 1)
        def _():
            c_cross.start()

        @pl.when(h == 3)
        def _():
            c_relay[1].wait_recv()
            c_relay[2].start()

        return 0

    for step in prob_steps(far, far_bufs, 0, 0):
        step()
    lax.fori_loop(0, last, far_loop, 0)
    far_bwd(last, (near, near_bufs, 0))
    c_pair.start()
    lax.fori_loop(0, last, near_loop, 0)
    near_bwd(last, None)
    c_near.start()

    stores = []

    def leave(src, dst):
        c = pltpu.make_async_copy(src, dst, local.at[6 + len(stores)])
        c.start()
        stores.append(c)

    def weight_grad(out, grads, own, other):
        for start in range(0, own.shape[1], 256):
            c = slice(start, min(start + 256, own.shape[1]))
            g = dot(grads[0].reshape(hw, cols), own[:, c]) + dot(grads[1].reshape(hw, cols), other[:, c])
            out[:, :, c] = g.astype(BF16).reshape(n_heads, hd, g.shape[1])

    weight_grad(go_s, o_s, dy_s, dyp)
    leave(go_s, go_ref)
    c_cross.wait_recv()
    c_near.wait_recv()
    for slot in (1, 0):
        total = dkv[slot] + rcv[1, slot] + rcv[2, slot]
        dkvb[slot, :hd, :] = (total[:hd, :] * scale).astype(BF16)
        dkvb[slot, hd:, :] = total[hd:, :].astype(BF16)
        if slot == 1:
            c_last = copy(19, dkvb.at[1], dkvg, peer)
            c_last.start()
    weight_grad(gq_s, dq_s, x_s, xp)
    leave(gq_s, gq_ref)
    gkv_s[...] = (dot(dkvb[0], x_s[...]) + dot(dkvb[1], xp[...])).astype(BF16)
    leave(gkv_s.at[:hd], gk_ref)
    leave(gkv_s.at[hd:], gv_ref)
    c_o = copy(20, o_s.at[1], og, peer)
    c_o.wait_recv()
    c_relay[0].wait_recv()
    c_relay[2].wait_recv()
    rows = 128
    for i in range(cols // rows):
        blk = slice(i * rows, (i + 1) * rows)
        y = (dot_tn(o_s[0, :, :, blk].reshape(hw, rows), weight(w_own, "o"))
             + dot_tn(og[:, :, blk].reshape(hw, rows), weight(w_peer, "o")))
        y_s[blk, :] = y.astype(BF16)
    leave(y_s, y_ref)
    c_dq = copy(21, dq_s.at[1], dqg, peer)
    c_dq.wait_recv()
    for i in range(cols // rows):
        blk = slice(i * rows, (i + 1) * rows)
        dx = (dot_tn(dq_s[0, :, :, blk].reshape(hw, rows), weight(w_own, "q"))
              + dot_tn(dqg[:, :, blk].reshape(hw, rows), weight(w_peer, "q")))
        dx += dot_tn(dkvb[0, :hd, blk], weight(w_own, "k")) + dot_tn(dkvb[0, hd:, blk], weight(w_own, "v"))
        dx_f[blk, :] = dx
    c_last.wait_recv()
    for i in range(cols // rows):
        blk = slice(i * rows, (i + 1) * rows)
        dx = dx_f[blk, :] + dot_tn(dkvg[:hd, blk], weight(w_peer, "k")) + dot_tn(dkvg[hd:, blk], weight(w_peer, "v"))
        dx_s[blk, :] = dx.astype(BF16)
    leave(dx_s, dx_ref)
    for c in c_x + [c_dy, c_o, c_dq, c_last, c_w, c_pair, c_cross, c_near] + c_relay + c_kv:
        c.wait_send()
    for c in stores:
        c.wait()


def hand_out(n, *refs):
    src, dst, held, sems = refs[:n], refs[n:2 * n], refs[2 * n:3 * n], refs[3 * n]
    loads = [pltpu.make_async_copy(src[i], held[i], sems.at[0, i]) for i in range(n)]
    stores = [pltpu.make_async_copy(held[i], dst[i], sems.at[1, i]) for i in range(n)]
    for c in loads:
        c.start()
    for load, store in zip(loads, stores):
        load.wait()
        store.start()
    for c in stores:
        c.wait()


def solution(mesh):
    shards = mesh.shape["cp"]

    def device_fn(x_own, w_query, w_key, w_value, w_out, dy_own):
        model, n_heads, hd = w_query.shape
        cols = x_own.shape[0]
        hw = n_heads * hd
        scale = hd ** -0.5
        wq = w_query.transpose(1, 2, 0).reshape(shards, hw // shards, model)
        wk = w_key.transpose(1, 2, 0).reshape(shards, hd // shards, model)
        wv = w_value.transpose(1, 2, 0).reshape(shards, hd // shards, model)
        wo = w_out.reshape(shards, hw // shards, model)
        per_head = (2, n_heads, hd, cols)
        b = lambda *s: pltpu.VMEM(s, BF16)
        f = lambda *s: pltpu.VMEM(s, F32)
        area = n_heads * 9 * cols * cols
        y, dx, gq, gk, gv, go = pl.pallas_call(
            functools.partial(kernel, shards, n_heads, hd, scale * math.log2(math.e), scale),
            out_shape=(jax.ShapeDtypeStruct((cols, model), BF16), jax.ShapeDtypeStruct((cols, model), BF16),
                       jax.ShapeDtypeStruct((n_heads, hd, model), BF16), jax.ShapeDtypeStruct((hd, model), BF16),
                       jax.ShapeDtypeStruct((hd, model), BF16), jax.ShapeDtypeStruct((n_heads, hd, model), BF16)),
            in_specs=[HBM] * 6,
            out_specs=(ANY,) * 6,
            scratch_shapes=[b(cols, model)] * 4 + [b(shards, 2 * (hw + hd) // shards, model)] * 2
            + [b(*per_head), b(*per_head), b(*per_head), b(*per_head[1:]), b(*per_head), b(*per_head[1:]),
               b(2 * shards, 2 * hd, cols), b(2 * shards, cols, hd), b(2 * shards, 2, hd + PAD, cols),
               b(2, n_heads, cols, hd + PAD), b(2, n_heads, cols, hd + PAD), f(*per_head),
               f(2, n_heads, 1, cols), f(2, n_heads, 8, cols), f(2, 1, cols),
               f(9, cols, cols), b(5, cols, cols), b(5, cols, cols), f(2 * shards, 2 * hd, cols),
               f(shards - 1, 2, 2 * hd, cols), b(2, 2 * hd, cols), b(2 * hd, cols),
               b(cols, model), b(cols, model), f(cols, model), b(n_heads, hd, model), b(2 * hd, model), b(n_heads, hd, model),
               pltpu.SemaphoreType.DMA((N_COPIES,)), pltpu.SemaphoreType.DMA((N_COPIES,)), pltpu.SemaphoreType.DMA((12,))],
            compiler_params=pltpu.CompilerParams(vmem_limit_bytes=VMEM_LIMIT, collective_id=0, has_side_effects=True),
            cost_estimate=pl.CostEstimate(flops=area * 7 * 2 * hd, bytes_accessed=16 << 20, transcendentals=2 * area),
            name="attention",
        )(x_own, dy_own, wq, wk, wv, wo)
        outs = (y, dx, gq, gk, gv, go)
        y, dx, gq, gk, gv, go = pl.pallas_call(
            functools.partial(hand_out, len(outs)),
            out_shape=tuple(jax.ShapeDtypeStruct(o.shape, o.dtype) for o in outs),
            in_specs=[HBM] * len(outs),
            out_specs=(HBM,) * len(outs),
            scratch_shapes=[pltpu.VMEM(o.shape, o.dtype) for o in outs] + [pltpu.SemaphoreType.DMA((2, len(outs)))],
            cost_estimate=pl.CostEstimate(flops=0, bytes_accessed=8 << 20, transcendentals=0),
            name="hand_out",
        )(*outs)
        back = lambda g, n: g.reshape(n, hd, model).transpose(2, 0, 1)[None]
        return y, dx, back(gq, n_heads), back(gk, 1), back(gv, 1), go[None]

    return jax.shard_map(device_fn, mesh=mesh,
                         in_specs=(ROW_SPEC, HEAD_SPEC, HEAD_SPEC, HEAD_SPEC, OUT_W_SPEC, ROW_SPEC),
                         out_specs=(ROW_SPEC, ROW_SPEC, GRAD_SPEC, GRAD_SPEC, GRAD_SPEC, GRAD_OUT_SPEC),
                         check_vma=False)
```

```python
import functools
import math

import jax
import jax.numpy as jnp
from jax import lax
from jax.experimental import pallas as pl
from jax.experimental.pallas import tpu as pltpu
from jax.sharding import PartitionSpec as P

ROW_SPEC = P(("dp", "cp", "tp"), None)
HEAD_SPEC = P(None, "tp", None)
OUT_W_SPEC = P("tp", None, None)
GRAD_SPEC = P(("dp", "cp"), None, "tp", None)
GRAD_OUT_SPEC = P(("dp", "cp"), "tp", None, None)
F32 = jnp.float32
BF16 = jnp.bfloat16
NT = (((1,), (1,)), ((), ()))
TN = (((0,), (0,)), ((), ()))
ANY = pl.BlockSpec(memory_space=pl.ANY)
HBM = pl.BlockSpec(memory_space=pltpu.HBM)
VMEM_LIMIT = 64 * 1024 * 1024 - 64 * 1024
N_COPIES = 24
PAD = 16
BIG = 3.0e38


def dot(a, b):
    return jnp.dot(a, b, preferred_element_type=F32)


def dot_nt(a, b):
    return lax.dot_general(a, b, NT, preferred_element_type=F32)


def dot_tn(a, b):
    return lax.dot_general(a, b, TN, preferred_element_type=F32)


def shard_units(rank, half, d, shards):
    early = (rank + shards - d) // shards
    slot = early * half + (1 - early) * (1 - half)
    return [(slot, 2 * d + half, early, False), (1 - half, 2 * d + slot, 0, False)]


def diag_mask(size):
    return lax.broadcasted_iota(jnp.int32, (size, size), 1) >= lax.broadcasted_iota(jnp.int32, (size, size), 0)


def pick(first, pair):
    if isinstance(first, int):
        return pair[1 - first]
    return jnp.where(first == 1, pair[0], pair[1])


def add_to(pair, first, value):
    if isinstance(first, int):
        pair[1 - first] = pair[1 - first] + value
    else:
        pair[0] = pair[0] + jnp.where(first == 1, value, 0.0)
        pair[1] = pair[1] + jnp.where(first == 1, 0.0, value)


def transpose_bf16(x):
    return x.astype(F32).T.astype(BF16)


def with_columns(x_t, row):
    hi = jnp.clip(row, -BIG, BIG).astype(BF16).astype(F32)
    mid = (row - hi).astype(BF16).astype(F32)
    low = row - hi - mid
    line = lax.broadcasted_iota(jnp.int32, (PAD, row.shape[1]), 0)
    extra = jnp.where(line == 0, hi, jnp.where(line == 1, mid, jnp.where(line == 2, low, 0.0)))
    return jnp.concatenate([x_t.astype(F32), extra], axis=0).T.astype(BF16)


def kernel(shards, n_heads, hd, c_scale, scale,
           x_hbm, dy_hbm, wq_hbm, wk_hbm, wv_hbm, wo_hbm,
           y_ref, dx_ref, gq_ref, gk_ref, gv_ref, go_ref,
           x_s, xp, dy_s, dyp, w_own, w_peer,
           q_s, do_s, o_s, og, dq_s, dqg, kvt, k_s, ka, q_n, do_n, acc, m_s, l_s, max_s, s_s, pb, db, dkv, rcv, dkvb, dkvg,
           y_s, dx_s, dx_f, gq_s, gkv_s, go_s, go_f, send, recv, local):
    rank = lax.axis_index("cp")
    half = lax.axis_index("tp")
    core = rank % 2
    cols = q_s.shape[-1]
    hw = n_heads * hd
    peer = {"tp": 1 - half}
    partner = {"cp": rank + 1 - 2 * core}

    d_near = shards - 1 - 2 * core
    d_far = (2, 1 + 2 * core)

    def at_cp(i):
        return {"cp": i % shards}

    def copy(i, src, dst, device):
        return pltpu.make_async_remote_copy(src_ref=src, dst_ref=dst, send_sem=send.at[i], recv_sem=recv.at[i],
                                            device_id=device, device_id_type=pl.DeviceIdType.MESH)

    n_o, n_k = hw // shards, hd // shards
    w_rows = {"o": (0, n_o), "q": (n_o, n_o), "k": (2 * n_o, n_k), "v": (2 * n_o + n_k, n_k)}

    def load(i, src, name):
        start, size = w_rows[name]
        return pltpu.make_async_copy(src, w_own.at[:, pl.ds(start, size), :], local.at[i])

    def weight(ref, name):
        start, size = w_rows[name]
        return ref[:, start:start + size, :].reshape(shards * size, ref.shape[2])

    loads = [pltpu.make_async_copy(x_hbm, x_s, local.at[0]), load(1, wk_hbm, "k"), load(2, wv_hbm, "v"), load(3, wq_hbm, "q"),
             load(4, wo_hbm, "o"), pltpu.make_async_copy(dy_hbm, dy_s, local.at[5])]
    for c in loads:
        c.start()
    barrier = pltpu.get_barrier_semaphore()
    pl.semaphore_signal(barrier, inc=1, device_id=peer, device_id_type=pl.DeviceIdType.MESH)
    for d in range(1, shards):
        pl.semaphore_signal(barrier, inc=1, device_id=at_cp(rank + d), device_id_type=pl.DeviceIdType.MESH)
    pl.semaphore_wait(barrier, shards)

    across = (rank + 2) % shards
    mid = cols // 2
    c_x = [copy(i, x_hbm.at[pl.ds(j * mid, mid)], xp.at[pl.ds(j * mid, mid)], peer) for i, j in ((0, 0), (22, 1))]
    c_dy = [copy(i, dy_hbm.at[pl.ds(j * mid, mid)], dyp.at[pl.ds(j * mid, mid)], peer) for i, j in ((1, 0), (23, 1))]
    c_w = copy(2, w_own.at[rank], w_peer.at[rank], peer)
    c_relay = [copy(3, w_peer.at[rank], w_peer.at[rank], partner), copy(4, w_peer.at[rank], w_peer.at[rank], at_cp(across)),
               copy(5, w_peer.at[across], w_peer.at[across], partner)]
    for c in c_x + c_dy:
        c.start()

    def send_kv(slot):
        ahead = (2, shards - 1 - 2 * core, 1 + 2 * core)
        cs = [copy(10 + 3 * slot + i, kvt.at[slot], kvt.at[2 * d + slot], at_cp(rank + d)) for i, d in enumerate(ahead)]
        for c in cs:
            c.start()
        return cs

    def keys_ready(tile):
        k_s[tile] = transpose_bf16(kvt[tile, :hd, :])
        minus = jnp.where(lax.broadcasted_iota(jnp.int32, (PAD, cols), 0) < 3, -1.0, 0.0).astype(BF16)
        for i in (0, 1):
            ka[tile, i, :hd, :] = kvt[tile, i * hd:(i + 1) * hd, :]
            ka[tile, i, hd:, :] = minus

    for c in loads[:3]:
        c.wait()
    kvt[0, :hd, :] = dot_nt(weight(w_own, "k"), x_s[...]).astype(BF16)
    kvt[0, hd:, :] = dot_nt(weight(w_own, "v"), x_s[...]).astype(BF16)
    c_kv = send_kv(0)
    loads[3].wait()
    q_s[0] = dot_nt(weight(w_own, "q"), x_s[...]).astype(BF16).reshape(n_heads, hd, cols)
    loads[4].wait()
    c_w.start()
    loads[5].wait()
    do_s[0] = dot_nt(weight(w_own, "o"), dy_s[...]).astype(BF16).reshape(n_heads, hd, cols)
    keys_ready(0)
    part = cols // 2
    triangle = diag_mask(part)

    def own_diagonal(h, _):
        s0 = dot(k_s[0, :part], q_s[0, h])
        s0 = jnp.concatenate([jnp.where(triangle, s0[:, :part], -jnp.inf), s0[:, part:]], axis=1)
        s1 = jnp.where(triangle, dot(k_s[0, part:], q_s[0, h, :, part:]), -jnp.inf)
        m0, m1 = jnp.max(s0, axis=0, keepdims=True), jnp.max(s1, axis=0, keepdims=True)
        m = jnp.concatenate([m0[:, :part], jnp.maximum(m0[:, part:], m1)], axis=1) * c_scale
        p0, p1 = jnp.exp2(s0 * c_scale - m), jnp.exp2(s1 * c_scale - m[:, part:])
        zeros = jnp.zeros((8, part), F32)
        l_s[0, h] = (jnp.sum(p0.reshape(part // 8, 8, cols), axis=0)
                     + jnp.concatenate([zeros, jnp.sum(p1.reshape(part // 8, 8, part), axis=0)], axis=1))
        o1 = dot(kvt[0, hd:, part:], p1.astype(BF16))
        acc[0, h] = dot(kvt[0, hd:, :part], p0.astype(BF16)) + jnp.concatenate([jnp.zeros_like(o1), o1], axis=1)
        m_s[0, h] = m
        m_s[1, h] = jnp.full_like(m, -jnp.inf)
        l_s[1, h] = jnp.zeros((8, cols), F32)
        acc[1, h] = jnp.zeros((hd, cols), F32)
        return 0

    lax.fori_loop(0, n_heads, own_diagonal, 0)
    for j, c in enumerate(c_x):
        q = slice(j * mid, (j + 1) * mid)
        c.wait_recv()
        kvt[1, :hd, q] = dot_nt(weight(w_own, "k"), xp[q, :]).astype(BF16)
        kvt[1, hd:, q] = dot_nt(weight(w_own, "v"), xp[q, :]).astype(BF16)
        if j == 1:
            c_kv += send_kv(1)
        q_s[1, :, :, q] = dot_nt(weight(w_own, "q"), xp[q, :]).astype(BF16).reshape(n_heads, hd, mid)
    keys_ready(1)

    near = ([(half, half, 1, True), (1 - half, half, 0, False), (1 - half, 1 - half, 0, True)]
            + shard_units(rank, half, d_near, shards))
    far = shard_units(rank, half, d_far[0], shards) + shard_units(rank, half, d_far[1], shards)
    slots = (half, 1 - half)
    near_fwd_units = [(1, 1, half, True)] + near[1:2] + near[3:]

    def spans(diag, c):
        return slice(c * part, (c + 1) * part), slice(c * part, cols) if diag else slice(0, cols)

    def masked(x, diag, fill):
        if not diag:
            return x
        left = jnp.where(triangle, x[:, :part], fill)
        return left if x.shape[1] == part else jnp.concatenate([left, x[:, part:]], axis=1)

    def widen(x, fill):
        if x.shape[1] == cols:
            return x
        return jnp.concatenate([jnp.full((x.shape[0], cols - x.shape[1]), fill, x.dtype), x], axis=1)

    def interleave(first_list, second_list):
        i = j = 0
        while i < len(first_list) or j < len(second_list):
            if j >= len(second_list) or (i < len(first_list) and i * len(second_list) <= j * len(first_list)):
                first_list[i]()
                i += 1
            else:
                second_list[j]()
                j += 1

    def score_steps(units, base, h, maxes):
        def step(u, c):
            qi, kt, first, diag = units[u]
            r, q = spans(diag, c)
            s = masked(dot(k_s[kt, r], q_s[qi, h, :, q]), diag, -jnp.inf)
            s_s[base + u, r, q] = s
            mx = widen(jnp.max(s.reshape(part // 8, 8, s.shape[1]), axis=0), -jnp.inf)
            maxes[u] = mx if c == 0 else jnp.maximum(maxes[u], mx)
        return [functools.partial(step, u, c) for u in range(len(units)) for c in (0, 1)]

    def score_max(units, maxes):
        for g in (0, 1):
            best = None
            for u, (_, _, first, _) in enumerate(units):
                if isinstance(first, int):
                    if first == g:
                        continue
                    val = maxes[u]
                else:
                    val = jnp.where(first == 1 - g, maxes[u], -jnp.inf)
                best = val if best is None else jnp.maximum(best, val)
            max_s[g] = jnp.max(best, axis=0, keepdims=True) * c_scale

    def attend_steps(units, base, h, is_near):
        old = [m_s[slots[g], h] for g in (0, 1)]
        m = [jnp.maximum(max_s[g], old[g]) for g in (0, 1)]
        fix = [jnp.exp2(x - y) for x, y in zip(old, m)]
        l = [l_s[slots[g], h] * fix[g] for g in (0, 1)]
        o = [acc[slots[g], h] * fix[g] for g in (0, 1)]
        sums = {}

        def step(u, c):
            qi, kt, first, diag = units[u]
            r, q = spans(diag, c)
            p = jnp.exp2(s_s[base + u, r, q] * c_scale - pick(first, m)[:, q])
            l_u = widen(jnp.sum(p.reshape(part // 8, 8, p.shape[1]), axis=0), 0.0)
            o_u = widen(dot(kvt[kt, hd:, r], p.astype(BF16)), 0.0)
            if c == 0:
                sums[u] = (l_u, o_u)
            else:
                add_to(l, first, sums[u][0] + l_u)
                add_to(o, first, sums[u][1] + o_u)

        def finish():
            for g in (0, 1):
                if is_near:
                    m_s[slots[g], h] = m[g]
                    l_s[slots[g], h] = l[g]
                    acc[slots[g], h] = o[g]
                else:
                    l_row = jnp.sum(l[g], axis=0, keepdims=True)
                    o_s[slots[g], h] = (o[g] / l_row).astype(BF16)
                    q_n[slots[g], h] = with_columns(q_s[slots[g], h], (m[g] + jnp.log2(l_row)) * (1.0 / c_scale))

        return [functools.partial(step, u, c) for u in range(len(units)) for c in (0, 1)], finish

    def forward(units, base, h, is_near, nxt):
        steps, finish = attend_steps(units, base, h, is_near)
        maxes = {}
        following = score_steps(*nxt, maxes) if nxt else []
        interleave(steps, following)
        finish()
        if nxt:
            score_max(nxt[0], maxes)

    def send_o(h):
        copy(20, o_s.at[1, h], og.at[h], peer).start()

    def near_fwd(h, _):
        forward(near_fwd_units, 4, h, True, (near_fwd_units, 4, h + 1))
        return 0

    def far_fwd(h, _):
        forward(far, 0, h, False, (far, 0, h + 1))
        send_o(h)
        return 0

    last = n_heads - 1
    maxes = {}
    for c in (c_kv[2], c_kv[5]):
        c.wait_recv()
    keys_ready(2 * d_near)
    keys_ready(2 * d_near + 1)
    for step in score_steps(near_fwd_units, 4, 0, maxes):
        step()
    score_max(near_fwd_units, maxes)
    lax.fori_loop(0, last, near_fwd, 0)
    for c in (c_kv[0], c_kv[1], c_kv[3], c_kv[4]):
        c.wait_recv()
    for d in d_far:
        keys_ready(2 * d)
        keys_ready(2 * d + 1)
    forward(near_fwd_units, 4, last, True, (far, 0, 0))
    lax.fori_loop(0, last, far_fwd, 0)
    forward(far, 0, last, False, None)
    send_o(last)
    dkv[...] = jnp.zeros_like(dkv)

    def do_ready(i):
        for h in range(n_heads):
            delta = jnp.sum(do_s[i, h].astype(F32) * o_s[i, h].astype(F32), axis=0, keepdims=True)
            do_n[i, h] = with_columns(do_s[i, h], delta)

    def column_blocks(width):
        return [slice(start, min(start + 256, width)) for start in range(0, width, 256)]

    do_ready(0)
    for c in column_blocks(dy_s.shape[1]):
        go_f[:, c] = dot(o_s[0].reshape(hw, cols), dy_s[:, c])
    for j, c in enumerate(c_dy):
        q = slice(j * mid, (j + 1) * mid)
        c.wait_recv()
        do_s[1, :, :, q] = dot_nt(weight(w_own, "o"), dyp[q, :]).astype(BF16).reshape(n_heads, hd, mid)
    do_ready(1)
    lower = lax.broadcasted_iota(jnp.int32, (part, part), 0) >= lax.broadcasted_iota(jnp.int32, (part, part), 1)

    def prob_steps(units, bufs, h, u):
        qi, kt, first, diag = units[u]
        buf = bufs[u % len(bufs)]
        kept = {}

        def probs(c):
            r, k = slice(c * part, (c + 1) * part), slice(0, part if diag and c == 0 else cols)
            p = jnp.exp2(dot(q_n[qi, h, r], ka[kt, 0, :, k]) * c_scale)
            if diag:
                p = jnp.concatenate([p[:, :c * part], jnp.where(lower, p[:, c * part:], 0.0)], axis=1) if c else jnp.where(lower, p, 0.0)
            pb[buf, r, k] = p.astype(BF16)
            kept[c] = p

        def grads(c):
            r, k = slice(c * part, (c + 1) * part), slice(0, part if diag and c == 0 else cols)
            db[buf, r, k] = (kept[c] * dot(do_n[qi, h, r], ka[kt, 1, :, k])).astype(BF16)

        return [functools.partial(f, c) for c in (0, 1) for f in (probs, grads)]

    def grad_steps(units, bufs, h, u, dq):
        qi, kt, first, diag = units[u]
        buf = bufs[u % len(bufs)]
        kept = {}

        def over_queries(name, src, lhs, rows, c):
            q, k = slice(c * part, (c + 1) * part), slice(0, part if diag and c == 0 else cols)
            val = dot(lhs[qi, h, :, q], src[buf, q, k])
            if diag:
                dkv[kt, rows, k] += val
            elif c == 0:
                kept[name] = val
            else:
                dkv[kt, rows, :] += kept[name] + val

        def over_keys(c):
            k, q = spans(diag, c)
            val = widen(dot_nt(kvt[kt, :hd, k], db[buf, q, k]), 0.0)
            if c == 0:
                kept["q"] = val
            else:
                add_to(dq, first, kept["q"] + val)

        return ([functools.partial(over_queries, "v", pb, do_s, slice(hd, 2 * hd), c) for c in (0, 1)]
                + [functools.partial(over_queries, "k", db, q_s, slice(0, hd), c) for c in (0, 1)]
                + [functools.partial(over_keys, c) for c in (0, 1)])

    def backward(units, bufs, h, nxt):
        dq = [jnp.zeros((hd, cols), F32), jnp.zeros((hd, cols), F32)]
        for u in range(len(units)):
            if u + 1 < len(units):
                ahead = prob_steps(units, bufs, h, u + 1)
            else:
                ahead = prob_steps(*nxt, 0) if nxt else []
            products = grad_steps(units, bufs, h, u, dq)
            for i, step in enumerate(products):
                step()
                if i < len(ahead):
                    ahead[i]()
        return dq

    near_bufs, far_bufs = (0, 1, 2), (3, 4)

    def far_bwd(h, nxt):
        dq = backward(far, far_bufs, h, nxt)
        for g in (0, 1):
            acc[slots[g], h] = dq[g]

    def near_bwd(h, nxt):
        dq = backward(near, near_bufs, h, nxt)
        for g in (0, 1):
            dq_s[slots[g], h] = ((dq[g] + acc[slots[g], h]) * scale).astype(BF16)
        copy(21, dq_s.at[1, h], dqg.at[h], peer).start()

    c_pair = copy(16, dkv.at[pl.ds(2 * d_far[1], 2)], rcv.at[0], partner)
    c_cross = copy(17, dkv.at[pl.ds(2 * d_far[0], 2)], rcv.at[1], at_cp(across))
    c_near = copy(18, dkv.at[pl.ds(2 * d_near, 2)], rcv.at[2], partner)

    def far_loop(h, _):
        far_bwd(h, (far, far_bufs, h + 1))

        @pl.when(h == 3)
        def _():
            c_w.wait_recv()
            c_relay[0].start()
            c_relay[1].start()

        return 0

    def near_loop(h, _):
        near_bwd(h, (near, near_bufs, h + 1))

        @pl.when(h == 0)
        def _():
            c_pair.wait_recv()
            for slot in (0, 1):
                dkv[2 * d_far[0] + slot] += rcv[0, slot]

        @pl.when(h == 1)
        def _():
            c_cross.start()

        @pl.when(h == 3)
        def _():
            c_relay[1].wait_recv()
            c_relay[2].start()

        return 0

    for step in prob_steps(far, far_bufs, 0, 0):
        step()
    lax.fori_loop(0, last, far_loop, 0)
    far_bwd(last, (near, near_bufs, 0))
    c_pair.start()
    lax.fori_loop(0, last, near_loop, 0)
    near_bwd(last, None)
    c_near.start()

    stores = []

    def leave(src, dst):
        c = pltpu.make_async_copy(src, dst, local.at[6 + len(stores)])
        c.start()
        stores.append(c)

    for c in column_blocks(dy_s.shape[1]):
        g = go_f[:, c] + dot(o_s[1].reshape(hw, cols), dyp[:, c])
        go_s[:, :, c] = g.astype(BF16).reshape(n_heads, hd, g.shape[1])
    leave(go_s, go_ref)
    c_cross.wait_recv()
    c_near.wait_recv()
    for slot in (1, 0):
        total = dkv[slot] + rcv[1, slot] + rcv[2, slot]
        dkvb[slot, :hd, :] = (total[:hd, :] * scale).astype(BF16)
        dkvb[slot, hd:, :] = total[hd:, :].astype(BF16)
        if slot == 1:
            c_last = copy(19, dkvb.at[1], dkvg, peer)
            c_last.start()
    for c in column_blocks(x_s.shape[1]):
        g = dot(dq_s[0].reshape(hw, cols), x_s[:, c]) + dot(dq_s[1].reshape(hw, cols), xp[:, c])
        gq_s[:, :, c] = g.astype(BF16).reshape(n_heads, hd, g.shape[1])
    leave(gq_s, gq_ref)
    gkv_s[...] = (dot(dkvb[0], x_s[...]) + dot(dkvb[1], xp[...])).astype(BF16)
    leave(gkv_s.at[:hd], gk_ref)
    leave(gkv_s.at[hd:], gv_ref)
    c_o = copy(20, o_s.at[1], og, peer)
    c_o.wait_recv()
    c_relay[0].wait_recv()
    c_relay[2].wait_recv()
    rows = 256
    for i in range(cols // rows):
        blk = slice(i * rows, (i + 1) * rows)
        y = (dot_tn(o_s[0, :, :, blk].reshape(hw, rows), weight(w_own, "o"))
             + dot_tn(og[:, :, blk].reshape(hw, rows), weight(w_peer, "o")))
        y_s[blk, :] = y.astype(BF16)
    leave(y_s, y_ref)
    c_dq = copy(21, dq_s.at[1], dqg, peer)
    c_dq.wait_recv()
    for i in range(cols // rows):
        blk = slice(i * rows, (i + 1) * rows)
        dx = (dot_tn(dq_s[0, :, :, blk].reshape(hw, rows), weight(w_own, "q"))
              + dot_tn(dqg[:, :, blk].reshape(hw, rows), weight(w_peer, "q")))
        dx += dot_tn(dkvb[0, :hd, blk], weight(w_own, "k")) + dot_tn(dkvb[0, hd:, blk], weight(w_own, "v"))
        dx_f[blk, :] = dx
    c_last.wait_recv()
    for i in range(cols // rows):
        blk = slice(i * rows, (i + 1) * rows)
        dx = dx_f[blk, :] + dot_tn(dkvg[:hd, blk], weight(w_peer, "k")) + dot_tn(dkvg[hd:, blk], weight(w_peer, "v"))
        dx_s[blk, :] = dx.astype(BF16)
    leave(dx_s, dx_ref)
    for c in c_x + c_dy + [c_o, c_dq, c_last, c_w, c_pair, c_cross, c_near] + c_relay + c_kv:
        c.wait_send()
    for c in stores:
        c.wait()


def hand_out(n, *refs):
    src, dst, held, sems = refs[:n], refs[n:2 * n], refs[2 * n:3 * n], refs[3 * n]
    loads = [pltpu.make_async_copy(src[i], held[i], sems.at[0, i]) for i in range(n)]
    stores = [pltpu.make_async_copy(held[i], dst[i], sems.at[1, i]) for i in range(n)]
    for c in loads:
        c.start()
    for load, store in zip(loads, stores):
        load.wait()
        store.start()
    for c in stores:
        c.wait()


def solution(mesh):
    shards = mesh.shape["cp"]

    def device_fn(x_own, w_query, w_key, w_value, w_out, dy_own):
        model, n_heads, hd = w_query.shape
        cols = x_own.shape[0]
        hw = n_heads * hd
        scale = hd ** -0.5
        wq = w_query.transpose(1, 2, 0).reshape(shards, hw // shards, model)
        wk = w_key.transpose(1, 2, 0).reshape(shards, hd // shards, model)
        wv = w_value.transpose(1, 2, 0).reshape(shards, hd // shards, model)
        wo = w_out.reshape(shards, hw // shards, model)
        per_head = (2, n_heads, hd, cols)
        b = lambda *s: pltpu.VMEM(s, BF16)
        f = lambda *s: pltpu.VMEM(s, F32)
        area = n_heads * 9 * cols * cols
        y, dx, gq, gk, gv, go = pl.pallas_call(
            functools.partial(kernel, shards, n_heads, hd, scale * math.log2(math.e), scale),
            out_shape=(jax.ShapeDtypeStruct((cols, model), BF16), jax.ShapeDtypeStruct((cols, model), BF16),
                       jax.ShapeDtypeStruct((n_heads, hd, model), BF16), jax.ShapeDtypeStruct((hd, model), BF16),
                       jax.ShapeDtypeStruct((hd, model), BF16), jax.ShapeDtypeStruct((n_heads, hd, model), BF16)),
            in_specs=[HBM] * 6,
            out_specs=(ANY,) * 6,
            scratch_shapes=[b(cols, model)] * 4 + [b(shards, 2 * (hw + hd) // shards, model)] * 2
            + [b(*per_head), b(*per_head), b(*per_head), b(*per_head[1:]), b(*per_head), b(*per_head[1:]),
               b(2 * shards, 2 * hd, cols), b(2 * shards, cols, hd), b(2 * shards, 2, hd + PAD, cols),
               b(2, n_heads, cols, hd + PAD), b(2, n_heads, cols, hd + PAD), f(*per_head),
               f(2, n_heads, 1, cols), f(2, n_heads, 8, cols), f(2, 1, cols),
               f(8, cols, cols), b(5, cols, cols), b(5, cols, cols), f(2 * shards, 2 * hd, cols),
               f(shards - 1, 2, 2 * hd, cols), b(2, 2 * hd, cols), b(2 * hd, cols),
               b(cols, model), b(cols, model), f(cols, model), b(n_heads, hd, model), b(2 * hd, model), b(n_heads, hd, model), f(hw, model),
               pltpu.SemaphoreType.DMA((N_COPIES,)), pltpu.SemaphoreType.DMA((N_COPIES,)), pltpu.SemaphoreType.DMA((12,))],
            compiler_params=pltpu.CompilerParams(vmem_limit_bytes=VMEM_LIMIT, collective_id=0, has_side_effects=True),
            cost_estimate=pl.CostEstimate(flops=area * 7 * 2 * hd, bytes_accessed=16 << 20, transcendentals=2 * area),
            name="attention",
        )(x_own, dy_own, wq, wk, wv, wo)
        outs = (y, dx, gq, gk, gv, go)
        y, dx, gq, gk, gv, go = pl.pallas_call(
            functools.partial(hand_out, len(outs)),
            out_shape=tuple(jax.ShapeDtypeStruct(o.shape, o.dtype) for o in outs),
            in_specs=[HBM] * len(outs),
            out_specs=(HBM,) * len(outs),
            scratch_shapes=[pltpu.VMEM(o.shape, o.dtype) for o in outs] + [pltpu.SemaphoreType.DMA((2, len(outs)))],
            cost_estimate=pl.CostEstimate(flops=0, bytes_accessed=8 << 20, transcendentals=0),
            name="hand_out",
        )(*outs)
        back = lambda g, n: g.reshape(n, hd, model).transpose(2, 0, 1)[None]
        return y, dx, back(gq, n_heads), back(gk, 1), back(gv, 1), go[None]

    return jax.shard_map(device_fn, mesh=mesh,
                         in_specs=(ROW_SPEC, HEAD_SPEC, HEAD_SPEC, HEAD_SPEC, OUT_W_SPEC, ROW_SPEC),
                         out_specs=(ROW_SPEC, ROW_SPEC, GRAD_SPEC, GRAD_SPEC, GRAD_SPEC, GRAD_OUT_SPEC),
                         check_vma=False)
```

```python
import functools
import math

import jax
import jax.numpy as jnp
from jax import lax
from jax.experimental import pallas as pl
from jax.experimental.pallas import tpu as pltpu
from jax.sharding import PartitionSpec as P

ROW_SPEC = P(("dp", "cp", "tp"), None)
HEAD_SPEC = P(None, "tp", None)
OUT_W_SPEC = P("tp", None, None)
GRAD_SPEC = P(("dp", "cp"), None, "tp", None)
GRAD_OUT_SPEC = P(("dp", "cp"), "tp", None, None)
F32 = jnp.float32
BF16 = jnp.bfloat16
NT = (((1,), (1,)), ((), ()))
TN = (((0,), (0,)), ((), ()))
ANY = pl.BlockSpec(memory_space=pl.ANY)
HBM = pl.BlockSpec(memory_space=pltpu.HBM)
VMEM_LIMIT = 64 * 1024 * 1024 - 64 * 1024
N_COPIES = 24
PAD = 16
BIG = 3.0e38


def dot(a, b):
    return jnp.dot(a, b, preferred_element_type=F32)


def dot_nt(a, b):
    return lax.dot_general(a, b, NT, preferred_element_type=F32)


def dot_tn(a, b):
    return lax.dot_general(a, b, TN, preferred_element_type=F32)


def shard_units(rank, half, d, shards):
    early = (rank + shards - d) // shards
    slot = early * half + (1 - early) * (1 - half)
    return [(slot, 2 * d + half, early, False), (1 - half, 2 * d + slot, 0, False)]


def diag_mask(size):
    return lax.broadcasted_iota(jnp.int32, (size, size), 1) >= lax.broadcasted_iota(jnp.int32, (size, size), 0)


def pick(first, pair):
    if isinstance(first, int):
        return pair[1 - first]
    return jnp.where(first == 1, pair[0], pair[1])


def add_to(pair, first, value):
    if isinstance(first, int):
        pair[1 - first] = pair[1 - first] + value
    else:
        pair[0] = pair[0] + jnp.where(first == 1, value, 0.0)
        pair[1] = pair[1] + jnp.where(first == 1, 0.0, value)


def transpose_bf16(x):
    return x.astype(F32).T.astype(BF16)


def with_columns(x_t, row):
    hi = jnp.clip(row, -BIG, BIG).astype(BF16).astype(F32)
    mid = (row - hi).astype(BF16).astype(F32)
    low = row - hi - mid
    line = lax.broadcasted_iota(jnp.int32, (PAD, row.shape[1]), 0)
    extra = jnp.where(line == 0, hi, jnp.where(line == 1, mid, jnp.where(line == 2, low, 0.0)))
    return jnp.concatenate([x_t.astype(F32), extra], axis=0).T.astype(BF16)


def kernel(shards, n_heads, hd, c_scale, scale,
           x_hbm, dy_hbm, wq_hbm, wk_hbm, wv_hbm, wo_hbm,
           y_ref, dx_ref, gq_ref, gk_ref, gv_ref, go_ref,
           x_s, xp, dy_s, dyp, w_own, w_peer,
           q_s, do_s, o_s, og, dq_s, dqg, kvt, k_s, ka, q_n, do_n, acc, m_s, l_s, max_s, s_s, pb, db, dkv, rcv, dkvb, dkvg,
           y_s, dx_s, dx_f, gq_s, gkv_s, go_s, go_f, send, recv, local):
    rank = lax.axis_index("cp")
    half = lax.axis_index("tp")
    core = rank % 2
    cols = q_s.shape[-1]
    hw = n_heads * hd
    peer = {"tp": 1 - half}
    partner = {"cp": rank + 1 - 2 * core}

    d_near = shards - 1 - 2 * core
    d_far = (2, 1 + 2 * core)

    def at_cp(i):
        return {"cp": i % shards}

    def copy(i, src, dst, device):
        return pltpu.make_async_remote_copy(src_ref=src, dst_ref=dst, send_sem=send.at[i], recv_sem=recv.at[i],
                                            device_id=device, device_id_type=pl.DeviceIdType.MESH)

    n_o, n_k = hw // shards, hd // shards
    w_rows = {"o": (0, n_o), "q": (n_o, n_o), "k": (2 * n_o, n_k), "v": (2 * n_o + n_k, n_k)}

    def load(i, src, name):
        start, size = w_rows[name]
        return pltpu.make_async_copy(src, w_own.at[:, pl.ds(start, size), :], local.at[i])

    def weight(ref, name):
        start, size = w_rows[name]
        return ref[:, start:start + size, :].reshape(shards * size, ref.shape[2])

    loads = [pltpu.make_async_copy(x_hbm, x_s, local.at[0]), load(1, wk_hbm, "k"), load(2, wv_hbm, "v"), load(3, wq_hbm, "q"),
             load(4, wo_hbm, "o"), pltpu.make_async_copy(dy_hbm, dy_s, local.at[5])]
    for c in loads:
        c.start()
    barrier = pltpu.get_barrier_semaphore()
    pl.semaphore_signal(barrier, inc=1, device_id=peer, device_id_type=pl.DeviceIdType.MESH)
    for d in range(1, shards):
        pl.semaphore_signal(barrier, inc=1, device_id=at_cp(rank + d), device_id_type=pl.DeviceIdType.MESH)
    pl.semaphore_wait(barrier, shards)

    across = (rank + 2) % shards
    mid = cols // 2
    c_x = [copy(i, x_hbm.at[pl.ds(j * mid, mid)], xp.at[pl.ds(j * mid, mid)], peer) for i, j in ((0, 0), (22, 1))]
    c_dy = [copy(i, dy_hbm.at[pl.ds(j * mid, mid)], dyp.at[pl.ds(j * mid, mid)], peer) for i, j in ((1, 0), (23, 1))]
    c_w = copy(2, w_own.at[rank], w_peer.at[rank], peer)
    c_relay = [copy(3, w_peer.at[rank], w_peer.at[rank], partner), copy(4, w_peer.at[rank], w_peer.at[rank], at_cp(across)),
               copy(5, w_peer.at[across], w_peer.at[across], partner)]
    for c in c_x + c_dy:
        c.start()

    def send_kv(slot):
        ahead = (2, shards - 1 - 2 * core, 1 + 2 * core)
        cs = [copy(10 + 3 * slot + i, kvt.at[slot], kvt.at[2 * d + slot], at_cp(rank + d)) for i, d in enumerate(ahead)]
        for c in cs:
            c.start()
        return cs

    def keys_ready(tile):
        k_s[tile] = transpose_bf16(kvt[tile, :hd, :])
        minus = jnp.where(lax.broadcasted_iota(jnp.int32, (PAD, cols), 0) < 3, -1.0, 0.0).astype(BF16)
        for i in (0, 1):
            ka[tile, i, :hd, :] = kvt[tile, i * hd:(i + 1) * hd, :]
            ka[tile, i, hd:, :] = minus

    for c in loads[:3]:
        c.wait()
    kvt[0, :hd, :] = dot_nt(weight(w_own, "k"), x_s[...]).astype(BF16)
    kvt[0, hd:, :] = dot_nt(weight(w_own, "v"), x_s[...]).astype(BF16)
    c_kv = send_kv(0)
    loads[3].wait()
    q_s[0] = dot_nt(weight(w_own, "q"), x_s[...]).astype(BF16).reshape(n_heads, hd, cols)
    loads[4].wait()
    c_w.start()
    loads[5].wait()
    do_s[0] = dot_nt(weight(w_own, "o"), dy_s[...]).astype(BF16).reshape(n_heads, hd, cols)
    keys_ready(0)
    part = cols // 2
    triangle = diag_mask(part)

    def own_diagonal(h, _):
        s0 = dot(k_s[0, :part], q_s[0, h])
        s0 = jnp.concatenate([jnp.where(triangle, s0[:, :part], -jnp.inf), s0[:, part:]], axis=1)
        s1 = jnp.where(triangle, dot(k_s[0, part:], q_s[0, h, :, part:]), -jnp.inf)
        m0, m1 = jnp.max(s0, axis=0, keepdims=True), jnp.max(s1, axis=0, keepdims=True)
        m = jnp.concatenate([m0[:, :part], jnp.maximum(m0[:, part:], m1)], axis=1) * c_scale
        p0, p1 = jnp.exp2(s0 * c_scale - m), jnp.exp2(s1 * c_scale - m[:, part:])
        zeros = jnp.zeros((8, part), F32)
        l_s[0, h] = (jnp.sum(p0.reshape(part // 8, 8, cols), axis=0)
                     + jnp.concatenate([zeros, jnp.sum(p1.reshape(part // 8, 8, part), axis=0)], axis=1))
        o1 = dot(kvt[0, hd:, part:], p1.astype(BF16))
        acc[0, h] = dot(kvt[0, hd:, :part], p0.astype(BF16)) + jnp.concatenate([jnp.zeros_like(o1), o1], axis=1)
        m_s[0, h] = m
        m_s[1, h] = jnp.full_like(m, -jnp.inf)
        l_s[1, h] = jnp.zeros((8, cols), F32)
        acc[1, h] = jnp.zeros((hd, cols), F32)
        return 0

    lax.fori_loop(0, n_heads, own_diagonal, 0)
    for j, c in enumerate(c_x):
        q = slice(j * mid, (j + 1) * mid)
        c.wait_recv()
        kvt[1, :hd, q] = dot_nt(weight(w_own, "k"), xp[q, :]).astype(BF16)
        kvt[1, hd:, q] = dot_nt(weight(w_own, "v"), xp[q, :]).astype(BF16)
        if j == 1:
            c_kv += send_kv(1)
        q_s[1, :, :, q] = dot_nt(weight(w_own, "q"), xp[q, :]).astype(BF16).reshape(n_heads, hd, mid)
    keys_ready(1)

    near_rest = [(1, 1, half, True), (1 - half, half, 0, False)] + shard_units(rank, half, d_near, shards)
    far = shard_units(rank, half, d_far[0], shards) + shard_units(rank, half, d_far[1], shards)
    slots = (half, 1 - half)

    def spans(diag, c):
        return slice(c * part, (c + 1) * part), slice(c * part, cols) if diag else slice(0, cols)

    def masked(x, diag, fill):
        if not diag:
            return x
        left = jnp.where(triangle, x[:, :part], fill)
        return left if x.shape[1] == part else jnp.concatenate([left, x[:, part:]], axis=1)

    def widen(x, fill):
        if x.shape[1] == cols:
            return x
        return jnp.concatenate([jnp.full((x.shape[0], cols - x.shape[1]), fill, x.dtype), x], axis=1)

    def interleave(first_list, second_list):
        i = j = 0
        while i < len(first_list) or j < len(second_list):
            if j >= len(second_list) or (i < len(first_list) and i * len(second_list) <= j * len(first_list)):
                first_list[i]()
                i += 1
            else:
                second_list[j]()
                j += 1

    def score_steps(units, base, h, maxes):
        def step(u, c):
            qi, kt, first, diag = units[u]
            r, q = spans(diag, c)
            s = masked(dot(k_s[kt, r], q_s[qi, h, :, q]), diag, -jnp.inf)
            s_s[base + u, r, q] = s
            mx = widen(jnp.max(s.reshape(part // 8, 8, s.shape[1]), axis=0), -jnp.inf)
            maxes[u] = mx if c == 0 else jnp.maximum(maxes[u], mx)
        return [functools.partial(step, u, c) for u in range(len(units)) for c in (0, 1)]

    def score_max(units, maxes):
        for g in (0, 1):
            best = None
            for u, (_, _, first, _) in enumerate(units):
                if isinstance(first, int):
                    if first == g:
                        continue
                    val = maxes[u]
                else:
                    val = jnp.where(first == 1 - g, maxes[u], -jnp.inf)
                best = val if best is None else jnp.maximum(best, val)
            max_s[g] = jnp.max(best, axis=0, keepdims=True) * c_scale

    def attend_steps(units, base, h, is_near):
        old = [m_s[slots[g], h] for g in (0, 1)]
        m = [jnp.maximum(max_s[g], old[g]) for g in (0, 1)]
        fix = [jnp.exp2(x - y) for x, y in zip(old, m)]
        l = [l_s[slots[g], h] * fix[g] for g in (0, 1)]
        o = [acc[slots[g], h] * fix[g] for g in (0, 1)]
        sums = {}

        def step(u, c):
            qi, kt, first, diag = units[u]
            r, q = spans(diag, c)
            p = jnp.exp2(s_s[base + u, r, q] * c_scale - pick(first, m)[:, q])
            l_u = widen(jnp.sum(p.reshape(part // 8, 8, p.shape[1]), axis=0), 0.0)
            o_u = widen(dot(kvt[kt, hd:, r], p.astype(BF16)), 0.0)
            if c == 0:
                sums[u] = (l_u, o_u)
            else:
                add_to(l, first, sums[u][0] + l_u)
                add_to(o, first, sums[u][1] + o_u)

        def finish():
            for g in (0, 1):
                if is_near:
                    m_s[slots[g], h] = m[g]
                    l_s[slots[g], h] = l[g]
                    acc[slots[g], h] = o[g]
                else:
                    l_row = jnp.sum(l[g], axis=0, keepdims=True)
                    o_s[slots[g], h] = (o[g] / l_row).astype(BF16)
                    q_n[slots[g], h] = with_columns(q_s[slots[g], h], (m[g] + jnp.log2(l_row)) * (1.0 / c_scale))

        return [functools.partial(step, u, c) for u in range(len(units)) for c in (0, 1)], finish

    def forward(units, base, h, is_near, nxt):
        steps, finish = attend_steps(units, base, h, is_near)
        maxes = {}
        following = score_steps(*nxt, maxes) if nxt else []
        interleave(steps, following)
        finish()
        if nxt:
            score_max(nxt[0], maxes)

    def send_o(h):
        copy(20, o_s.at[1, h], og.at[h], peer).start()

    def near_fwd(h, _):
        forward(near_rest, 4, h, True, (near_rest, 4, h + 1))
        return 0

    def far_fwd(h, _):
        forward(far, 0, h, False, (far, 0, h + 1))
        send_o(h)
        return 0

    last = n_heads - 1
    maxes = {}
    for c in (c_kv[2], c_kv[5]):
        c.wait_recv()
    keys_ready(2 * d_near)
    keys_ready(2 * d_near + 1)
    for step in score_steps(near_rest, 4, 0, maxes):
        step()
    score_max(near_rest, maxes)
    lax.fori_loop(0, last, near_fwd, 0)
    for c in (c_kv[0], c_kv[1], c_kv[3], c_kv[4]):
        c.wait_recv()
    for d in d_far:
        keys_ready(2 * d)
        keys_ready(2 * d + 1)
    forward(near_rest, 4, last, True, (far, 0, 0))
    lax.fori_loop(0, last, far_fwd, 0)
    forward(far, 0, last, False, None)
    send_o(last)
    dkv[...] = jnp.zeros_like(dkv)

    def do_ready(i):
        for h in range(n_heads):
            delta = jnp.sum(do_s[i, h].astype(F32) * o_s[i, h].astype(F32), axis=0, keepdims=True)
            do_n[i, h] = with_columns(do_s[i, h], delta)

    def column_blocks(width):
        return [slice(start, min(start + 256, width)) for start in range(0, width, 256)]

    do_ready(0)
    for c in column_blocks(dy_s.shape[1]):
        go_f[:, c] = dot(o_s[0].reshape(hw, cols), dy_s[:, c])
    lower = lax.broadcasted_iota(jnp.int32, (part, part), 0) >= lax.broadcasted_iota(jnp.int32, (part, part), 1)

    def prob_steps(units, bufs, h, u):
        qi, kt, first, diag = units[u]
        buf = bufs[u % len(bufs)]
        kept = {}

        def probs(c):
            r, k = slice(c * part, (c + 1) * part), slice(0, part if diag and c == 0 else cols)
            p = jnp.exp2(dot(q_n[qi, h, r], ka[kt, 0, :, k]) * c_scale)
            if diag:
                p = jnp.concatenate([p[:, :c * part], jnp.where(lower, p[:, c * part:], 0.0)], axis=1) if c else jnp.where(lower, p, 0.0)
            pb[buf, r, k] = p.astype(BF16)
            kept[c] = p

        def grads(c):
            r, k = slice(c * part, (c + 1) * part), slice(0, part if diag and c == 0 else cols)
            db[buf, r, k] = (kept[c] * dot(do_n[qi, h, r], ka[kt, 1, :, k])).astype(BF16)

        return [functools.partial(f, c) for c in (0, 1) for f in (probs, grads)]

    def grad_steps(units, bufs, h, u, dq):
        qi, kt, first, diag = units[u]
        buf = bufs[u % len(bufs)]
        kept = {}

        def over_queries(name, src, lhs, rows, c):
            q, k = slice(c * part, (c + 1) * part), slice(0, part if diag and c == 0 else cols)
            val = dot(lhs[qi, h, :, q], src[buf, q, k])
            if diag:
                dkv[kt, rows, k] += val
            elif c == 0:
                kept[name] = val
            else:
                dkv[kt, rows, :] += kept[name] + val

        def over_keys(c):
            k, q = spans(diag, c)
            val = widen(dot_nt(kvt[kt, :hd, k], db[buf, q, k]), 0.0)
            if c == 0:
                kept["q"] = val
            else:
                add_to(dq, first, kept["q"] + val)

        return ([functools.partial(over_queries, "v", pb, do_s, slice(hd, 2 * hd), c) for c in (0, 1)]
                + [functools.partial(over_queries, "k", db, q_s, slice(0, hd), c) for c in (0, 1)]
                + [functools.partial(over_keys, c) for c in (0, 1)])

    def backward(units, bufs, h, nxt):
        dq = [jnp.zeros((hd, cols), F32), jnp.zeros((hd, cols), F32)]
        for u in range(len(units)):
            if u + 1 < len(units):
                ahead = prob_steps(units, bufs, h, u + 1)
            else:
                ahead = prob_steps(*nxt, 0) if nxt else []
            products = grad_steps(units, bufs, h, u, dq)
            for i, step in enumerate(products):
                step()
                if i < len(ahead):
                    ahead[i]()
        return dq

    own = [(0, 0, 1, True)]
    for step in prob_steps(own, (0,), 0, 0):
        step()
    for h in range(n_heads):
        dq = [jnp.zeros((hd, cols), F32), None]
        ahead = prob_steps(own, ((h + 1) % 2,), h + 1, 0) if h < last else []
        interleave(grad_steps(own, (h % 2,), h, 0, dq), ahead)
        acc[0, h] = dq[0]
        acc[1, h] = jnp.zeros((hd, cols), F32)

    for j, c in enumerate(c_dy):
        q = slice(j * mid, (j + 1) * mid)
        c.wait_recv()
        do_s[1, :, :, q] = dot_nt(weight(w_own, "o"), dyp[q, :]).astype(BF16).reshape(n_heads, hd, mid)
    do_ready(1)
    near_bufs, far_bufs = (0, 1), (2, 3)

    def far_bwd(h, nxt):
        dq = backward(far, far_bufs, h, nxt)
        for g in (0, 1):
            acc[slots[g], h] += dq[g]

    def near_bwd(h, nxt):
        dq = backward(near_rest, near_bufs, h, nxt)
        for g in (0, 1):
            dq_s[slots[g], h] = ((dq[g] + acc[slots[g], h]) * scale).astype(BF16)
        copy(21, dq_s.at[1, h], dqg.at[h], peer).start()

    c_pair = copy(16, dkv.at[pl.ds(2 * d_far[1], 2)], rcv.at[0], partner)
    c_cross = copy(17, dkv.at[pl.ds(2 * d_far[0], 2)], rcv.at[1], at_cp(across))
    c_near = copy(18, dkv.at[pl.ds(2 * d_near, 2)], rcv.at[2], partner)

    def far_loop(h, _):
        far_bwd(h, (far, far_bufs, h + 1))

        @pl.when(h == 3)
        def _():
            c_w.wait_recv()
            c_relay[0].start()
            c_relay[1].start()

        return 0

    def near_loop(h, _):
        near_bwd(h, (near_rest, near_bufs, h + 1))

        @pl.when(h == 0)
        def _():
            c_pair.wait_recv()
            for slot in (0, 1):
                dkv[2 * d_far[0] + slot] += rcv[0, slot]

        @pl.when(h == 1)
        def _():
            c_cross.start()

        @pl.when(h == 3)
        def _():
            c_relay[1].wait_recv()
            c_relay[2].start()

        return 0

    for step in prob_steps(far, far_bufs, 0, 0):
        step()
    lax.fori_loop(0, last, far_loop, 0)
    far_bwd(last, (near_rest, near_bufs, 0))
    c_pair.start()
    lax.fori_loop(0, last, near_loop, 0)
    near_bwd(last, None)
    c_near.start()

    stores = []

    def leave(src, dst):
        c = pltpu.make_async_copy(src, dst, local.at[6 + len(stores)])
        c.start()
        stores.append(c)

    for c in column_blocks(dy_s.shape[1]):
        g = go_f[:, c] + dot(o_s[1].reshape(hw, cols), dyp[:, c])
        go_s[:, :, c] = g.astype(BF16).reshape(n_heads, hd, g.shape[1])
    leave(go_s, go_ref)
    c_cross.wait_recv()
    c_near.wait_recv()
    for slot in (1, 0):
        total = dkv[slot] + rcv[1, slot] + rcv[2, slot]
        dkvb[slot, :hd, :] = (total[:hd, :] * scale).astype(BF16)
        dkvb[slot, hd:, :] = total[hd:, :].astype(BF16)
        if slot == 1:
            c_last = copy(19, dkvb.at[1], dkvg, peer)
            c_last.start()
    for c in column_blocks(x_s.shape[1]):
        g = dot(dq_s[0].reshape(hw, cols), x_s[:, c]) + dot(dq_s[1].reshape(hw, cols), xp[:, c])
        gq_s[:, :, c] = g.astype(BF16).reshape(n_heads, hd, g.shape[1])
    leave(gq_s, gq_ref)
    gkv_s[...] = (dot(dkvb[0], x_s[...]) + dot(dkvb[1], xp[...])).astype(BF16)
    leave(gkv_s.at[:hd], gk_ref)
    leave(gkv_s.at[hd:], gv_ref)
    c_o = copy(20, o_s.at[1], og, peer)
    c_o.wait_recv()
    c_relay[0].wait_recv()
    c_relay[2].wait_recv()
    rows = 256
    for i in range(cols // rows):
        blk = slice(i * rows, (i + 1) * rows)
        y = (dot_tn(o_s[0, :, :, blk].reshape(hw, rows), weight(w_own, "o"))
             + dot_tn(og[:, :, blk].reshape(hw, rows), weight(w_peer, "o")))
        y_s[blk, :] = y.astype(BF16)
    leave(y_s, y_ref)
    c_dq = copy(21, dq_s.at[1], dqg, peer)
    c_dq.wait_recv()
    for i in range(cols // rows):
        blk = slice(i * rows, (i + 1) * rows)
        dx = (dot_tn(dq_s[0, :, :, blk].reshape(hw, rows), weight(w_own, "q"))
              + dot_tn(dqg[:, :, blk].reshape(hw, rows), weight(w_peer, "q")))
        dx += dot_tn(dkvb[0, :hd, blk], weight(w_own, "k")) + dot_tn(dkvb[0, hd:, blk], weight(w_own, "v"))
        dx_f[blk, :] = dx
    c_last.wait_recv()
    for i in range(cols // rows):
        blk = slice(i * rows, (i + 1) * rows)
        dx = dx_f[blk, :] + dot_tn(dkvg[:hd, blk], weight(w_peer, "k")) + dot_tn(dkvg[hd:, blk], weight(w_peer, "v"))
        dx_s[blk, :] = dx.astype(BF16)
    leave(dx_s, dx_ref)
    for c in c_x + c_dy + [c_o, c_dq, c_last, c_w, c_pair, c_cross, c_near] + c_relay + c_kv:
        c.wait_send()
    for c in stores:
        c.wait()


def hand_out(n, *refs):
    src, dst, held, sems = refs[:n], refs[n:2 * n], refs[2 * n:3 * n], refs[3 * n]
    loads = [pltpu.make_async_copy(src[i], held[i], sems.at[0, i]) for i in range(n)]
    stores = [pltpu.make_async_copy(held[i], dst[i], sems.at[1, i]) for i in range(n)]
    for c in loads:
        c.start()
    for load, store in zip(loads, stores):
        load.wait()
        store.start()
    for c in stores:
        c.wait()


def solution(mesh):
    shards = mesh.shape["cp"]

    def device_fn(x_own, w_query, w_key, w_value, w_out, dy_own):
        model, n_heads, hd = w_query.shape
        cols = x_own.shape[0]
        hw = n_heads * hd
        scale = hd ** -0.5
        wq = w_query.transpose(1, 2, 0).reshape(shards, hw // shards, model)
        wk = w_key.transpose(1, 2, 0).reshape(shards, hd // shards, model)
        wv = w_value.transpose(1, 2, 0).reshape(shards, hd // shards, model)
        wo = w_out.reshape(shards, hw // shards, model)
        per_head = (2, n_heads, hd, cols)
        b = lambda *s: pltpu.VMEM(s, BF16)
        f = lambda *s: pltpu.VMEM(s, F32)
        area = n_heads * 9 * cols * cols
        y, dx, gq, gk, gv, go = pl.pallas_call(
            functools.partial(kernel, shards, n_heads, hd, scale * math.log2(math.e), scale),
            out_shape=(jax.ShapeDtypeStruct((cols, model), BF16), jax.ShapeDtypeStruct((cols, model), BF16),
                       jax.ShapeDtypeStruct((n_heads, hd, model), BF16), jax.ShapeDtypeStruct((hd, model), BF16),
                       jax.ShapeDtypeStruct((hd, model), BF16), jax.ShapeDtypeStruct((n_heads, hd, model), BF16)),
            in_specs=[HBM] * 6,
            out_specs=(ANY,) * 6,
            scratch_shapes=[b(cols, model)] * 4 + [b(shards, 2 * (hw + hd) // shards, model)] * 2
            + [b(*per_head), b(*per_head), b(*per_head), b(*per_head[1:]), b(*per_head), b(*per_head[1:]),
               b(2 * shards, 2 * hd, cols), b(2 * shards, cols, hd), b(2 * shards, 2, hd + PAD, cols),
               b(2, n_heads, cols, hd + PAD), b(2, n_heads, cols, hd + PAD), f(*per_head),
               f(2, n_heads, 1, cols), f(2, n_heads, 8, cols), f(2, 1, cols),
               f(8, cols, cols), b(4, cols, cols), b(4, cols, cols), f(2 * shards, 2 * hd, cols),
               f(shards - 1, 2, 2 * hd, cols), b(2, 2 * hd, cols), b(2 * hd, cols),
               b(cols, model), b(cols, model), f(cols, model), b(n_heads, hd, model), b(2 * hd, model), b(n_heads, hd, model), f(hw, model),
               pltpu.SemaphoreType.DMA((N_COPIES,)), pltpu.SemaphoreType.DMA((N_COPIES,)), pltpu.SemaphoreType.DMA((12,))],
            compiler_params=pltpu.CompilerParams(vmem_limit_bytes=VMEM_LIMIT, collective_id=0, has_side_effects=True),
            cost_estimate=pl.CostEstimate(flops=area * 7 * 2 * hd, bytes_accessed=16 << 20, transcendentals=2 * area),
            name="attention",
        )(x_own, dy_own, wq, wk, wv, wo)
        outs = (y, dx, gq, gk, gv, go)
        y, dx, gq, gk, gv, go = pl.pallas_call(
            functools.partial(hand_out, len(outs)),
            out_shape=tuple(jax.ShapeDtypeStruct(o.shape, o.dtype) for o in outs),
            in_specs=[HBM] * len(outs),
            out_specs=(HBM,) * len(outs),
            scratch_shapes=[pltpu.VMEM(o.shape, o.dtype) for o in outs] + [pltpu.SemaphoreType.DMA((2, len(outs)))],
            cost_estimate=pl.CostEstimate(flops=0, bytes_accessed=8 << 20, transcendentals=0),
            name="hand_out",
        )(*outs)
        back = lambda g, n: g.reshape(n, hd, model).transpose(2, 0, 1)[None]
        return y, dx, back(gq, n_heads), back(gk, 1), back(gv, 1), go[None]

    return jax.shard_map(device_fn, mesh=mesh,
                         in_specs=(ROW_SPEC, HEAD_SPEC, HEAD_SPEC, HEAD_SPEC, OUT_W_SPEC, ROW_SPEC),
                         out_specs=(ROW_SPEC, ROW_SPEC, GRAD_SPEC, GRAD_SPEC, GRAD_SPEC, GRAD_OUT_SPEC),
                         check_vma=False)
```

```python
import functools
import math

import jax
import jax.numpy as jnp
from jax import lax
from jax.experimental import pallas as pl
from jax.experimental.pallas import tpu as pltpu
from jax.sharding import PartitionSpec as P

ROW_SPEC = P(("dp", "cp", "tp"), None)
HEAD_SPEC = P(None, "tp", None)
OUT_W_SPEC = P("tp", None, None)
GRAD_SPEC = P(("dp", "cp"), None, "tp", None)
GRAD_OUT_SPEC = P(("dp", "cp"), "tp", None, None)
F32 = jnp.float32
BF16 = jnp.bfloat16
NT = (((1,), (1,)), ((), ()))
TN = (((0,), (0,)), ((), ()))
ANY = pl.BlockSpec(memory_space=pl.ANY)
HBM = pl.BlockSpec(memory_space=pltpu.HBM)
VMEM_LIMIT = 64 * 1024 * 1024 - 64 * 1024
N_COPIES = 24
PAD = 16
BIG = 3.0e38


def dot(a, b):
    return jnp.dot(a, b, preferred_element_type=F32)


def dot_nt(a, b):
    return lax.dot_general(a, b, NT, preferred_element_type=F32)


def dot_tn(a, b):
    return lax.dot_general(a, b, TN, preferred_element_type=F32)


def shard_units(rank, half, d, shards):
    early = (rank + shards - d) // shards
    slot = early * half + (1 - early) * (1 - half)
    return [(slot, 2 * d + half, early, False), (1 - half, 2 * d + slot, 0, False)]


def diag_mask(size):
    return lax.broadcasted_iota(jnp.int32, (size, size), 1) >= lax.broadcasted_iota(jnp.int32, (size, size), 0)


def pick(first, pair):
    if isinstance(first, int):
        return pair[1 - first]
    return jnp.where(first == 1, pair[0], pair[1])


def add_to(pair, first, value):
    if isinstance(first, int):
        pair[1 - first] = pair[1 - first] + value
    else:
        pair[0] = pair[0] + jnp.where(first == 1, value, 0.0)
        pair[1] = pair[1] + jnp.where(first == 1, 0.0, value)


def transpose_bf16(x):
    return x.astype(F32).T.astype(BF16)


def with_columns(x_t, row):
    hi = jnp.clip(row, -BIG, BIG).astype(BF16).astype(F32)
    mid = (row - hi).astype(BF16).astype(F32)
    low = row - hi - mid
    line = lax.broadcasted_iota(jnp.int32, (PAD, row.shape[1]), 0)
    extra = jnp.where(line == 0, hi, jnp.where(line == 1, mid, jnp.where(line == 2, low, 0.0)))
    return jnp.concatenate([x_t.astype(F32), extra], axis=0).T.astype(BF16)


def kernel(shards, n_heads, hd, c_scale, scale,
           x_hbm, dy_hbm, wq_hbm, wk_hbm, wv_hbm, wo_hbm,
           y_ref, dx_ref, gq_ref, gk_ref, gv_ref, go_ref,
           x_s, xp, dy_s, dyp, w_own, w_peer,
           q_s, do_s, o_s, og, dq_s, dqg, kvt, k_s, ka, q_n, do_n, acc, m_s, l_s, max_s, s_s, pb, db, dkv, rcv, dkvb, dkvg,
           y_s, dx_s, dx_f, gq_s, gkv_s, go_s, go_f, send, recv, local):
    rank = lax.axis_index("cp")
    half = lax.axis_index("tp")
    core = rank % 2
    cols = q_s.shape[-1]
    hw = n_heads * hd
    peer = {"tp": 1 - half}
    partner = {"cp": rank + 1 - 2 * core}

    d_near = shards - 1 - 2 * core
    d_far = (2, 1 + 2 * core)

    def at_cp(i):
        return {"cp": i % shards}

    def copy(i, src, dst, device):
        return pltpu.make_async_remote_copy(src_ref=src, dst_ref=dst, send_sem=send.at[i], recv_sem=recv.at[i],
                                            device_id=device, device_id_type=pl.DeviceIdType.MESH)

    n_o, n_k = hw // shards, hd // shards
    w_rows = {"o": (0, n_o), "q": (n_o, n_o), "k": (2 * n_o, n_k), "v": (2 * n_o + n_k, n_k)}

    def load(i, src, name):
        start, size = w_rows[name]
        return pltpu.make_async_copy(src, w_own.at[:, pl.ds(start, size), :], local.at[i])

    def weight(ref, name):
        start, size = w_rows[name]
        return ref[:, start:start + size, :].reshape(shards * size, ref.shape[2])

    loads = [pltpu.make_async_copy(x_hbm, x_s, local.at[0]), load(1, wk_hbm, "k"), load(2, wv_hbm, "v"), load(3, wq_hbm, "q"),
             load(4, wo_hbm, "o"), pltpu.make_async_copy(dy_hbm, dy_s, local.at[5])]
    for c in loads:
        c.start()
    barrier = pltpu.get_barrier_semaphore()
    pl.semaphore_signal(barrier, inc=1, device_id=peer, device_id_type=pl.DeviceIdType.MESH)
    for d in range(1, shards):
        pl.semaphore_signal(barrier, inc=1, device_id=at_cp(rank + d), device_id_type=pl.DeviceIdType.MESH)
    pl.semaphore_wait(barrier, shards)

    across = (rank + 2) % shards
    mid = cols // 2
    c_x = [copy(i, x_hbm.at[pl.ds(j * mid, mid)], xp.at[pl.ds(j * mid, mid)], peer) for i, j in ((0, 0), (22, 1))]
    c_dy = [copy(i, dy_hbm.at[pl.ds(j * mid, mid)], dyp.at[pl.ds(j * mid, mid)], peer) for i, j in ((1, 0), (23, 1))]
    c_w = copy(2, w_own.at[rank], w_peer.at[rank], peer)
    c_relay = [copy(3, w_peer.at[rank], w_peer.at[rank], partner), copy(4, w_peer.at[rank], w_peer.at[rank], at_cp(across)),
               copy(5, w_peer.at[across], w_peer.at[across], partner)]
    for c in c_x + c_dy:
        c.start()

    def send_kv(slot):
        ahead = (2, shards - 1 - 2 * core, 1 + 2 * core)
        cs = [copy(10 + 3 * slot + i, kvt.at[slot], kvt.at[2 * d + slot], at_cp(rank + d)) for i, d in enumerate(ahead)]
        for c in cs:
            c.start()
        return cs

    def keys_ready(tile):
        k_s[tile] = transpose_bf16(kvt[tile, :hd, :])
        minus = jnp.where(lax.broadcasted_iota(jnp.int32, (PAD, cols), 0) < 3, -1.0, 0.0).astype(BF16)
        for i in (0, 1):
            ka[tile, i, :hd, :] = kvt[tile, i * hd:(i + 1) * hd, :]
            ka[tile, i, hd:, :] = minus

    for c in loads[:3]:
        c.wait()
    kvt[0, :hd, :] = dot_nt(weight(w_own, "k"), x_s[...]).astype(BF16)
    kvt[0, hd:, :] = dot_nt(weight(w_own, "v"), x_s[...]).astype(BF16)
    c_kv = send_kv(0)
    loads[3].wait()
    q_s[0] = dot_nt(weight(w_own, "q"), x_s[...]).astype(BF16).reshape(n_heads, hd, cols)
    loads[4].wait()
    c_w.start()
    loads[5].wait()
    do_s[0] = dot_nt(weight(w_own, "o"), dy_s[...]).astype(BF16).reshape(n_heads, hd, cols)
    keys_ready(0)
    part = cols // 2
    triangle = diag_mask(part)

    def own_diagonal(h, _):
        s0 = dot(k_s[0, :part], q_s[0, h])
        s0 = jnp.concatenate([jnp.where(triangle, s0[:, :part], -jnp.inf), s0[:, part:]], axis=1)
        s1 = jnp.where(triangle, dot(k_s[0, part:], q_s[0, h, :, part:]), -jnp.inf)
        m0, m1 = jnp.max(s0, axis=0, keepdims=True), jnp.max(s1, axis=0, keepdims=True)
        m = jnp.concatenate([m0[:, :part], jnp.maximum(m0[:, part:], m1)], axis=1) * c_scale
        p0, p1 = jnp.exp2(s0 * c_scale - m), jnp.exp2(s1 * c_scale - m[:, part:])
        zeros = jnp.zeros((8, part), F32)
        l_s[0, h] = (jnp.sum(p0.reshape(part // 8, 8, cols), axis=0)
                     + jnp.concatenate([zeros, jnp.sum(p1.reshape(part // 8, 8, part), axis=0)], axis=1))
        o1 = dot(kvt[0, hd:, part:], p1.astype(BF16))
        acc[0, h] = dot(kvt[0, hd:, :part], p0.astype(BF16)) + jnp.concatenate([jnp.zeros_like(o1), o1], axis=1)
        m_s[0, h] = m
        m_s[1, h] = jnp.full_like(m, -jnp.inf)
        l_s[1, h] = jnp.zeros((8, cols), F32)
        acc[1, h] = jnp.zeros((hd, cols), F32)
        return 0

    lax.fori_loop(0, n_heads, own_diagonal, 0)
    for j, c in enumerate(c_x):
        q = slice(j * mid, (j + 1) * mid)
        c.wait_recv()
        kvt[1, :hd, q] = dot_nt(weight(w_own, "k"), xp[q, :]).astype(BF16)
        kvt[1, hd:, q] = dot_nt(weight(w_own, "v"), xp[q, :]).astype(BF16)
        if j == 1:
            c_kv += send_kv(1)
        q_s[1, :, :, q] = dot_nt(weight(w_own, "q"), xp[q, :]).astype(BF16).reshape(n_heads, hd, mid)
    keys_ready(1)

    near = ([(half, half, 1, True), (1 - half, half, 0, False), (1 - half, 1 - half, 0, True)]
            + shard_units(rank, half, d_near, shards))
    far = shard_units(rank, half, d_far[0], shards) + shard_units(rank, half, d_far[1], shards)
    slots = (half, 1 - half)
    near_fwd_units = [(1, 1, half, True)] + near[1:2] + near[3:]

    def spans(diag, c):
        return slice(c * part, (c + 1) * part), slice(c * part, cols) if diag else slice(0, cols)

    def masked(x, diag, fill):
        if not diag:
            return x
        left = jnp.where(triangle, x[:, :part], fill)
        return left if x.shape[1] == part else jnp.concatenate([left, x[:, part:]], axis=1)

    def widen(x, fill):
        if x.shape[1] == cols:
            return x
        return jnp.concatenate([jnp.full((x.shape[0], cols - x.shape[1]), fill, x.dtype), x], axis=1)

    def interleave(first_list, second_list):
        i = j = 0
        while i < len(first_list) or j < len(second_list):
            if j >= len(second_list) or (i < len(first_list) and i * len(second_list) <= j * len(first_list)):
                first_list[i]()
                i += 1
            else:
                second_list[j]()
                j += 1

    def score_steps(units, base, h, maxes):
        def step(u, c):
            qi, kt, first, diag = units[u]
            r, q = spans(diag, c)
            s = masked(dot(k_s[kt, r], q_s[qi, h, :, q]), diag, -jnp.inf)
            s_s[base + u, r, q] = s
            mx = widen(jnp.max(s.reshape(part // 8, 8, s.shape[1]), axis=0), -jnp.inf)
            maxes[u] = mx if c == 0 else jnp.maximum(maxes[u], mx)
        return [functools.partial(step, u, c) for u in range(len(units)) for c in (0, 1)]

    def score_max(units, maxes):
        for g in (0, 1):
            best = None
            for u, (_, _, first, _) in enumerate(units):
                if isinstance(first, int):
                    if first == g:
                        continue
                    val = maxes[u]
                else:
                    val = jnp.where(first == 1 - g, maxes[u], -jnp.inf)
                best = val if best is None else jnp.maximum(best, val)
            max_s[g] = jnp.max(best, axis=0, keepdims=True) * c_scale

    def attend_steps(units, base, h, is_near):
        old = [m_s[slots[g], h] for g in (0, 1)]
        m = [jnp.maximum(max_s[g], old[g]) for g in (0, 1)]
        fix = [jnp.exp2(x - y) for x, y in zip(old, m)]
        l = [l_s[slots[g], h] * fix[g] for g in (0, 1)]
        o = [acc[slots[g], h] * fix[g] for g in (0, 1)]
        sums = {}

        def step(u, c):
            qi, kt, first, diag = units[u]
            r, q = spans(diag, c)
            p = jnp.exp2(s_s[base + u, r, q] * c_scale - pick(first, m)[:, q])
            l_u = widen(jnp.sum(p.reshape(part // 8, 8, p.shape[1]), axis=0), 0.0)
            o_u = widen(dot(kvt[kt, hd:, r], p.astype(BF16)), 0.0)
            if c == 0:
                sums[u] = (l_u, o_u)
            else:
                add_to(l, first, sums[u][0] + l_u)
                add_to(o, first, sums[u][1] + o_u)

        def finish():
            for g in (0, 1):
                if is_near:
                    m_s[slots[g], h] = m[g]
                    l_s[slots[g], h] = l[g]
                    acc[slots[g], h] = o[g]
                else:
                    l_row = jnp.sum(l[g], axis=0, keepdims=True)
                    o_s[slots[g], h] = (o[g] / l_row).astype(BF16)
                    q_n[slots[g], h] = with_columns(q_s[slots[g], h], (m[g] + jnp.log2(l_row)) * (1.0 / c_scale))

        return [functools.partial(step, u, c) for u in range(len(units)) for c in (0, 1)], finish

    def forward(units, base, h, is_near, nxt):
        steps, finish = attend_steps(units, base, h, is_near)
        maxes = {}
        following = score_steps(*nxt, maxes) if nxt else []
        interleave(steps, following)
        finish()
        if nxt:
            score_max(nxt[0], maxes)

    def send_o(h):
        copy(20, o_s.at[1, h], og.at[h], peer).start()

    def near_fwd(h, _):
        forward(near_fwd_units, 4, h, True, (near_fwd_units, 4, h + 1))
        return 0

    def far_fwd(h, _):
        forward(far, 0, h, False, (far, 0, h + 1))
        send_o(h)
        return 0

    last = n_heads - 1
    maxes = {}
    for c in (c_kv[2], c_kv[5]):
        c.wait_recv()
    keys_ready(2 * d_near)
    keys_ready(2 * d_near + 1)
    for step in score_steps(near_fwd_units, 4, 0, maxes):
        step()
    score_max(near_fwd_units, maxes)
    lax.fori_loop(0, last, near_fwd, 0)
    for c in (c_kv[0], c_kv[1], c_kv[3], c_kv[4]):
        c.wait_recv()
    for d in d_far:
        keys_ready(2 * d)
        keys_ready(2 * d + 1)
    forward(near_fwd_units, 4, last, True, (far, 0, 0))
    lax.fori_loop(0, last, far_fwd, 0)
    forward(far, 0, last, False, None)
    send_o(last)
    dkv[...] = jnp.zeros_like(dkv)

    def do_ready(i):
        for h in range(n_heads):
            delta = jnp.sum(do_s[i, h].astype(F32) * o_s[i, h].astype(F32), axis=0, keepdims=True)
            do_n[i, h] = with_columns(do_s[i, h], delta)

    def column_blocks(width):
        return [slice(start, min(start + 256, width)) for start in range(0, width, 256)]

    do_ready(0)
    for c in column_blocks(dy_s.shape[1]):
        go_f[:, c] = dot(o_s[0].reshape(hw, cols), dy_s[:, c])
    for j, c in enumerate(c_dy):
        q = slice(j * mid, (j + 1) * mid)
        c.wait_recv()
        do_s[1, :, :, q] = dot_nt(weight(w_own, "o"), dyp[q, :]).astype(BF16).reshape(n_heads, hd, mid)
    do_ready(1)
    lower = lax.broadcasted_iota(jnp.int32, (part, part), 0) >= lax.broadcasted_iota(jnp.int32, (part, part), 1)

    def prob_steps(units, bufs, h, u):
        qi, kt, first, diag = units[u]
        buf = bufs[u % len(bufs)]
        kept = {}

        def probs(c):
            r, k = slice(c * part, (c + 1) * part), slice(0, part if diag and c == 0 else cols)
            p = jnp.exp2(dot(q_n[qi, h, r], ka[kt, 0, :, k]) * c_scale)
            if diag:
                p = jnp.concatenate([p[:, :c * part], jnp.where(lower, p[:, c * part:], 0.0)], axis=1) if c else jnp.where(lower, p, 0.0)
            pb[buf, r, k] = p.astype(BF16)
            kept[c] = p

        def grads(c):
            r, k = slice(c * part, (c + 1) * part), slice(0, part if diag and c == 0 else cols)
            db[buf, r, k] = (kept[c] * dot(do_n[qi, h, r], ka[kt, 1, :, k])).astype(BF16)

        return [functools.partial(f, c) for c in (0, 1) for f in (probs, grads)]

    def grad_steps(units, bufs, h, u, dq):
        qi, kt, first, diag = units[u]
        buf = bufs[u % len(bufs)]
        kept = {}

        def over_queries(name, src, lhs, rows, c):
            q, k = slice(c * part, (c + 1) * part), slice(0, part if diag and c == 0 else cols)
            val = dot(lhs[qi, h, :, q], src[buf, q, k])
            if diag:
                dkv[kt, rows, k] += val
            elif c == 0:
                kept[name] = val
            else:
                dkv[kt, rows, :] += kept[name] + val

        def over_keys(c):
            k, q = spans(diag, c)
            val = widen(dot_nt(kvt[kt, :hd, k], db[buf, q, k]), 0.0)
            if c == 0:
                kept["q"] = val
            else:
                add_to(dq, first, kept["q"] + val)

        return ([functools.partial(over_queries, "v", pb, do_s, slice(hd, 2 * hd), c) for c in (0, 1)]
                + [functools.partial(over_queries, "k", db, q_s, slice(0, hd), c) for c in (0, 1)]
                + [functools.partial(over_keys, c) for c in (0, 1)])

    def backward(units, bufs, h, nxt):
        dq = [jnp.zeros((hd, cols), F32), jnp.zeros((hd, cols), F32)]
        for u in range(len(units)):
            if u + 1 < len(units):
                ahead = prob_steps(units, bufs, h, u + 1)
            else:
                ahead = prob_steps(*nxt, 0) if nxt else []
            products = grad_steps(units, bufs, h, u, dq)
            for i, step in enumerate(products):
                step()
                if i < len(ahead):
                    ahead[i]()
        return dq

    near_bufs, far_bufs = (0, 1, 2), (3, 4)

    def far_bwd(h, nxt):
        dq = backward(far, far_bufs, h, nxt)
        for g in (0, 1):
            acc[slots[g], h] = dq[g]

    def near_bwd(h, nxt):
        dq = backward(near, near_bufs, h, nxt)
        for g in (0, 1):
            dq_s[slots[g], h] = ((dq[g] + acc[slots[g], h]) * scale).astype(BF16)
        copy(21, dq_s.at[1, h], dqg.at[h], peer).start()

    c_pair = copy(16, dkv.at[pl.ds(2 * d_far[1], 2)], rcv.at[0], partner)
    c_cross = copy(17, dkv.at[pl.ds(2 * d_far[0], 2)], rcv.at[1], at_cp(across))
    c_near = copy(18, dkv.at[pl.ds(2 * d_near, 2)], rcv.at[2], partner)

    def far_loop(h, _):
        far_bwd(h, (far, far_bufs, h + 1))

        @pl.when(h == 3)
        def _():
            c_w.wait_recv()
            c_relay[0].start()
            c_relay[1].start()

        return 0

    def near_loop(h, _):
        near_bwd(h, (near, near_bufs, h + 1))

        @pl.when(h == 0)
        def _():
            c_pair.wait_recv()
            for slot in (0, 1):
                dkv[2 * d_far[0] + slot] += rcv[0, slot]

        @pl.when(h == 1)
        def _():
            c_cross.start()

        @pl.when(h == 3)
        def _():
            c_relay[1].wait_recv()
            c_relay[2].start()

        return 0

    for step in prob_steps(far, far_bufs, 0, 0):
        step()
    lax.fori_loop(0, last, far_loop, 0)
    far_bwd(last, (near, near_bufs, 0))
    c_pair.start()
    lax.fori_loop(0, last, near_loop, 0)
    near_bwd(last, None)
    c_near.start()

    stores = []

    def leave(src, dst):
        c = pltpu.make_async_copy(src, dst, local.at[6 + len(stores)])
        c.start()
        stores.append(c)

    for c in column_blocks(dy_s.shape[1]):
        g = go_f[:, c] + dot(o_s[1].reshape(hw, cols), dyp[:, c])
        go_s[:, :, c] = g.astype(BF16).reshape(n_heads, hd, g.shape[1])
    leave(go_s, go_ref)
    c_cross.wait_recv()
    c_near.wait_recv()
    for slot in (1, 0):
        total = dkv[slot] + rcv[1, slot] + rcv[2, slot]
        dkvb[slot, :hd, :] = (total[:hd, :] * scale).astype(BF16)
        dkvb[slot, hd:, :] = total[hd:, :].astype(BF16)
        if slot == 1:
            c_last = copy(19, dkvb.at[1], dkvg, peer)
            c_last.start()
    for c in column_blocks(x_s.shape[1]):
        g = dot(dq_s[0].reshape(hw, cols), x_s[:, c]) + dot(dq_s[1].reshape(hw, cols), xp[:, c])
        gq_s[:, :, c] = g.astype(BF16).reshape(n_heads, hd, g.shape[1])
    leave(gq_s, gq_ref)
    gkv_s[...] = (dot(dkvb[0], x_s[...]) + dot(dkvb[1], xp[...])).astype(BF16)
    leave(gkv_s.at[:hd], gk_ref)
    leave(gkv_s.at[hd:], gv_ref)
    c_o = copy(20, o_s.at[1], og, peer)
    c_o.wait_recv()
    c_relay[0].wait_recv()
    c_relay[2].wait_recv()
    rows = 256
    for i in range(cols // rows):
        blk = slice(i * rows, (i + 1) * rows)
        y = (dot_tn(o_s[0, :, :, blk].reshape(hw, rows), weight(w_own, "o"))
             + dot_tn(og[:, :, blk].reshape(hw, rows), weight(w_peer, "o")))
        y_s[blk, :] = y.astype(BF16)
    leave(y_s, y_ref)
    c_dq = copy(21, dq_s.at[1], dqg, peer)
    c_dq.wait_recv()
    for i in range(cols // rows):
        blk = slice(i * rows, (i + 1) * rows)
        dx = (dot_tn(dq_s[0, :, :, blk].reshape(hw, rows), weight(w_own, "q"))
              + dot_tn(dqg[:, :, blk].reshape(hw, rows), weight(w_peer, "q")))
        dx += dot_tn(dkvb[0, :hd, blk], weight(w_own, "k")) + dot_tn(dkvb[0, hd:, blk], weight(w_own, "v"))
        dx_f[blk, :] = dx
    c_last.wait_recv()
    for i in range(cols // rows):
        blk = slice(i * rows, (i + 1) * rows)
        dx = dx_f[blk, :] + dot_tn(dkvg[:hd, blk], weight(w_peer, "k")) + dot_tn(dkvg[hd:, blk], weight(w_peer, "v"))
        dx_s[blk, :] = dx.astype(BF16)
        leave(dx_s.at[blk], dx_ref.at[blk])
    for c in c_x + c_dy + [c_o, c_dq, c_last, c_w, c_pair, c_cross, c_near] + c_relay + c_kv:
        c.wait_send()
    for c in stores:
        c.wait()


def hand_out(n, pieces, *refs):
    src, dst, held, sems = refs[:n], refs[n:2 * n], refs[2 * n:3 * n], refs[3 * n]
    loads, stores = [], []
    for j, (i, start, size) in enumerate(pieces):
        rows = pl.ds(start, size)
        loads.append(pltpu.make_async_copy(src[i].at[rows], held[i].at[rows], sems.at[0, j]))
        stores.append(pltpu.make_async_copy(held[i].at[rows], dst[i].at[rows], sems.at[1, j]))
    for c in loads:
        c.start()
    for load, store in zip(loads, stores):
        load.wait()
        store.start()
    for c in stores:
        c.wait()


def cut(shapes, most):
    pieces = []
    for i, shape in enumerate(shapes):
        step = max(1, most // (2 * math.prod(shape[1:])))
        pieces += [(i, start, min(step, shape[0] - start)) for start in range(0, shape[0], step)]
    return pieces


def solution(mesh):
    shards = mesh.shape["cp"]

    def device_fn(x_own, w_query, w_key, w_value, w_out, dy_own):
        model, n_heads, hd = w_query.shape
        cols = x_own.shape[0]
        hw = n_heads * hd
        scale = hd ** -0.5
        wq = w_query.transpose(1, 2, 0).reshape(shards, hw // shards, model)
        wk = w_key.transpose(1, 2, 0).reshape(shards, hd // shards, model)
        wv = w_value.transpose(1, 2, 0).reshape(shards, hd // shards, model)
        wo = w_out.reshape(shards, hw // shards, model)
        per_head = (2, n_heads, hd, cols)
        b = lambda *s: pltpu.VMEM(s, BF16)
        f = lambda *s: pltpu.VMEM(s, F32)
        area = n_heads * 9 * cols * cols
        y, dx, gq, gk, gv, go = pl.pallas_call(
            functools.partial(kernel, shards, n_heads, hd, scale * math.log2(math.e), scale),
            out_shape=(jax.ShapeDtypeStruct((cols, model), BF16), jax.ShapeDtypeStruct((cols, model), BF16),
                       jax.ShapeDtypeStruct((n_heads, hd, model), BF16), jax.ShapeDtypeStruct((hd, model), BF16),
                       jax.ShapeDtypeStruct((hd, model), BF16), jax.ShapeDtypeStruct((n_heads, hd, model), BF16)),
            in_specs=[HBM] * 6,
            out_specs=(ANY,) * 6,
            scratch_shapes=[b(cols, model)] * 4 + [b(shards, 2 * (hw + hd) // shards, model)] * 2
            + [b(*per_head), b(*per_head), b(*per_head), b(*per_head[1:]), b(*per_head), b(*per_head[1:]),
               b(2 * shards, 2 * hd, cols), b(2 * shards, cols, hd), b(2 * shards, 2, hd + PAD, cols),
               b(2, n_heads, cols, hd + PAD), b(2, n_heads, cols, hd + PAD), f(*per_head),
               f(2, n_heads, 1, cols), f(2, n_heads, 8, cols), f(2, 1, cols),
               f(8, cols, cols), b(5, cols, cols), b(5, cols, cols), f(2 * shards, 2 * hd, cols),
               f(shards - 1, 2, 2 * hd, cols), b(2, 2 * hd, cols), b(2 * hd, cols),
               b(cols, model), b(cols, model), f(cols, model), b(n_heads, hd, model), b(2 * hd, model), b(n_heads, hd, model), f(hw, model),
               pltpu.SemaphoreType.DMA((N_COPIES,)), pltpu.SemaphoreType.DMA((N_COPIES,)), pltpu.SemaphoreType.DMA((13,))],
            compiler_params=pltpu.CompilerParams(vmem_limit_bytes=VMEM_LIMIT, collective_id=0, has_side_effects=True),
            cost_estimate=pl.CostEstimate(flops=area * 7 * 2 * hd, bytes_accessed=16 << 20, transcendentals=2 * area),
            name="attention",
        )(x_own, dy_own, wq, wk, wv, wo)
        outs = (y, dx, gq, gk, gv, go)
        pieces = cut([o.shape for o in outs], 128 * model * 2)
        y, dx, gq, gk, gv, go = pl.pallas_call(
            functools.partial(hand_out, len(outs), pieces),
            out_shape=tuple(jax.ShapeDtypeStruct(o.shape, o.dtype) for o in outs),
            in_specs=[HBM] * len(outs),
            out_specs=(HBM,) * len(outs),
            scratch_shapes=[pltpu.VMEM(o.shape, o.dtype) for o in outs] + [pltpu.SemaphoreType.DMA((2, len(pieces)))],
            cost_estimate=pl.CostEstimate(flops=0, bytes_accessed=8 << 20, transcendentals=0),
            name="hand_out",
        )(*outs)
        back = lambda g, n: g.reshape(n, hd, model).transpose(2, 0, 1)[None]
        return y, dx, back(gq, n_heads), back(gk, 1), back(gv, 1), go[None]

    return jax.shard_map(device_fn, mesh=mesh,
                         in_specs=(ROW_SPEC, HEAD_SPEC, HEAD_SPEC, HEAD_SPEC, OUT_W_SPEC, ROW_SPEC),
                         out_specs=(ROW_SPEC, ROW_SPEC, GRAD_SPEC, GRAD_SPEC, GRAD_SPEC, GRAD_OUT_SPEC),
                         check_vma=False)
```

```python
import functools
import math

import jax
import jax.numpy as jnp
from jax import lax
from jax.experimental import pallas as pl
from jax.experimental.pallas import tpu as pltpu
from jax.sharding import PartitionSpec as P

ROW_SPEC = P(("dp", "cp", "tp"), None)
HEAD_SPEC = P(None, "tp", None)
OUT_W_SPEC = P("tp", None, None)
GRAD_SPEC = P(("dp", "cp"), None, "tp", None)
GRAD_OUT_SPEC = P(("dp", "cp"), "tp", None, None)
F32 = jnp.float32
BF16 = jnp.bfloat16
NT = (((1,), (1,)), ((), ()))
TN = (((0,), (0,)), ((), ()))
ANY = pl.BlockSpec(memory_space=pl.ANY)
HBM = pl.BlockSpec(memory_space=pltpu.HBM)
VMEM_LIMIT = 64 * 1024 * 1024 - 64 * 1024
N_COPIES = 24
PAD = 16
BIG = 3.0e38


def dot(a, b):
    return jnp.dot(a, b, preferred_element_type=F32)


def dot_nt(a, b):
    return lax.dot_general(a, b, NT, preferred_element_type=F32)


def dot_tn(a, b):
    return lax.dot_general(a, b, TN, preferred_element_type=F32)


def shard_units(rank, half, d, shards):
    early = (rank + shards - d) // shards
    slot = early * half + (1 - early) * (1 - half)
    return [(slot, 2 * d + half, early, False), (1 - half, 2 * d + slot, 0, False)]


def diag_mask(size):
    return lax.broadcasted_iota(jnp.int32, (size, size), 1) >= lax.broadcasted_iota(jnp.int32, (size, size), 0)


def pick(first, pair):
    if isinstance(first, int):
        return pair[1 - first]
    return jnp.where(first == 1, pair[0], pair[1])


def add_to(pair, first, value):
    if isinstance(first, int):
        pair[1 - first] = pair[1 - first] + value
    else:
        pair[0] = pair[0] + jnp.where(first == 1, value, 0.0)
        pair[1] = pair[1] + jnp.where(first == 1, 0.0, value)


def transpose_bf16(x):
    return x.astype(F32).T.astype(BF16)


def with_columns(x_t, row):
    hi = jnp.clip(row, -BIG, BIG).astype(BF16).astype(F32)
    mid = (row - hi).astype(BF16).astype(F32)
    low = row - hi - mid
    line = lax.broadcasted_iota(jnp.int32, (PAD, row.shape[1]), 0)
    extra = jnp.where(line == 0, hi, jnp.where(line == 1, mid, jnp.where(line == 2, low, 0.0)))
    return jnp.concatenate([x_t.astype(F32), extra], axis=0).T.astype(BF16)


def kernel(shards, n_heads, hd, c_scale, scale,
           x_hbm, dy_hbm, wq_hbm, wk_hbm, wv_hbm, wo_hbm,
           y_ref, dx_ref, gq_ref, gk_ref, gv_ref, go_ref,
           x_s, xp, dy_s, dyp, w_own, w_peer,
           q_s, do_s, o_s, og, dq_s, dqg, kvt, k_s, ka, q_n, do_n, acc, m_s, l_s, max_s, s_s, pb, db, dkv, rcv, dkvb, dkvg,
           y_s, dx_s, dx_f, gq_s, gkv_s, go_s, go_f, send, recv, local):
    rank = lax.axis_index("cp")
    half = lax.axis_index("tp")
    core = rank % 2
    cols = q_s.shape[-1]
    hw = n_heads * hd
    peer = {"tp": 1 - half}
    partner = {"cp": rank + 1 - 2 * core}

    d_near = shards - 1 - 2 * core
    d_far = (2, 1 + 2 * core)

    def at_cp(i):
        return {"cp": i % shards}

    def copy(i, src, dst, device):
        return pltpu.make_async_remote_copy(src_ref=src, dst_ref=dst, send_sem=send.at[i], recv_sem=recv.at[i],
                                            device_id=device, device_id_type=pl.DeviceIdType.MESH)

    n_o, n_k = hw // shards, hd // shards
    w_rows = {"o": (0, n_o), "q": (n_o, n_o), "k": (2 * n_o, n_k), "v": (2 * n_o + n_k, n_k)}

    def load(i, src, name):
        start, size = w_rows[name]
        return pltpu.make_async_copy(src, w_own.at[:, pl.ds(start, size), :], local.at[i])

    def weight(ref, name):
        start, size = w_rows[name]
        return ref[:, start:start + size, :].reshape(shards * size, ref.shape[2])

    loads = [pltpu.make_async_copy(x_hbm, x_s, local.at[0]), load(1, wk_hbm, "k"), load(2, wv_hbm, "v"), load(3, wq_hbm, "q"),
             load(4, wo_hbm, "o"), pltpu.make_async_copy(dy_hbm, dy_s, local.at[5])]
    for c in loads:
        c.start()
    barrier = pltpu.get_barrier_semaphore()
    pl.semaphore_signal(barrier, inc=1, device_id=peer, device_id_type=pl.DeviceIdType.MESH)
    for d in range(1, shards):
        pl.semaphore_signal(barrier, inc=1, device_id=at_cp(rank + d), device_id_type=pl.DeviceIdType.MESH)
    pl.semaphore_wait(barrier, shards)

    across = (rank + 2) % shards
    mid = cols // 2
    c_x = [copy(i, x_hbm.at[pl.ds(j * mid, mid)], xp.at[pl.ds(j * mid, mid)], peer) for i, j in ((0, 0), (22, 1))]
    c_dy = [copy(i, dy_hbm.at[pl.ds(j * mid, mid)], dyp.at[pl.ds(j * mid, mid)], peer) for i, j in ((1, 0), (23, 1))]
    c_w = copy(2, w_own.at[rank], w_peer.at[rank], peer)
    c_relay = [copy(3, w_peer.at[rank], w_peer.at[rank], partner), copy(4, w_peer.at[rank], w_peer.at[rank], at_cp(across)),
               copy(5, w_peer.at[across], w_peer.at[across], partner)]
    for c in c_x + c_dy:
        c.start()

    def send_kv(slot):
        ahead = (2, shards - 1 - 2 * core, 1 + 2 * core)
        cs = [copy(10 + 3 * slot + i, kvt.at[slot], kvt.at[2 * d + slot], at_cp(rank + d)) for i, d in enumerate(ahead)]
        for c in cs:
            c.start()
        return cs

    def keys_ready(tile):
        k_s[tile] = transpose_bf16(kvt[tile, :hd, :])
        minus = jnp.where(lax.broadcasted_iota(jnp.int32, (PAD, cols), 0) < 3, -1.0, 0.0).astype(BF16)
        for i in (0, 1):
            ka[tile, i, :hd, :] = kvt[tile, i * hd:(i + 1) * hd, :]
            ka[tile, i, hd:, :] = minus

    for c in loads[:3]:
        c.wait()
    kvt[0, :hd, :] = dot_nt(weight(w_own, "k"), x_s[...]).astype(BF16)
    kvt[0, hd:, :] = dot_nt(weight(w_own, "v"), x_s[...]).astype(BF16)
    c_kv = send_kv(0)
    loads[3].wait()
    q_s[0] = dot_nt(weight(w_own, "q"), x_s[...]).astype(BF16).reshape(n_heads, hd, cols)
    loads[4].wait()
    c_w.start()
    loads[5].wait()
    do_s[0] = dot_nt(weight(w_own, "o"), dy_s[...]).astype(BF16).reshape(n_heads, hd, cols)
    keys_ready(0)
    part = cols // 2
    triangle = diag_mask(part)

    def own_diagonal(h, _):
        s0 = dot(k_s[0, :part], q_s[0, h])
        s0 = jnp.concatenate([jnp.where(triangle, s0[:, :part], -jnp.inf), s0[:, part:]], axis=1)
        s1 = jnp.where(triangle, dot(k_s[0, part:], q_s[0, h, :, part:]), -jnp.inf)
        m0, m1 = jnp.max(s0, axis=0, keepdims=True), jnp.max(s1, axis=0, keepdims=True)
        m = jnp.concatenate([m0[:, :part], jnp.maximum(m0[:, part:], m1)], axis=1) * c_scale
        p0, p1 = jnp.exp2(s0 * c_scale - m), jnp.exp2(s1 * c_scale - m[:, part:])
        zeros = jnp.zeros((8, part), F32)
        l_s[0, h] = (jnp.sum(p0.reshape(part // 8, 8, cols), axis=0)
                     + jnp.concatenate([zeros, jnp.sum(p1.reshape(part // 8, 8, part), axis=0)], axis=1))
        o1 = dot(kvt[0, hd:, part:], p1.astype(BF16))
        acc[0, h] = dot(kvt[0, hd:, :part], p0.astype(BF16)) + jnp.concatenate([jnp.zeros_like(o1), o1], axis=1)
        m_s[0, h] = m
        m_s[1, h] = jnp.full_like(m, -jnp.inf)
        l_s[1, h] = jnp.zeros((8, cols), F32)
        acc[1, h] = jnp.zeros((hd, cols), F32)
        return 0

    lax.fori_loop(0, n_heads, own_diagonal, 0)
    for j, c in enumerate(c_x):
        q = slice(j * mid, (j + 1) * mid)
        c.wait_recv()
        kvt[1, :hd, q] = dot_nt(weight(w_own, "k"), xp[q, :]).astype(BF16)
        kvt[1, hd:, q] = dot_nt(weight(w_own, "v"), xp[q, :]).astype(BF16)
        if j == 1:
            c_kv += send_kv(1)
        q_s[1, :, :, q] = dot_nt(weight(w_own, "q"), xp[q, :]).astype(BF16).reshape(n_heads, hd, mid)
    keys_ready(1)

    near = ([(half, half, 1, True), (1 - half, half, 0, False), (1 - half, 1 - half, 0, True)]
            + shard_units(rank, half, d_near, shards))
    far = shard_units(rank, half, d_far[0], shards) + shard_units(rank, half, d_far[1], shards)
    slots = (half, 1 - half)
    near_fwd_units = [(1, 1, half, True)] + near[1:2] + near[3:]

    def spans(diag, c):
        return slice(c * part, (c + 1) * part), slice(c * part, cols) if diag else slice(0, cols)

    def masked(x, diag, fill):
        if not diag:
            return x
        left = jnp.where(triangle, x[:, :part], fill)
        return left if x.shape[1] == part else jnp.concatenate([left, x[:, part:]], axis=1)

    def widen(x, fill):
        if x.shape[1] == cols:
            return x
        return jnp.concatenate([jnp.full((x.shape[0], cols - x.shape[1]), fill, x.dtype), x], axis=1)

    def interleave(first_list, second_list):
        i = j = 0
        while i < len(first_list) or j < len(second_list):
            if j >= len(second_list) or (i < len(first_list) and i * len(second_list) <= j * len(first_list)):
                first_list[i]()
                i += 1
            else:
                second_list[j]()
                j += 1

    def pieces(units):
        return [(u, c) for u, unit in enumerate(units) for c in ((0, 1) if unit[3] else (None,))]

    def score_steps(units, base, h, maxes):
        def step(u, c):
            qi, kt, first, diag = units[u]
            r, q = spans(diag, c) if diag else (slice(0, cols), slice(0, cols))
            s = masked(dot(k_s[kt, r], q_s[qi, h, :, q]), diag, -jnp.inf)
            s_s[base + u, r, q] = s
            mx = widen(jnp.max(s.reshape(s.shape[0] // 8, 8, s.shape[1]), axis=0), -jnp.inf)
            maxes[u] = jnp.maximum(maxes[u], mx) if c == 1 else mx
        return [functools.partial(step, u, c) for u, c in pieces(units)]

    def score_max(units, maxes):
        for g in (0, 1):
            best = None
            for u, (_, _, first, _) in enumerate(units):
                if isinstance(first, int):
                    if first == g:
                        continue
                    val = maxes[u]
                else:
                    val = jnp.where(first == 1 - g, maxes[u], -jnp.inf)
                best = val if best is None else jnp.maximum(best, val)
            max_s[g] = jnp.max(best, axis=0, keepdims=True) * c_scale

    def attend_steps(units, base, h, is_near):
        old = [m_s[slots[g], h] for g in (0, 1)]
        m = [jnp.maximum(max_s[g], old[g]) for g in (0, 1)]
        fix = [jnp.exp2(x - y) for x, y in zip(old, m)]
        l = [l_s[slots[g], h] * fix[g] for g in (0, 1)]
        o = [acc[slots[g], h] * fix[g] for g in (0, 1)]
        sums = {}

        def step(u, c):
            qi, kt, first, diag = units[u]
            r, q = spans(diag, c) if diag else (slice(0, cols), slice(0, cols))
            p = jnp.exp2(s_s[base + u, r, q] * c_scale - pick(first, m)[:, q])
            l_u = widen(jnp.sum(p.reshape(p.shape[0] // 8, 8, p.shape[1]), axis=0), 0.0)
            o_u = widen(dot(kvt[kt, hd:, r], p.astype(BF16)), 0.0)
            if c is None:
                add_to(l, first, l_u)
                add_to(o, first, o_u)
            elif c == 0:
                sums[u] = (l_u, o_u)
            else:
                add_to(l, first, sums[u][0] + l_u)
                add_to(o, first, sums[u][1] + o_u)

        def finish():
            for g in (0, 1):
                if is_near:
                    m_s[slots[g], h] = m[g]
                    l_s[slots[g], h] = l[g]
                    acc[slots[g], h] = o[g]
                else:
                    l_row = jnp.sum(l[g], axis=0, keepdims=True)
                    o_s[slots[g], h] = (o[g] / l_row).astype(BF16)
                    q_n[slots[g], h] = with_columns(q_s[slots[g], h], (m[g] + jnp.log2(l_row)) * (1.0 / c_scale))

        return [functools.partial(step, u, c) for u, c in pieces(units)], finish

    def forward(units, base, h, is_near, nxt):
        steps, finish = attend_steps(units, base, h, is_near)
        maxes = {}
        following = score_steps(*nxt, maxes) if nxt else []
        interleave(steps, following)
        finish()
        if nxt:
            score_max(nxt[0], maxes)

    def send_o(h):
        copy(20, o_s.at[1, h], og.at[h], peer).start()

    def near_fwd(h, _):
        forward(near_fwd_units, 4, h, True, (near_fwd_units, 4, h + 1))
        return 0

    def far_fwd(h, _):
        forward(far, 0, h, False, (far, 0, h + 1))
        send_o(h)
        return 0

    last = n_heads - 1
    maxes = {}
    for c in (c_kv[2], c_kv[5]):
        c.wait_recv()
    keys_ready(2 * d_near)
    keys_ready(2 * d_near + 1)
    for step in score_steps(near_fwd_units, 4, 0, maxes):
        step()
    score_max(near_fwd_units, maxes)
    lax.fori_loop(0, last, near_fwd, 0)
    for c in (c_kv[0], c_kv[1], c_kv[3], c_kv[4]):
        c.wait_recv()
    for d in d_far:
        keys_ready(2 * d)
        keys_ready(2 * d + 1)
    forward(near_fwd_units, 4, last, True, (far, 0, 0))
    lax.fori_loop(0, last, far_fwd, 0)
    forward(far, 0, last, False, None)
    send_o(last)
    dkv[...] = jnp.zeros_like(dkv)

    def do_ready(i):
        for h in range(n_heads):
            delta = jnp.sum(do_s[i, h].astype(F32) * o_s[i, h].astype(F32), axis=0, keepdims=True)
            do_n[i, h] = with_columns(do_s[i, h], delta)

    def column_blocks(width):
        return [slice(start, min(start + 256, width)) for start in range(0, width, 256)]

    do_ready(0)
    for c in column_blocks(dy_s.shape[1]):
        go_f[:, c] = dot(o_s[0].reshape(hw, cols), dy_s[:, c])
    for j, c in enumerate(c_dy):
        q = slice(j * mid, (j + 1) * mid)
        c.wait_recv()
        do_s[1, :, :, q] = dot_nt(weight(w_own, "o"), dyp[q, :]).astype(BF16).reshape(n_heads, hd, mid)
    do_ready(1)
    lower = lax.broadcasted_iota(jnp.int32, (part, part), 0) >= lax.broadcasted_iota(jnp.int32, (part, part), 1)

    def prob_steps(units, bufs, h, u):
        qi, kt, first, diag = units[u]
        buf = bufs[u % len(bufs)]
        kept = {}

        def probs(c):
            r, k = slice(c * part, (c + 1) * part), slice(0, part if diag and c == 0 else cols)
            p = jnp.exp2(dot(q_n[qi, h, r], ka[kt, 0, :, k]) * c_scale)
            if diag:
                p = jnp.concatenate([p[:, :c * part], jnp.where(lower, p[:, c * part:], 0.0)], axis=1) if c else jnp.where(lower, p, 0.0)
            pb[buf, r, k] = p.astype(BF16)
            kept[c] = p

        def grads(c):
            r, k = slice(c * part, (c + 1) * part), slice(0, part if diag and c == 0 else cols)
            db[buf, r, k] = (kept[c] * dot(do_n[qi, h, r], ka[kt, 1, :, k])).astype(BF16)

        return [functools.partial(f, c) for c in (0, 1) for f in (probs, grads)]

    def grad_steps(units, bufs, h, u, dq):
        qi, kt, first, diag = units[u]
        buf = bufs[u % len(bufs)]
        kept = {}

        def over_queries(name, src, lhs, rows, c):
            q, k = slice(c * part, (c + 1) * part), slice(0, part if diag and c == 0 else cols)
            val = dot(lhs[qi, h, :, q], src[buf, q, k])
            if diag:
                dkv[kt, rows, k] += val
            elif c == 0:
                kept[name] = val
            else:
                dkv[kt, rows, :] += kept[name] + val

        def over_keys(c):
            k, q = spans(diag, c)
            val = widen(dot_nt(kvt[kt, :hd, k], db[buf, q, k]), 0.0)
            if c == 0:
                kept["q"] = val
            else:
                add_to(dq, first, kept["q"] + val)

        return ([functools.partial(over_queries, "v", pb, do_s, slice(hd, 2 * hd), c) for c in (0, 1)]
                + [functools.partial(over_queries, "k", db, q_s, slice(0, hd), c) for c in (0, 1)]
                + [functools.partial(over_keys, c) for c in (0, 1)])

    def backward(units, bufs, h, nxt):
        dq = [jnp.zeros((hd, cols), F32), jnp.zeros((hd, cols), F32)]
        for u in range(len(units)):
            if u + 1 < len(units):
                ahead = prob_steps(units, bufs, h, u + 1)
            else:
                ahead = prob_steps(*nxt, 0) if nxt else []
            products = grad_steps(units, bufs, h, u, dq)
            for i, step in enumerate(products):
                step()
                if i < len(ahead):
                    ahead[i]()
        return dq

    near_bufs, far_bufs = (0, 1, 2), (3, 4)

    def far_bwd(h, nxt):
        dq = backward(far, far_bufs, h, nxt)
        for g in (0, 1):
            acc[slots[g], h] = dq[g]

    def near_bwd(h, nxt):
        dq = backward(near, near_bufs, h, nxt)
        for g in (0, 1):
            dq_s[slots[g], h] = ((dq[g] + acc[slots[g], h]) * scale).astype(BF16)
        copy(21, dq_s.at[1, h], dqg.at[h], peer).start()

    c_pair = copy(16, dkv.at[pl.ds(2 * d_far[1], 2)], rcv.at[0], partner)
    c_cross = copy(17, dkv.at[pl.ds(2 * d_far[0], 2)], rcv.at[1], at_cp(across))
    c_near = copy(18, dkv.at[pl.ds(2 * d_near, 2)], rcv.at[2], partner)

    def far_loop(h, _):
        far_bwd(h, (far, far_bufs, h + 1))

        @pl.when(h == 3)
        def _():
            c_w.wait_recv()
            c_relay[0].start()
            c_relay[1].start()

        return 0

    def near_loop(h, _):
        near_bwd(h, (near, near_bufs, h + 1))

        @pl.when(h == 0)
        def _():
            c_pair.wait_recv()
            for slot in (0, 1):
                dkv[2 * d_far[0] + slot] += rcv[0, slot]

        @pl.when(h == 1)
        def _():
            c_cross.start()

        @pl.when(h == 3)
        def _():
            c_relay[1].wait_recv()
            c_relay[2].start()

        return 0

    for step in prob_steps(far, far_bufs, 0, 0):
        step()
    lax.fori_loop(0, last, far_loop, 0)
    far_bwd(last, (near, near_bufs, 0))
    c_pair.start()
    lax.fori_loop(0, last, near_loop, 0)
    near_bwd(last, None)
    c_near.start()

    stores = []

    def leave(src, dst):
        c = pltpu.make_async_copy(src, dst, local.at[6 + len(stores)])
        c.start()
        stores.append(c)

    for c in column_blocks(dy_s.shape[1]):
        g = go_f[:, c] + dot(o_s[1].reshape(hw, cols), dyp[:, c])
        go_s[:, :, c] = g.astype(BF16).reshape(n_heads, hd, g.shape[1])
    leave(go_s, go_ref)

    def query_weights(blocks):
        for c in blocks:
            g = dot(dq_s[0].reshape(hw, cols), x_s[:, c]) + dot(dq_s[1].reshape(hw, cols), xp[:, c])
            gq_s[:, :, c] = g.astype(BF16).reshape(n_heads, hd, g.shape[1])

    query_weights(column_blocks(x_s.shape[1])[:2])
    c_cross.wait_recv()
    c_near.wait_recv()
    for slot in (1, 0):
        total = dkv[slot] + rcv[1, slot] + rcv[2, slot]
        dkvb[slot, :hd, :] = (total[:hd, :] * scale).astype(BF16)
        dkvb[slot, hd:, :] = total[hd:, :].astype(BF16)
        if slot == 1:
            c_last = copy(19, dkvb.at[1], dkvg, peer)
            c_last.start()
    query_weights(column_blocks(x_s.shape[1])[2:])
    leave(gq_s, gq_ref)
    gkv_s[...] = (dot(dkvb[0], x_s[...]) + dot(dkvb[1], xp[...])).astype(BF16)
    leave(gkv_s.at[:hd], gk_ref)
    leave(gkv_s.at[hd:], gv_ref)
    c_o = copy(20, o_s.at[1], og, peer)
    c_o.wait_recv()
    c_relay[0].wait_recv()
    c_relay[2].wait_recv()
    rows = 256
    for i in range(cols // rows):
        blk = slice(i * rows, (i + 1) * rows)
        y = (dot_tn(o_s[0, :, :, blk].reshape(hw, rows), weight(w_own, "o"))
             + dot_tn(og[:, :, blk].reshape(hw, rows), weight(w_peer, "o")))
        y_s[blk, :] = y.astype(BF16)
    leave(y_s, y_ref)
    c_dq = copy(21, dq_s.at[1], dqg, peer)
    c_dq.wait_recv()
    for i in range(cols // rows):
        blk = slice(i * rows, (i + 1) * rows)
        dx = (dot_tn(dq_s[0, :, :, blk].reshape(hw, rows), weight(w_own, "q"))
              + dot_tn(dqg[:, :, blk].reshape(hw, rows), weight(w_peer, "q")))
        dx += dot_tn(dkvb[0, :hd, blk], weight(w_own, "k")) + dot_tn(dkvb[0, hd:, blk], weight(w_own, "v"))
        dx_f[blk, :] = dx
    c_last.wait_recv()
    for i in range(cols // rows):
        blk = slice(i * rows, (i + 1) * rows)
        dx = dx_f[blk, :] + dot_tn(dkvg[:hd, blk], weight(w_peer, "k")) + dot_tn(dkvg[hd:, blk], weight(w_peer, "v"))
        dx_s[blk, :] = dx.astype(BF16)
        leave(dx_s.at[blk], dx_ref.at[blk])
    for c in c_x + c_dy + [c_o, c_dq, c_last, c_w, c_pair, c_cross, c_near] + c_relay + c_kv:
        c.wait_send()
    for c in stores:
        c.wait()


def hand_out(n, *refs):
    src, dst, held, sems = refs[:n], refs[n:2 * n], refs[2 * n:3 * n], refs[3 * n]
    loads = [pltpu.make_async_copy(src[i], held[i], sems.at[0, i]) for i in range(n)]
    stores = [pltpu.make_async_copy(held[i], dst[i], sems.at[1, i]) for i in range(n)]
    for c in loads:
        c.start()
    for load, store in zip(loads, stores):
        load.wait()
        store.start()
    for c in stores:
        c.wait()


def solution(mesh):
    shards = mesh.shape["cp"]

    def device_fn(x_own, w_query, w_key, w_value, w_out, dy_own):
        model, n_heads, hd = w_query.shape
        cols = x_own.shape[0]
        hw = n_heads * hd
        scale = hd ** -0.5
        wq = w_query.transpose(1, 2, 0).reshape(shards, hw // shards, model)
        wk = w_key.transpose(1, 2, 0).reshape(shards, hd // shards, model)
        wv = w_value.transpose(1, 2, 0).reshape(shards, hd // shards, model)
        wo = w_out.reshape(shards, hw // shards, model)
        per_head = (2, n_heads, hd, cols)
        b = lambda *s: pltpu.VMEM(s, BF16)
        f = lambda *s: pltpu.VMEM(s, F32)
        area = n_heads * 9 * cols * cols
        y, dx, gq, gk, gv, go = pl.pallas_call(
            functools.partial(kernel, shards, n_heads, hd, scale * math.log2(math.e), scale),
            out_shape=(jax.ShapeDtypeStruct((cols, model), BF16), jax.ShapeDtypeStruct((cols, model), BF16),
                       jax.ShapeDtypeStruct((n_heads, hd, model), BF16), jax.ShapeDtypeStruct((hd, model), BF16),
                       jax.ShapeDtypeStruct((hd, model), BF16), jax.ShapeDtypeStruct((n_heads, hd, model), BF16)),
            in_specs=[HBM] * 6,
            out_specs=(ANY,) * 6,
            scratch_shapes=[b(cols, model)] * 4 + [b(shards, 2 * (hw + hd) // shards, model)] * 2
            + [b(*per_head), b(*per_head), b(*per_head), b(*per_head[1:]), b(*per_head), b(*per_head[1:]),
               b(2 * shards, 2 * hd, cols), b(2 * shards, cols, hd), b(2 * shards, 2, hd + PAD, cols),
               b(2, n_heads, cols, hd + PAD), b(2, n_heads, cols, hd + PAD), f(*per_head),
               f(2, n_heads, 1, cols), f(2, n_heads, 8, cols), f(2, 1, cols),
               f(8, cols, cols), b(5, cols, cols), b(5, cols, cols), f(2 * shards, 2 * hd, cols),
               f(shards - 1, 2, 2 * hd, cols), b(2, 2 * hd, cols), b(2 * hd, cols),
               b(cols, model), b(cols, model), f(cols, model), b(n_heads, hd, model), b(2 * hd, model), b(n_heads, hd, model), f(hw, model),
               pltpu.SemaphoreType.DMA((N_COPIES,)), pltpu.SemaphoreType.DMA((N_COPIES,)), pltpu.SemaphoreType.DMA((13,))],
            compiler_params=pltpu.CompilerParams(vmem_limit_bytes=VMEM_LIMIT, collective_id=0, has_side_effects=True),
            cost_estimate=pl.CostEstimate(flops=area * 7 * 2 * hd, bytes_accessed=16 << 20, transcendentals=2 * area),
            name="attention",
        )(x_own, dy_own, wq, wk, wv, wo)
        outs = (y, dx, gq, gk, gv, go)
        y, dx, gq, gk, gv, go = pl.pallas_call(
            functools.partial(hand_out, len(outs)),
            out_shape=tuple(jax.ShapeDtypeStruct(o.shape, o.dtype) for o in outs),
            in_specs=[HBM] * len(outs),
            out_specs=(HBM,) * len(outs),
            scratch_shapes=[pltpu.VMEM(o.shape, o.dtype) for o in outs] + [pltpu.SemaphoreType.DMA((2, len(outs)))],
            cost_estimate=pl.CostEstimate(flops=0, bytes_accessed=8 << 20, transcendentals=0),
            name="hand_out",
        )(*outs)
        back = lambda g, n: g.reshape(n, hd, model).transpose(2, 0, 1)[None]
        return y, dx, back(gq, n_heads), back(gk, 1), back(gv, 1), go[None]

    return jax.shard_map(device_fn, mesh=mesh,
                         in_specs=(ROW_SPEC, HEAD_SPEC, HEAD_SPEC, HEAD_SPEC, OUT_W_SPEC, ROW_SPEC),
                         out_specs=(ROW_SPEC, ROW_SPEC, GRAD_SPEC, GRAD_SPEC, GRAD_SPEC, GRAD_OUT_SPEC),
                         check_vma=False)
```

```python
import functools
import math

import jax
import jax.numpy as jnp
from jax import lax
from jax.experimental import pallas as pl
from jax.experimental.pallas import tpu as pltpu
from jax.sharding import PartitionSpec as P

ROW_SPEC = P(("dp", "cp", "tp"), None)
HEAD_SPEC = P(None, "tp", None)
OUT_W_SPEC = P("tp", None, None)
GRAD_SPEC = P(("dp", "cp"), None, "tp", None)
GRAD_OUT_SPEC = P(("dp", "cp"), "tp", None, None)
F32 = jnp.float32
BF16 = jnp.bfloat16
NT = (((1,), (1,)), ((), ()))
TN = (((0,), (0,)), ((), ()))
ANY = pl.BlockSpec(memory_space=pl.ANY)
HBM = pl.BlockSpec(memory_space=pltpu.HBM)
VMEM_LIMIT = 64 * 1024 * 1024 - 64 * 1024
N_COPIES = 24
PAD = 16
BIG = 3.0e38


def dot(a, b):
    return jnp.dot(a, b, preferred_element_type=F32)


def dot_nt(a, b):
    return lax.dot_general(a, b, NT, preferred_element_type=F32)


def dot_tn(a, b):
    return lax.dot_general(a, b, TN, preferred_element_type=F32)


def shard_units(rank, half, d, shards):
    early = (rank + shards - d) // shards
    slot = early * half + (1 - early) * (1 - half)
    return [(slot, 2 * d + half, early, False), (1 - half, 2 * d + slot, 0, False)]


def diag_mask(size):
    return lax.broadcasted_iota(jnp.int32, (size, size), 1) >= lax.broadcasted_iota(jnp.int32, (size, size), 0)


def pick(first, pair):
    if isinstance(first, int):
        return pair[1 - first]
    return jnp.where(first == 1, pair[0], pair[1])


def add_to(pair, first, value):
    if isinstance(first, int):
        pair[1 - first] = pair[1 - first] + value
    else:
        pair[0] = pair[0] + jnp.where(first == 1, value, 0.0)
        pair[1] = pair[1] + jnp.where(first == 1, 0.0, value)


def transpose_bf16(x):
    return x.astype(F32).T.astype(BF16)


def with_columns(x_t, row):
    hi = jnp.clip(row, -BIG, BIG).astype(BF16).astype(F32)
    mid = (row - hi).astype(BF16).astype(F32)
    low = row - hi - mid
    line = lax.broadcasted_iota(jnp.int32, (PAD, row.shape[1]), 0)
    extra = jnp.where(line == 0, hi, jnp.where(line == 1, mid, jnp.where(line == 2, low, 0.0)))
    return jnp.concatenate([x_t.astype(F32), extra], axis=0).T.astype(BF16)


def kernel(shards, n_heads, hd, c_scale, scale,
           x_hbm, dy_hbm, wq_hbm, wk_hbm, wv_hbm, wo_hbm,
           y_ref, dx_ref, gq_ref, gk_ref, gv_ref, go_ref,
           x_s, xp, dy_s, dyp, w_own, w_peer,
           q_s, do_s, o_s, og, dq_s, dqg, kvt, k_s, ka, q_n, do_n, acc, m_s, l_s, max_s, s_s, pb, db, dkv, rcv, dkvb, dkvg,
           y_s, dx_s, dx_f, gq_s, gkv_s, go_s, go_f, send, recv, local):
    rank = lax.axis_index("cp")
    half = lax.axis_index("tp")
    core = rank % 2
    cols = q_s.shape[-1]
    hw = n_heads * hd
    peer = {"tp": 1 - half}
    partner = {"cp": rank + 1 - 2 * core}

    d_near = shards - 1 - 2 * core
    d_far = (2, 1 + 2 * core)

    def at_cp(i):
        return {"cp": i % shards}

    def copy(i, src, dst, device):
        return pltpu.make_async_remote_copy(src_ref=src, dst_ref=dst, send_sem=send.at[i], recv_sem=recv.at[i],
                                            device_id=device, device_id_type=pl.DeviceIdType.MESH)

    n_o, n_k = hw // shards, hd // shards
    w_rows = {"o": (0, n_o), "q": (n_o, n_o), "k": (2 * n_o, n_k), "v": (2 * n_o + n_k, n_k)}

    def load(i, src, name):
        start, size = w_rows[name]
        return pltpu.make_async_copy(src, w_own.at[:, pl.ds(start, size), :], local.at[i])

    def weight(ref, name):
        start, size = w_rows[name]
        return ref[:, start:start + size, :].reshape(shards * size, ref.shape[2])

    loads = [pltpu.make_async_copy(x_hbm, x_s, local.at[0]), load(1, wk_hbm, "k"), load(2, wv_hbm, "v"), load(3, wq_hbm, "q"),
             load(4, wo_hbm, "o"), pltpu.make_async_copy(dy_hbm, dy_s, local.at[5])]
    for c in loads:
        c.start()
    barrier = pltpu.get_barrier_semaphore()
    pl.semaphore_signal(barrier, inc=1, device_id=peer, device_id_type=pl.DeviceIdType.MESH)
    for d in range(1, shards):
        pl.semaphore_signal(barrier, inc=1, device_id=at_cp(rank + d), device_id_type=pl.DeviceIdType.MESH)
    pl.semaphore_wait(barrier, shards)

    across = (rank + 2) % shards
    mid = cols // 2
    c_x = [copy(i, x_hbm.at[pl.ds(j * mid, mid)], xp.at[pl.ds(j * mid, mid)], peer) for i, j in ((0, 0), (22, 1))]
    c_dy = [copy(i, dy_hbm.at[pl.ds(j * mid, mid)], dyp.at[pl.ds(j * mid, mid)], peer) for i, j in ((1, 0), (23, 1))]
    c_w = copy(2, w_own.at[rank], w_peer.at[rank], peer)
    c_relay = [copy(3, w_peer.at[rank], w_peer.at[rank], partner), copy(4, w_peer.at[rank], w_peer.at[rank], at_cp(across)),
               copy(5, w_peer.at[across], w_peer.at[across], partner)]
    for c in c_x + c_dy:
        c.start()

    def send_kv(slot):
        ahead = (2, shards - 1 - 2 * core, 1 + 2 * core)
        cs = [copy(10 + 3 * slot + i, kvt.at[slot], kvt.at[2 * d + slot], at_cp(rank + d)) for i, d in enumerate(ahead)]
        for c in cs:
            c.start()
        return cs

    def keys_ready(tile):
        k_s[tile] = transpose_bf16(kvt[tile, :hd, :])
        minus = jnp.where(lax.broadcasted_iota(jnp.int32, (PAD, cols), 0) < 3, -1.0, 0.0).astype(BF16)
        for i in (0, 1):
            ka[tile, i, :hd, :] = kvt[tile, i * hd:(i + 1) * hd, :]
            ka[tile, i, hd:, :] = minus

    for c in loads[:3]:
        c.wait()
    kvt[0, :hd, :] = dot_nt(weight(w_own, "k"), x_s[...]).astype(BF16)
    kvt[0, hd:, :] = dot_nt(weight(w_own, "v"), x_s[...]).astype(BF16)
    c_kv = send_kv(0)
    loads[3].wait()
    q_s[0] = dot_nt(weight(w_own, "q"), x_s[...]).astype(BF16).reshape(n_heads, hd, cols)
    loads[4].wait()
    c_w.start()
    loads[5].wait()
    do_s[0] = dot_nt(weight(w_own, "o"), dy_s[...]).astype(BF16).reshape(n_heads, hd, cols)
    keys_ready(0)
    part = cols // 2
    triangle = diag_mask(part)

    def own_diagonal(h, _):
        s0 = dot(k_s[0, :part], q_s[0, h])
        s0 = jnp.concatenate([jnp.where(triangle, s0[:, :part], -jnp.inf), s0[:, part:]], axis=1)
        s1 = jnp.where(triangle, dot(k_s[0, part:], q_s[0, h, :, part:]), -jnp.inf)
        m0, m1 = jnp.max(s0, axis=0, keepdims=True), jnp.max(s1, axis=0, keepdims=True)
        m = jnp.concatenate([m0[:, :part], jnp.maximum(m0[:, part:], m1)], axis=1) * c_scale
        p0, p1 = jnp.exp2(s0 * c_scale - m), jnp.exp2(s1 * c_scale - m[:, part:])
        zeros = jnp.zeros((8, part), F32)
        l_s[0, h] = (jnp.sum(p0.reshape(part // 8, 8, cols), axis=0)
                     + jnp.concatenate([zeros, jnp.sum(p1.reshape(part // 8, 8, part), axis=0)], axis=1))
        o1 = dot(kvt[0, hd:, part:], p1.astype(BF16))
        acc[0, h] = dot(kvt[0, hd:, :part], p0.astype(BF16)) + jnp.concatenate([jnp.zeros_like(o1), o1], axis=1)
        m_s[0, h] = m
        m_s[1, h] = jnp.full_like(m, -jnp.inf)
        l_s[1, h] = jnp.zeros((8, cols), F32)
        acc[1, h] = jnp.zeros((hd, cols), F32)
        return 0

    lax.fori_loop(0, n_heads, own_diagonal, 0)
    dkv[...] = jnp.zeros_like(dkv)
    for c in c_kv:
        c.wait_recv()
    for d in (d_near,) + d_far:
        keys_ready(2 * d)
    for j, c in enumerate(c_x):
        q = slice(j * mid, (j + 1) * mid)
        c.wait_recv()
        kvt[1, :hd, q] = dot_nt(weight(w_own, "k"), xp[q, :]).astype(BF16)
        kvt[1, hd:, q] = dot_nt(weight(w_own, "v"), xp[q, :]).astype(BF16)
        if j == 1:
            c_kv += send_kv(1)
        q_s[1, :, :, q] = dot_nt(weight(w_own, "q"), xp[q, :]).astype(BF16).reshape(n_heads, hd, mid)
    keys_ready(1)

    near = ([(half, half, 1, True), (1 - half, half, 0, False), (1 - half, 1 - half, 0, True)]
            + shard_units(rank, half, d_near, shards))
    far = shard_units(rank, half, d_far[0], shards) + shard_units(rank, half, d_far[1], shards)
    slots = (half, 1 - half)
    near_fwd_units = [(1, 1, half, True)] + near[1:2] + near[3:]

    def spans(diag, c):
        return slice(c * part, (c + 1) * part), slice(c * part, cols) if diag else slice(0, cols)

    def masked(x, diag, fill):
        if not diag:
            return x
        left = jnp.where(triangle, x[:, :part], fill)
        return left if x.shape[1] == part else jnp.concatenate([left, x[:, part:]], axis=1)

    def widen(x, fill):
        if x.shape[1] == cols:
            return x
        return jnp.concatenate([jnp.full((x.shape[0], cols - x.shape[1]), fill, x.dtype), x], axis=1)

    def interleave(first_list, second_list):
        i = j = 0
        while i < len(first_list) or j < len(second_list):
            if j >= len(second_list) or (i < len(first_list) and i * len(second_list) <= j * len(first_list)):
                first_list[i]()
                i += 1
            else:
                second_list[j]()
                j += 1

    def pieces(units):
        return [(u, c) for u, unit in enumerate(units) for c in ((0, 1) if unit[3] else (None,))]

    def score_steps(units, base, h, maxes):
        def step(u, c):
            qi, kt, first, diag = units[u]
            r, q = spans(diag, c) if diag else (slice(0, cols), slice(0, cols))
            s = masked(dot(k_s[kt, r], q_s[qi, h, :, q]), diag, -jnp.inf)
            s_s[base + u, r, q] = s
            mx = widen(jnp.max(s.reshape(s.shape[0] // 8, 8, s.shape[1]), axis=0), -jnp.inf)
            maxes[u] = jnp.maximum(maxes[u], mx) if c == 1 else mx
        return [functools.partial(step, u, c) for u, c in pieces(units)]

    def score_max(units, maxes):
        for g in (0, 1):
            best = None
            for u, (_, _, first, _) in enumerate(units):
                if isinstance(first, int):
                    if first == g:
                        continue
                    val = maxes[u]
                else:
                    val = jnp.where(first == 1 - g, maxes[u], -jnp.inf)
                best = val if best is None else jnp.maximum(best, val)
            max_s[g] = jnp.max(best, axis=0, keepdims=True) * c_scale

    def attend_steps(units, base, h, is_near):
        old = [m_s[slots[g], h] for g in (0, 1)]
        m = [jnp.maximum(max_s[g], old[g]) for g in (0, 1)]
        fix = [jnp.exp2(x - y) for x, y in zip(old, m)]
        l = [l_s[slots[g], h] * fix[g] for g in (0, 1)]
        o = [acc[slots[g], h] * fix[g] for g in (0, 1)]
        sums = {}

        def step(u, c):
            qi, kt, first, diag = units[u]
            r, q = spans(diag, c) if diag else (slice(0, cols), slice(0, cols))
            p = jnp.exp2(s_s[base + u, r, q] * c_scale - pick(first, m)[:, q])
            l_u = widen(jnp.sum(p.reshape(p.shape[0] // 8, 8, p.shape[1]), axis=0), 0.0)
            o_u = widen(dot(kvt[kt, hd:, r], p.astype(BF16)), 0.0)
            if c is None:
                add_to(l, first, l_u)
                add_to(o, first, o_u)
            elif c == 0:
                sums[u] = (l_u, o_u)
            else:
                add_to(l, first, sums[u][0] + l_u)
                add_to(o, first, sums[u][1] + o_u)

        def finish():
            for g in (0, 1):
                if is_near:
                    m_s[slots[g], h] = m[g]
                    l_s[slots[g], h] = l[g]
                    acc[slots[g], h] = o[g]
                else:
                    l_row = jnp.sum(l[g], axis=0, keepdims=True)
                    o_s[slots[g], h] = (o[g] / l_row).astype(BF16)
                    q_n[slots[g], h] = with_columns(q_s[slots[g], h], (m[g] + jnp.log2(l_row)) * (1.0 / c_scale))

        return [functools.partial(step, u, c) for u, c in pieces(units)], finish

    def forward(units, base, h, is_near, nxt):
        steps, finish = attend_steps(units, base, h, is_near)
        maxes = {}
        following = score_steps(*nxt, maxes) if nxt else []
        interleave(steps, following)
        finish()
        if nxt:
            score_max(nxt[0], maxes)

    def send_o(h):
        copy(20, o_s.at[1, h], og.at[h], peer).start()

    def near_fwd(h, _):
        forward(near_fwd_units, 4, h, True, (near_fwd_units, 4, h + 1))
        return 0

    def far_fwd(h, _):
        forward(far, 0, h, False, (far, 0, h + 1))
        send_o(h)
        return 0

    last = n_heads - 1
    maxes = {}
    c_kv[5].wait_recv()
    keys_ready(2 * d_near + 1)
    for step in score_steps(near_fwd_units, 4, 0, maxes):
        step()
    score_max(near_fwd_units, maxes)
    lax.fori_loop(0, last, near_fwd, 0)
    for c in c_kv[3:5]:
        c.wait_recv()
    for d in d_far:
        keys_ready(2 * d + 1)
    forward(near_fwd_units, 4, last, True, (far, 0, 0))
    lax.fori_loop(0, last, far_fwd, 0)
    forward(far, 0, last, False, None)
    send_o(last)

    def do_ready(i):
        for h in range(n_heads):
            delta = jnp.sum(do_s[i, h].astype(F32) * o_s[i, h].astype(F32), axis=0, keepdims=True)
            do_n[i, h] = with_columns(do_s[i, h], delta)

    def column_blocks(width):
        return [slice(start, min(start + 256, width)) for start in range(0, width, 256)]

    do_ready(0)
    for c in column_blocks(dy_s.shape[1]):
        go_f[:, c] = dot(o_s[0].reshape(hw, cols), dy_s[:, c])
    for j, c in enumerate(c_dy):
        q = slice(j * mid, (j + 1) * mid)
        c.wait_recv()
        do_s[1, :, :, q] = dot_nt(weight(w_own, "o"), dyp[q, :]).astype(BF16).reshape(n_heads, hd, mid)
    do_ready(1)
    lower = lax.broadcasted_iota(jnp.int32, (part, part), 0) >= lax.broadcasted_iota(jnp.int32, (part, part), 1)

    def prob_steps(units, bufs, h, u):
        qi, kt, first, diag = units[u]
        buf = bufs[u % len(bufs)]
        kept = {}

        def probs(c):
            r, k = slice(c * part, (c + 1) * part), slice(0, part if diag and c == 0 else cols)
            p = jnp.exp2(dot(q_n[qi, h, r], ka[kt, 0, :, k]) * c_scale)
            if diag:
                p = jnp.concatenate([p[:, :c * part], jnp.where(lower, p[:, c * part:], 0.0)], axis=1) if c else jnp.where(lower, p, 0.0)
            pb[buf, r, k] = p.astype(BF16)
            kept[c] = p

        def grads(c):
            r, k = slice(c * part, (c + 1) * part), slice(0, part if diag and c == 0 else cols)
            db[buf, r, k] = (kept[c] * dot(do_n[qi, h, r], ka[kt, 1, :, k])).astype(BF16)

        return [functools.partial(f, c) for c in (0, 1) for f in (probs, grads)]

    def grad_steps(units, bufs, h, u, dq):
        qi, kt, first, diag = units[u]
        buf = bufs[u % len(bufs)]
        kept = {}

        def over_queries(name, src, lhs, rows, c):
            q, k = slice(c * part, (c + 1) * part), slice(0, part if diag and c == 0 else cols)
            val = dot(lhs[qi, h, :, q], src[buf, q, k])
            if diag:
                dkv[kt, rows, k] += val
            elif c == 0:
                kept[name] = val
            else:
                dkv[kt, rows, :] += kept[name] + val

        def over_keys(c):
            k, q = spans(diag, c)
            val = widen(dot_nt(kvt[kt, :hd, k], db[buf, q, k]), 0.0)
            if c == 0:
                kept["q"] = val
            else:
                add_to(dq, first, kept["q"] + val)

        return ([functools.partial(over_queries, "v", pb, do_s, slice(hd, 2 * hd), c) for c in (0, 1)]
                + [functools.partial(over_queries, "k", db, q_s, slice(0, hd), c) for c in (0, 1)]
                + [functools.partial(over_keys, c) for c in (0, 1)])

    def backward(units, bufs, h, nxt):
        dq = [jnp.zeros((hd, cols), F32), jnp.zeros((hd, cols), F32)]
        for u in range(len(units)):
            if u + 1 < len(units):
                ahead = prob_steps(units, bufs, h, u + 1)
            else:
                ahead = prob_steps(*nxt, 0) if nxt else []
            products = grad_steps(units, bufs, h, u, dq)
            for i, step in enumerate(products):
                step()
                if i < len(ahead):
                    ahead[i]()
        return dq

    near_bufs, far_bufs = (0, 1, 2), (3, 4)

    def far_bwd(h, nxt):
        dq = backward(far, far_bufs, h, nxt)
        for g in (0, 1):
            acc[slots[g], h] = dq[g]

    def near_bwd(h, nxt):
        dq = backward(near, near_bufs, h, nxt)
        for g in (0, 1):
            dq_s[slots[g], h] = ((dq[g] + acc[slots[g], h]) * scale).astype(BF16)
        copy(21, dq_s.at[1, h], dqg.at[h], peer).start()

    c_pair = copy(16, dkv.at[pl.ds(2 * d_far[1], 2)], rcv.at[0], partner)
    c_cross = copy(17, dkv.at[pl.ds(2 * d_far[0], 2)], rcv.at[1], at_cp(across))
    c_near = copy(18, dkv.at[pl.ds(2 * d_near, 2)], rcv.at[2], partner)

    def far_loop(h, _):
        far_bwd(h, (far, far_bufs, h + 1))

        @pl.when(h == 3)
        def _():
            c_w.wait_recv()
            c_relay[0].start()
            c_relay[1].start()

        return 0

    def near_loop(h, _):
        near_bwd(h, (near, near_bufs, h + 1))

        @pl.when(h == 0)
        def _():
            c_pair.wait_recv()
            for slot in (0, 1):
                dkv[2 * d_far[0] + slot] += rcv[0, slot]

        @pl.when(h == 1)
        def _():
            c_cross.start()

        @pl.when(h == 3)
        def _():
            c_relay[1].wait_recv()
            c_relay[2].start()

        return 0

    for step in prob_steps(far, far_bufs, 0, 0):
        step()
    lax.fori_loop(0, last, far_loop, 0)
    far_bwd(last, (near, near_bufs, 0))
    c_pair.start()
    lax.fori_loop(0, last, near_loop, 0)
    near_bwd(last, None)
    c_near.start()

    stores = []

    def leave(src, dst):
        c = pltpu.make_async_copy(src, dst, local.at[6 + len(stores)])
        c.start()
        stores.append(c)

    for c in column_blocks(dy_s.shape[1]):
        g = go_f[:, c] + dot(o_s[1].reshape(hw, cols), dyp[:, c])
        go_s[:, :, c] = g.astype(BF16).reshape(n_heads, hd, g.shape[1])
    leave(go_s, go_ref)

    def query_weights(blocks):
        for c in blocks:
            g = dot(dq_s[0].reshape(hw, cols), x_s[:, c]) + dot(dq_s[1].reshape(hw, cols), xp[:, c])
            gq_s[:, :, c] = g.astype(BF16).reshape(n_heads, hd, g.shape[1])

    query_weights(column_blocks(x_s.shape[1])[:2])
    c_cross.wait_recv()
    c_near.wait_recv()
    for slot in (1, 0):
        total = dkv[slot] + rcv[1, slot] + rcv[2, slot]
        dkvb[slot, :hd, :] = (total[:hd, :] * scale).astype(BF16)
        dkvb[slot, hd:, :] = total[hd:, :].astype(BF16)
        if slot == 1:
            c_last = copy(19, dkvb.at[1], dkvg, peer)
            c_last.start()
    query_weights(column_blocks(x_s.shape[1])[2:])
    leave(gq_s, gq_ref)
    gkv_s[...] = (dot(dkvb[0], x_s[...]) + dot(dkvb[1], xp[...])).astype(BF16)
    leave(gkv_s.at[:hd], gk_ref)
    leave(gkv_s.at[hd:], gv_ref)
    c_o = copy(20, o_s.at[1], og, peer)
    c_o.wait_recv()
    c_relay[0].wait_recv()
    c_relay[2].wait_recv()
    rows = 256
    for i in range(cols // rows):
        blk = slice(i * rows, (i + 1) * rows)
        y = (dot_tn(o_s[0, :, :, blk].reshape(hw, rows), weight(w_own, "o"))
             + dot_tn(og[:, :, blk].reshape(hw, rows), weight(w_peer, "o")))
        y_s[blk, :] = y.astype(BF16)
    leave(y_s, y_ref)
    c_dq = copy(21, dq_s.at[1], dqg, peer)
    c_dq.wait_recv()
    for i in range(cols // rows):
        blk = slice(i * rows, (i + 1) * rows)
        dx = (dot_tn(dq_s[0, :, :, blk].reshape(hw, rows), weight(w_own, "q"))
              + dot_tn(dqg[:, :, blk].reshape(hw, rows), weight(w_peer, "q")))
        dx += dot_tn(dkvb[0, :hd, blk], weight(w_own, "k")) + dot_tn(dkvb[0, hd:, blk], weight(w_own, "v"))
        dx_f[blk, :] = dx
    c_last.wait_recv()
    for i in range(cols // rows):
        blk = slice(i * rows, (i + 1) * rows)
        dx = dx_f[blk, :] + dot_tn(dkvg[:hd, blk], weight(w_peer, "k")) + dot_tn(dkvg[hd:, blk], weight(w_peer, "v"))
        dx_s[blk, :] = dx.astype(BF16)
        leave(dx_s.at[blk], dx_ref.at[blk])
    for c in c_x + c_dy + [c_o, c_dq, c_last, c_w, c_pair, c_cross, c_near] + c_relay + c_kv:
        c.wait_send()
    for c in stores:
        c.wait()


def hand_out(n, *refs):
    src, dst, held, sems = refs[:n], refs[n:2 * n], refs[2 * n:3 * n], refs[3 * n]
    loads = [pltpu.make_async_copy(src[i], held[i], sems.at[0, i]) for i in range(n)]
    stores = [pltpu.make_async_copy(held[i], dst[i], sems.at[1, i]) for i in range(n)]
    for c in loads:
        c.start()
    for load, store in zip(loads, stores):
        load.wait()
        store.start()
    for c in stores:
        c.wait()


def solution(mesh):
    shards = mesh.shape["cp"]

    def device_fn(x_own, w_query, w_key, w_value, w_out, dy_own):
        model, n_heads, hd = w_query.shape
        cols = x_own.shape[0]
        hw = n_heads * hd
        scale = hd ** -0.5
        wq = w_query.transpose(1, 2, 0).reshape(shards, hw // shards, model)
        wk = w_key.transpose(1, 2, 0).reshape(shards, hd // shards, model)
        wv = w_value.transpose(1, 2, 0).reshape(shards, hd // shards, model)
        wo = w_out.reshape(shards, hw // shards, model)
        per_head = (2, n_heads, hd, cols)
        b = lambda *s: pltpu.VMEM(s, BF16)
        f = lambda *s: pltpu.VMEM(s, F32)
        area = n_heads * 9 * cols * cols
        y, dx, gq, gk, gv, go = pl.pallas_call(
            functools.partial(kernel, shards, n_heads, hd, scale * math.log2(math.e), scale),
            out_shape=(jax.ShapeDtypeStruct((cols, model), BF16), jax.ShapeDtypeStruct((cols, model), BF16),
                       jax.ShapeDtypeStruct((n_heads, hd, model), BF16), jax.ShapeDtypeStruct((hd, model), BF16),
                       jax.ShapeDtypeStruct((hd, model), BF16), jax.ShapeDtypeStruct((n_heads, hd, model), BF16)),
            in_specs=[HBM] * 6,
            out_specs=(ANY,) * 6,
            scratch_shapes=[b(cols, model)] * 4 + [b(shards, 2 * (hw + hd) // shards, model)] * 2
            + [b(*per_head), b(*per_head), b(*per_head), b(*per_head[1:]), b(*per_head), b(*per_head[1:]),
               b(2 * shards, 2 * hd, cols), b(2 * shards, cols, hd), b(2 * shards, 2, hd + PAD, cols),
               b(2, n_heads, cols, hd + PAD), b(2, n_heads, cols, hd + PAD), f(*per_head),
               f(2, n_heads, 1, cols), f(2, n_heads, 8, cols), f(2, 1, cols),
               f(8, cols, cols), b(5, cols, cols), b(5, cols, cols), f(2 * shards, 2 * hd, cols),
               f(shards - 1, 2, 2 * hd, cols), b(2, 2 * hd, cols), b(2 * hd, cols),
               b(cols, model), b(cols, model), f(cols, model), b(n_heads, hd, model), b(2 * hd, model), b(n_heads, hd, model), f(hw, model),
               pltpu.SemaphoreType.DMA((N_COPIES,)), pltpu.SemaphoreType.DMA((N_COPIES,)), pltpu.SemaphoreType.DMA((13,))],
            compiler_params=pltpu.CompilerParams(vmem_limit_bytes=VMEM_LIMIT, collective_id=0, has_side_effects=True),
            cost_estimate=pl.CostEstimate(flops=area * 7 * 2 * hd, bytes_accessed=16 << 20, transcendentals=2 * area),
            name="attention",
        )(x_own, dy_own, wq, wk, wv, wo)
        outs = (y, dx, gq, gk, gv, go)
        y, dx, gq, gk, gv, go = pl.pallas_call(
            functools.partial(hand_out, len(outs)),
            out_shape=tuple(jax.ShapeDtypeStruct(o.shape, o.dtype) for o in outs),
            in_specs=[HBM] * len(outs),
            out_specs=(HBM,) * len(outs),
            scratch_shapes=[pltpu.VMEM(o.shape, o.dtype) for o in outs] + [pltpu.SemaphoreType.DMA((2, len(outs)))],
            cost_estimate=pl.CostEstimate(flops=0, bytes_accessed=8 << 20, transcendentals=0),
            name="hand_out",
        )(*outs)
        back = lambda g, n: g.reshape(n, hd, model).transpose(2, 0, 1)[None]
        return y, dx, back(gq, n_heads), back(gk, 1), back(gv, 1), go[None]

    return jax.shard_map(device_fn, mesh=mesh,
                         in_specs=(ROW_SPEC, HEAD_SPEC, HEAD_SPEC, HEAD_SPEC, OUT_W_SPEC, ROW_SPEC),
                         out_specs=(ROW_SPEC, ROW_SPEC, GRAD_SPEC, GRAD_SPEC, GRAD_SPEC, GRAD_OUT_SPEC),
                         check_vma=False)
```
